32 devices in a mesh: fsdp: 2 (over x), ctx: 4 (over z), tp: 4 (over y, core).
Axes of the slice: x: 2, y: 2, z: 4, core: 2. Of those that a mesh axis runs over, the one named last changes fastest.
Arguments:
- tokens: bfloat16 [2, 4096, 1024], P('fsdp', 'ctx'), may hold values from -6 to 6
- condition: float32 [2, 1024], replicated, may hold values from -6 to 6
- cotangent: bfloat16 [2, 4096, 1024], P('fsdp', 'ctx'), may hold values from -6 to 6
- joint_weight: float32 [1024, 3072], P(('fsdp', 'ctx'), 'tp'), may hold values from -0.1875 to 0.1875
- joint_moments: float32 [2, 1024, 3072], P(None, ('fsdp', 'ctx'), 'tp'), as said below
- output_weight: float32 [1024, 1024], P(('fsdp', 'ctx'), 'tp'), may hold values from -3 to 3
- output_moments: float32 [2, 1024, 1024], P(None, ('fsdp', 'ctx'), 'tp'), as said below
- expand_weight: float32 [1024, 4096], P(('fsdp', 'ctx'), 'tp'), may hold values from -0.1875 to 0.1875
- expand_moments: float32 [2, 1024, 4096], P(None, ('fsdp', 'ctx'), 'tp'), as said below
- shrink_weight: float32 [1024, 4096], P(('fsdp', 'ctx'), 'tp'), may hold values from -0.09375 to 0.09375
- shrink_moments: float32 [2, 1024, 4096], P(None, ('fsdp', 'ctx'), 'tp'), as said below
- modulate_weight: float32 [1024, 6144], P(('fsdp', 'ctx'), 'tp'), may hold values from -0.1875 to 0.1875
- modulate_moments: float32 [2, 1024, 6144], P(None, ('fsdp', 'ctx'), 'tp'), as said below
- attention_bias: float32 [2048], P('tp'), may hold values from -3 to 3
- attention_moments: float32 [2, 2048], P(None, 'tp'), as said below
- hidden_bias: float32 [4096], P('tp'), may hold values from -3 to 3
- hidden_moments: float32 [2, 4096], P(None, 'tp'), as said below
- condition_bias: float32 [6144], P('tp'), may hold values from -3 to 3
- condition_moments: float32 [2, 6144], P(None, 'tp'), as said below
- residual_bias: float32 [2, 1024], replicated, may hold values from -3 to 3
- residual_moments: float32 [2, 2, 1024], replicated, as said below
Outputs:
- mixed: bfloat16 [2, 4096, 1024], P('fsdp', 'ctx')
- tokens_grad: float32 [2, 4096, 1024], P('fsdp', 'ctx')
- condition_grad: float32 [2, 1024], P('fsdp')
- grad_norm: float32 [], replicated
- joint_updated: float32 [1024, 3072], P(('fsdp', 'ctx'), 'tp')
- joint_averages: float32 [2, 1024, 3072], P(None, ('fsdp', 'ctx'), 'tp')
- output_updated: float32 [1024, 1024], P(('fsdp', 'ctx'), 'tp')
- output_averages: float32 [2, 1024, 1024], P(None, ('fsdp', 'ctx'), 'tp')
- expand_updated: float32 [1024, 4096], P(('fsdp', 'ctx'), 'tp')
- expand_averages: float32 [2, 1024, 4096], P(None, ('fsdp', 'ctx'), 'tp')
- shrink_updated: float32 [1024, 4096], P(('fsdp', 'ctx'), 'tp')
- shrink_averages: float32 [2, 1024, 4096], P(None, ('fsdp', 'ctx'), 'tp')
- modulate_updated: float32 [1024, 6144], P(('fsdp', 'ctx'), 'tp')
- modulate_averages: float32 [2, 1024, 6144], P(None, ('fsdp', 'ctx'), 'tp')
- attention_updated: float32 [2048], P('tp')
- attention_averages: float32 [2, 2048], P(None, 'tp')
- hidden_updated: float32 [4096], P('tp')
- hidden_averages: float32 [2, 4096], P(None, 'tp')
- condition_updated: float32 [6144], P('tp')
- condition_averages: float32 [2, 6144], P(None, 'tp')
- residual_updated: float32 [2, 1024], replicated
- residual_averages: float32 [2, 2, 1024], replicated
The draws below stay inside these ranges and needn't reach their ends.
Inputs may be any that keep to these rules, and one draw needn't show every extreme that they name: `joint_moments`: the roots of the second moments (index 1 of the first dimension) are positive. `output_moments`: the roots of the second moments are positive. `expand_moments`: the roots of the second moments are positive. `shrink_moments`: the roots of the second moments are positive. `modulate_moments`: the roots of the second moments are positive. `attention_moments`: the roots of the second moments are positive. `hidden_moments`: the roots of the second moments are positive. `condition_moments`: the roots of the second moments are positive. `residual_moments`: the roots of the second moments are positive.
All inputs are finite; a program needn't handle non-finite values.
Results may differ from the reference program's by a relative error of at most 0.0095.
The reference program's roundings to bfloat16 on the way count: a program that leaves them out, or rounds other values in their place, can miss the bound.
Values may be sent and summed in bfloat16 or wider, within the bound.
A program may use at most 256 MiB of HBM per device.

```python
import jax
import jax.numpy as jnp
from jax import lax

D = 1024
HEADS = 16
HEAD_DIM = 64
FF = 4096
SEQ = 4096
ADAM_STEP = 10
LATENTS = 2


def moment_pair(key, shape, marker):
    own_key = jax.random.fold_in(key, marker)
    first_key = jax.random.fold_in(own_key, 11)
    second_key = jax.random.fold_in(own_key, 23)
    first_moment = jax.random.normal(first_key, shape, jnp.float32) * 3e-05
    root_moment = jnp.exp(jax.random.uniform(second_key, shape, jnp.float32, -12.65, -10.35))
    return jnp.stack([first_moment, root_moment])


def draw_joint_moments(key, part):
    return moment_pair(key, (D, 3 * D), 101)


def draw_output_moments(key, part):
    return moment_pair(key, (D, D), 102)


def draw_expand_moments(key, part):
    return moment_pair(key, (D, FF), 103)


def draw_shrink_moments(key, part):
    return moment_pair(key, (D, FF), 104)


def draw_modulate_moments(key, part):
    return moment_pair(key, (D, 6 * D), 105)


def draw_attention_moments(key, part):
    return moment_pair(key, (2 * D,), 106)


def draw_hidden_moments(key, part):
    return moment_pair(key, (FF,), 107)


def draw_condition_moments(key, part):
    return moment_pair(key, (6 * D,), 108)


def draw_residual_moments(key, part):
    return moment_pair(key, (2, D), 109)


def level_of(stream_key, extent, shards, least, largest):
    def one(axis_at, shards_of):
        heights = jax.random.uniform(jax.random.fold_in(jax.random.fold_in(stream_key, 6), axis_at), (shards_of,), jnp.float32, least / len(shards), largest / len(shards))
        return jnp.repeat(jnp.exp(heights), extent[axis_at] // shards_of).reshape((-1,) + (1,) * (len(extent) - axis_at - 1))

    gain = one(*shards[0])
    for cut in shards[1:]:
        gain = gain * one(*cut)
    return gain


def bell_draw(key, dims, scale, limit, cuts=(), dtype=jnp.bfloat16):
    factor_of = level_of(key, dims, cuts, -0.22, 0.18) if cuts else 1.0
    values = jax.random.normal(key, dims, jnp.float32) * scale * factor_of
    return jnp.minimum(jnp.maximum(values, -limit), limit).astype(dtype)


def setup_inputs(seed: int = 0) -> dict:
    streams_of = jax.random.split(jax.random.key(seed), 22)
    return {
        "tokens": bell_draw(streams_of[0], (LATENTS, SEQ, D), 1.0, 6.0, ((0, 2), (1, 4))),
        "condition": bell_draw(streams_of[1], (LATENTS, D), 1.0, 6.0, (), jnp.float32),
        "cotangent": bell_draw(streams_of[2], (LATENTS, SEQ, D), 1.0, 6.0, ((0, 2), (1, 4))),
        "joint_weight": bell_draw(streams_of[3], (D, 3 * D), D ** -0.5, 0.1875, ((0, 8), (1, 4)), jnp.float32),
        "joint_moments": draw_joint_moments(jax.random.fold_in(streams_of[21], 71), 0),
        "output_weight": bell_draw(streams_of[5], (D, D), 4 ** -0.5, 3.0, ((0, 8), (1, 4)), jnp.float32),
        "output_moments": draw_output_moments(jax.random.fold_in(streams_of[21], 71), 0),
        "expand_weight": bell_draw(streams_of[7], (D, FF), D ** -0.5, 0.1875, ((0, 8), (1, 4)), jnp.float32),
        "expand_moments": draw_expand_moments(jax.random.fold_in(streams_of[21], 71), 0),
        "shrink_weight": bell_draw(streams_of[9], (D, FF), FF ** -0.5, 0.09375, ((0, 8), (1, 4)), jnp.float32),
        "shrink_moments": draw_shrink_moments(jax.random.fold_in(streams_of[21], 71), 0),
        "modulate_weight": bell_draw(streams_of[11], (D, 6 * D), D ** -0.5, 0.1875, ((0, 8), (1, 4)), jnp.float32),
        "modulate_moments": draw_modulate_moments(jax.random.fold_in(streams_of[21], 71), 0),
        "attention_bias": bell_draw(streams_of[13], (2 * D,), 0.5, 3.0, ((0, 4),), jnp.float32),
        "attention_moments": draw_attention_moments(jax.random.fold_in(streams_of[21], 71), 0),
        "hidden_bias": bell_draw(streams_of[15], (FF,), 0.5, 3.0, ((0, 4),), jnp.float32),
        "hidden_moments": draw_hidden_moments(jax.random.fold_in(streams_of[21], 71), 0),
        "condition_bias": bell_draw(streams_of[17], (6 * D,), 0.5, 3.0, ((0, 4),), jnp.float32),
        "condition_moments": draw_condition_moments(jax.random.fold_in(streams_of[21], 71), 0),
        "residual_bias": bell_draw(streams_of[19], (2, D), 0.5, 3.0, (), jnp.float32),
        "residual_moments": draw_residual_moments(jax.random.fold_in(streams_of[21], 71), 0),
    }


@jax.custom_vjp
def low(v):
    return lax.optimization_barrier(v.astype(jnp.bfloat16)).astype(jnp.float32)

@jax.custom_vjp
def low_back(v):
    return v

def low_keep(v):
    return (low(v), None)

def low_pass(kept, grad):
    return (grad,)

def back_keep(v):
    return (v, None)

def back_low(kept, grad):
    return (low(grad),)
low.defvjp(low_keep, low_pass)
low_back.defvjp(back_keep, back_low)
norm_epsilon = 1e-06
first_decay = 0.9
second_decay = 0.999
adam_epsilon = 1e-08
learning_rate = 0.05
weight_decay = 0.1
clip_limit = 1.0

def exact_dot(left_side, right_side):
    return jnp.dot(left_side, right_side, precision=lax.Precision.HIGHEST, preferred_element_type=jnp.float32)

def normalize(values):
    center = values - lax.optimization_barrier(jnp.mean(values, axis=-1, keepdims=True))
    return center * lax.rsqrt(lax.optimization_barrier(jnp.mean(center * center, axis=-1, keepdims=True)) + norm_epsilon)

def attend(queries, keys_all, values_all):
    block_rows = min(512, SEQ)
    score_scale = HEAD_DIM ** (-0.5)

    def one_block(query_block):
        scores = low_back(jnp.einsum('qhd,khd->hqk', query_block, keys_all, precision=lax.Precision.HIGHEST) * score_scale)
        row_peak = lax.optimization_barrier(jnp.max(scores, axis=-1, keepdims=True))
        raised = jnp.exp(scores - row_peak)
        probability = raised / lax.optimization_barrier(jnp.sum(raised, axis=-1, keepdims=True))
        return jnp.einsum('hqk,khd->qhd', low(probability), values_all, precision=lax.Precision.HIGHEST)
    outputs = lax.map(jax.checkpoint(one_block), queries.reshape(SEQ // block_rows, block_rows, HEADS, HEAD_DIM))
    return outputs.reshape(SEQ, HEADS, HEAD_DIM)

def one_latent(inputs, condition_row, params):
    joint, output, expand, shrink, modulate, attention_bias, hidden_bias, condition_bias, residual_bias = params
    condition_low = low(jax.nn.silu(condition_row))
    modulation = exact_dot(condition_low[None, :], modulate)[0] + condition_bias
    shift_first = modulation[0:D]
    scale_first = modulation[D:2 * D]
    gate_first = modulation[2 * D:3 * D]
    shift_second = modulation[3 * D:4 * D]
    scale_second = modulation[4 * D:5 * D]
    gate_second = modulation[5 * D:6 * D]
    hidden_first = low(normalize(inputs) * (1.0 + scale_first) + shift_first)
    bias_pairs = attention_bias.reshape(HEADS, 2, HEAD_DIM)
    joint_offset = jnp.stack([bias_pairs[:, 0], jnp.zeros_like(bias_pairs[:, 0]), bias_pairs[:, 1]], axis=1).reshape(3 * D)
    joint_out = low(low_back(exact_dot(hidden_first, joint)) + joint_offset).reshape(SEQ, HEADS, 3, HEAD_DIM)
    attended = attend(joint_out[:, :, 0, :], joint_out[:, :, 1, :], joint_out[:, :, 2, :])
    attended = low(low_back(attended)).reshape(SEQ, D)
    attn_value = low_back(exact_dot(attended, output.T)) + residual_bias[0]
    middle = inputs + gate_first * attn_value
    hidden_second = low(normalize(middle) * (1.0 + scale_second) + shift_second)
    expand_pre = low_back(exact_dot(hidden_second, expand)) + hidden_bias
    activated = low(jax.nn.gelu(expand_pre, approximate=True))
    shrink_value = low_back(exact_dot(activated, shrink.T)) + residual_bias[1]
    return middle + gate_second * shrink_value

def forward(tokens_float, condition_float, joint, output, expand, shrink, modulate, attention_bias, hidden_bias, condition_bias, residual_bias):
    params = (low(joint), low(output), low(expand), low(shrink), low(modulate), attention_bias, hidden_bias, condition_bias, residual_bias)

    def per_latent(pair):
        return one_latent(pair[0], pair[1], params)
    return lax.map(jax.checkpoint(per_latent), (tokens_float, condition_float))

def adam_step(master, moments, gradient, clip_factor, decay_rate):
    scaled = clip_factor * gradient
    first_moment = first_decay * moments[0] + (1.0 - first_decay) * scaled
    second_moment = second_decay * moments[1] * moments[1] + (1.0 - second_decay) * scaled * scaled
    first_hat = first_moment / (1.0 - first_decay ** ADAM_STEP)
    second_hat = second_moment / (1.0 - second_decay ** ADAM_STEP)
    updated = master - learning_rate * (first_hat / (jnp.sqrt(second_hat) + adam_epsilon) + decay_rate * master)
    return (updated, jnp.stack([first_moment, jnp.sqrt(second_moment)]))

def reference(tokens, condition, cotangent, joint_weight, joint_moments, output_weight, output_moments, expand_weight, expand_moments, shrink_weight, shrink_moments, modulate_weight, modulate_moments, attention_bias, attention_moments, hidden_bias, hidden_moments, condition_bias, condition_moments, residual_bias, residual_moments):
    masters = (joint_weight, output_weight, expand_weight, shrink_weight, modulate_weight, attention_bias, hidden_bias, condition_bias, residual_bias)
    moment_list = (joint_moments, output_moments, expand_moments, shrink_moments, modulate_moments, attention_moments, hidden_moments, condition_moments, residual_moments)
    result, pull = jax.vjp(forward, tokens.astype(jnp.float32), condition, *masters)
    grads = pull(cotangent.astype(jnp.float32))
    tokens_grad = grads[0]
    condition_grad = grads[1]
    param_grads = grads[2:]
    squares = jnp.float32(0.0)
    for gradient in param_grads:
        squares = squares + jnp.sum(gradient * gradient)
    grad_norm = jnp.sqrt(squares)
    clip_factor = jnp.minimum(1.0, clip_limit / (grad_norm + 1e-06))
    outcome = []
    for position in range(9):
        decay_rate = weight_decay if position < 5 else 0.0
        updated, averages = adam_step(masters[position], moment_list[position], param_grads[position], clip_factor, decay_rate)
        outcome.append(updated)
        outcome.append(averages)
    return (result.astype(jnp.bfloat16), tokens_grad, condition_grad, grad_norm, outcome[0], outcome[1], outcome[2], outcome[3], outcome[4], outcome[5], outcome[6], outcome[7], outcome[8], outcome[9], outcome[10], outcome[11], outcome[12], outcome[13], outcome[14], outcome[15], outcome[16], outcome[17])
```

```python
from functools import partial

import jax
import jax.numpy as jnp
from jax import lax
from jax.experimental import pallas as pl
from jax.experimental.pallas import tpu as pltpu
from jax.sharding import PartitionSpec as P

HEAD_DIM = 64
ADAM_STEP = 10
F32 = jnp.float32
BF16 = jnp.bfloat16
MESH = pl.DeviceIdType.MESH
DMA = pltpu.SemaphoreType.DMA

norm_epsilon = 1e-06
first_decay = 0.9
second_decay = 0.999
adam_epsilon = 1e-08
learning_rate = 0.05
weight_decay = 0.1
clip_limit = 1.0
GELU_SCALE = 0.7978845608028654
GELU_CUBE = 0.044715


def dot(a, b, ca, cb):
    return lax.dot_general(a, b, (((ca,), (cb,)), ((), ())), preferred_element_type=F32)


def aligned(start, size):
    return pl.ds(pl.multiple_of(start, size), size)


def greet(peers):
    barrier = pltpu.get_barrier_semaphore()
    for peer in peers:
        pl.semaphore_signal(barrier, inc=1, device_id=peer, device_id_type=MESH)
    pl.semaphore_wait(barrier, len(peers))


def remote(source, target, send_sem, recv_sem, peer):
    return pltpu.make_async_remote_copy(
        src_ref=source,
        dst_ref=target,
        send_sem=send_sem,
        recv_sem=recv_sem,
        device_id=peer,
        device_id_type=MESH,
    )


def vmem(count):
    return [pl.BlockSpec(memory_space=pltpu.VMEM)] * count


def shape(dims, dtype):
    return jax.ShapeDtypeStruct(dims, dtype)


def cost(micros, flops=0):
    return pl.CostEstimate(flops=flops, bytes_accessed=int(micros * 3.0e6), transcendentals=0)


def call(body, name, outs, scratch, ident, micros):
    def run(*args):
        return pl.pallas_call(
            body,
            out_shape=outs,
            in_specs=vmem(len(args)),
            out_specs=vmem(len(outs)),
            scratch_shapes=scratch,
            compiler_params=pltpu.CompilerParams(
                collective_id=ident, has_side_effects=True, vmem_limit_bytes=63000000
            ),
            cost_estimate=cost(micros),
            name=name,
        )(*args)

    return run


def transposed(block):
    return block.astype(F32).T.astype(BF16)


def row_of(mod, start, width, part):
    pieces = []
    for at in range(start, start + width, 128):
        pieces.append(mod[at // part, pl.ds((at % part) // 128, 1), :])
    return jnp.concatenate(pieces, axis=1)


def centred(values):
    center = values - jnp.mean(values, axis=-1, keepdims=True)
    inverse = lax.rsqrt(jnp.mean(center * center, axis=-1, keepdims=True) + norm_epsilon)
    return center * inverse, inverse


def normal_back(grad, normed, inverse):
    return inverse * (
        grad
        - jnp.mean(grad, axis=-1, keepdims=True)
        - normed * jnp.mean(grad * normed, axis=-1, keepdims=True)
    )


def tp_places():
    mine = lax.axis_index("tp")
    partner = mine + 1 - 2 * lax.rem(mine, 2)
    cross = lax.rem(mine + 2, 4)
    far = lax.rem(partner + 2, 4)
    return mine, partner, cross, far


def entry_body(
    nf, nc, tok, weight, cond, modw, cbias, offset,
    joint, hidden, weight_t, mod,
    wbuf, pbuf, pland, normed, zsend, zrecv, xsend, xrecv, psend, precv, msend, mrecv,
):
    f, c, t = lax.axis_index("fsdp"), lax.axis_index("ctx"), lax.axis_index("tp")
    group = nf * nc
    mine = f * nc + c
    rows, width = tok.shape
    part = modw.shape[1]
    strips = part // 128

    def place(offset_):
        other = lax.rem(mine + offset_, group)
        return other // nc, lax.rem(other, nc)

    peers = []
    for o in range(1, group):
        pf, pc = place(o)
        peers.append({"fsdp": pf, "ctx": pc})
    for o in range(1, 4):
        peers.append({"tp": lax.rem(t + o, 4)})
    partial_mod = dot(cond[...], modw[...].astype(BF16), 1, 0)
    for latent in range(nf):
        for k in range(strips):
            pbuf[latent, pl.ds(k, 1), :] = partial_mod[latent : latent + 1, 128 * k : 128 * k + 128]
    wbuf[mine] = weight[...].astype(BF16)
    greet(peers)
    pcopies = []
    for o in range(1, group):
        pf, pc = place(o)
        copy = remote(pbuf.at[pf], pland.at[mine], psend.at[o], precv.at[o], {"fsdp": pf, "ctx": pc})
        copy.start()
        pcopies.append(copy)
    zcopies, xcopies = [], []
    for o in range(1, nc):
        copy = remote(
            wbuf.at[mine], wbuf.at[mine], zsend.at[o], zrecv.at[o], {"ctx": lax.rem(c + o, nc)}
        )
        copy.start()
        zcopies.append(copy)

    def across(slot, o):
        for fo in range(1, nf):
            copy = remote(
                wbuf.at[slot], wbuf.at[slot], xsend.at[fo, o], xrecv.at[fo, o],
                {"fsdp": lax.rem(f + fo, nf)},
            )
            copy.start()
            xcopies.append(copy)

    across(mine, 0)
    pland[mine] = pbuf[f]
    step = 256
    for at in range(0, rows, step):
        normed[at : at + step, :] = centred(tok[at : at + step, :].astype(F32))[0]
    for o in (1, 3, 2) if nc == 4 else range(1, nc):
        zcopies[o - 1].wait_recv()
        across(f * nc + lax.rem(c - o + nc, nc), o)
    for copy in pcopies:
        copy.wait_recv()
    total = pland[0]
    for k in range(1, group):
        total = total + pland[k]
    mod[t] = total + cbias[...]
    mcopies = []
    for o in range(1, 4):
        copy = remote(
            mod.at[t], mod.at[t], msend.at[o], mrecv.at[o], {"tp": lax.rem(t + o, 4)}
        )
        copy.start()
        mcopies.append(copy)
    for copy in mcopies:
        copy.wait_recv()
    shift = row_of(mod, 0, width, part)
    scale = row_of(mod, width, width, part)
    for at in range(0, rows, step):
        hidden[at : at + step, :] = (
            normed[at : at + step, :] * (1.0 + scale) + shift
        ).astype(BF16)
    for copy in xcopies:
        copy.wait_recv()
    deep = weight.shape[0]
    for k in range(group):
        weight_t[:, k * deep : (k + 1) * deep] = transposed(wbuf[k])
    for at in range(0, rows, step):
        joint[:, at : at + step] = (
            dot(weight_t[...], hidden[at : at + step, :], 1, 1) + offset[...]
        ).astype(BF16)
    for copy in pcopies + zcopies + xcopies + mcopies:
        copy.wait_send()


def entry(nf, nc, tok, weight, cond, modw, cbias, offset):
    rows, width = tok.shape
    deep, columns = weight.shape
    group = nf * nc
    return call(
        partial(entry_body, nf, nc),
        "entry",
        (
            shape((columns, rows), BF16),
            shape((rows, width), BF16),
            shape((columns, width), BF16),
            shape((4,) + cbias.shape, F32),
        ),
        [
            pltpu.VMEM((group, deep, columns), BF16),
            pltpu.VMEM((nf,) + cbias.shape, F32),
            pltpu.VMEM((group,) + cbias.shape, F32),
            pltpu.VMEM((rows, width), F32),
            DMA((nc,)), DMA((nc,)), DMA((nf, nc)), DMA((nf, nc)),
            DMA((group,)), DMA((group,)), DMA((4,)), DMA((4,)),
        ],
        1,
        30,
    )(tok, weight, cond, modw, cbias, offset)


def attend_body(
    nc, x, att, qkv, out, lse,
    stage, land, keys, scores, send, recv, osend, orecv,
):
    c = lax.axis_index("ctx")
    rows = x.shape[1]
    total = rows * nc
    hd = HEAD_DIM
    bq, bk = scores.shape[1], 512
    per = rows // bq
    greet([{"ctx": lax.rem(c + o, nc)} for o in range(1, nc)])
    copies = []
    for o in range(1, nc):
        dst = lax.rem(c + o, nc)
        copy = remote(
            x.at[aligned(dst * 3 * hd, 3 * hd), :], qkv.at[:, aligned(c * rows, rows)],
            send.at[o], recv.at[o], {"ctx": dst},
        )
        copy.start()
        copies.append(copy)
    qkv[:, aligned(c * rows, rows)] = x[aligned(c * 3 * hd, 3 * hd), :]
    for copy in copies:
        copy.wait_recv()
    for at in range(0, total, 1024):
        keys[at : at + 1024, :] = transposed(qkv[hd : 2 * hd, at : at + 1024])

    def block(i, carry):
        o = 1 + i // per
        owner = lax.rem(c + o, nc)
        sub = lax.rem(i, per)
        where = aligned(owner * rows + sub * bq, bq)
        query = qkv[0:hd, where] * BF16(hd**-0.5)
        peak = None
        for at in range(0, total, bk):
            s = dot(keys[at : at + bk, :], query, 1, 0)
            scores[at : at + bk, :] = s
            high = jnp.max(s.reshape(bk // 8, 8, bq), axis=0)
            peak = high if peak is None else jnp.maximum(peak, high)
        peak = jnp.max(peak, axis=0, keepdims=True)
        acc, mass = None, None
        for at in range(0, total, bk):
            p = jnp.exp(scores[at : at + bk, :] - peak)
            low = jnp.sum(p.reshape(bk // 8, 8, bq), axis=0)
            mass = low if mass is None else mass + low
            term = dot(qkv[2 * hd : 3 * hd, at : at + bk], p.astype(BF16), 1, 0)
            acc = term if acc is None else acc + term
        mass = jnp.sum(mass, axis=0, keepdims=True)
        acc = acc * (1.0 / mass)
        out[:, where] = acc
        lse[:, where] = peak + jnp.log(mass)
        stage[owner, :, aligned(sub * bq, bq)] = acc.astype(BF16)

        @pl.when(jnp.logical_and(sub == per - 1, o < nc))
        def _():
            remote(
                stage.at[owner], land.at[c], osend.at[o], orecv.at[o], {"ctx": owner}
            ).start()

        return carry

    lax.fori_loop(0, per * nc, block, 0)
    land[c] = stage[c]
    for o in range(1, nc):
        dst = lax.rem(c + o, nc)
        copy = remote(stage.at[dst], land.at[c], osend.at[o], orecv.at[o], {"ctx": dst})
        copy.wait_recv()
        copy.wait_send()
    for k in range(nc):
        att[k * hd : (k + 1) * hd, :] = land[k]
    for copy in copies:
        copy.wait_send()


def attend(nc, x):
    rows = x.shape[1]
    total = rows * nc
    hd = HEAD_DIM
    bq = min(512, rows)
    return call(
        partial(attend_body, nc),
        "attend",
        (
            shape((nc * hd, rows), BF16),
            shape((3 * hd, total), BF16),
            shape((hd, total), F32),
            shape((1, total), F32),
        ),
        [
            pltpu.VMEM((nc, hd, rows), BF16),
            pltpu.VMEM((nc, hd, rows), BF16),
            pltpu.VMEM((total, hd), BF16),
            pltpu.VMEM((total, bq), F32),
            DMA((nc,)), DMA((nc,)), DMA((nc,)), DMA((nc,)),
        ],
        2,
        70,
    )(x)


def project_body(
    att, weight, tok, mod, bias,
    value, middle, hidden,
    sbuf, rbuf, send, recv, gsend, grecv,
):
    mine, partner, cross, far = tp_places()
    own = value.shape[0]
    width = tok.shape[1]
    part = mod.shape[1] * 128
    att_t = [None]

    def piece(at):
        return dot(
            att[:, aligned(at * own, own)].astype(F32).T.astype(BF16), weight[...], 1, 1
        )

    greet([{"tp": lax.rem(mine + o, 4)} for o in range(1, 4)])
    sbuf[0] = piece(far).astype(BF16)
    first = remote(sbuf.at[0], rbuf.at[0], send.at[0], recv.at[0], {"tp": partner})
    first.start()
    sbuf[1] = piece(partner).astype(BF16)
    second = remote(sbuf.at[1], rbuf.at[1], send.at[1], recv.at[1], {"tp": partner})
    second.start()
    crossing = piece(cross)
    first.wait_recv()
    sbuf[2] = (crossing + rbuf[0].astype(F32)).astype(BF16)
    third = remote(sbuf.at[2], rbuf.at[2], send.at[2], recv.at[2], {"tp": cross})
    third.start()
    held = piece(mine)
    second.wait_recv()
    held = held + rbuf[1].astype(F32) + bias[0:1, :]
    third.wait_recv()
    held = held + rbuf[2].astype(F32)
    value[...] = held
    gate = row_of(mod, 2 * width, width, part)
    shift = row_of(mod, 3 * width, width, part)
    scale = row_of(mod, 4 * width, width, part)
    mid = tok[aligned(mine * own, own), :].astype(F32) + gate * held
    middle[...] = mid
    hidden[mine] = (centred(mid)[0] * (1.0 + scale) + shift).astype(BF16)
    copies = gather_start(hidden, mine, partner, cross, gsend, grecv)
    gather_end(hidden, copies, mine, partner, cross, gsend, grecv)
    for copy in (first, second, third):
        copy.wait_send()


def gather_start(slots, mine, partner, cross, send, recv):
    over = remote(slots.at[mine], slots.at[mine], send.at[0], recv.at[0], {"tp": cross})
    over.start()
    near = remote(slots.at[mine], slots.at[mine], send.at[1], recv.at[1], {"tp": partner})
    near.start()
    return over, near


def gather_end(slots, copies, mine, partner, cross, send, recv):
    over, near = copies
    over.wait_recv()
    relay = remote(slots.at[cross], slots.at[cross], send.at[2], recv.at[2], {"tp": partner})
    relay.start()
    near.wait_recv()
    relay.wait_recv()
    for copy in (over, near, relay):
        copy.wait_send()


def project(att, weight, tok, mod, bias):
    rows, width = tok.shape
    own = rows // 4
    return call(
        project_body,
        "project",
        (shape((own, width), F32), shape((own, width), F32), shape((4, own, width), BF16)),
        [
            pltpu.VMEM((3, own, width), BF16),
            pltpu.VMEM((3, own, width), BF16),
            DMA((3,)), DMA((3,)), DMA((3,)), DMA((3,)),
        ],
        3,
        36,
    )(att, weight, tok, mod, bias)


def branch_body(
    hidden, cot, expand, shrink, hbias, mod, middle, value,
    attn_low, mid_grad, shrink_grad, expand_grad, stats, hstats, sh_cross, sh_own,
    gbuf, abuf, ebuf, sbuf, rbuf, shold, tsend, trecv, send, recv, gsend, grecv,
):
    mine, partner, cross, far = tp_places()
    own, width = middle.shape
    part = mod.shape[1] * 128
    gate_first = row_of(mod, 2 * width, width, part)
    scale_second = row_of(mod, 4 * width, width, part)
    gate_second = row_of(mod, 5 * width, width, part)
    greet([{"tp": lax.rem(mine + o, 4)} for o in range(1, 4)])
    column = None
    copies = []
    held = None
    for turn, at in enumerate((far, partner, cross, mine)):
        where = aligned(at * own, own)
        grad = gate_second * cot[where, :].astype(F32)
        low = grad.astype(BF16)
        gbuf[where, :] = low
        if turn == 3:
            stats[3:4, :] = jnp.sum(grad, axis=0, keepdims=True)
        u = dot(hidden[at], expand[...], 1, 0) + hbias[...]
        squared = u * u
        th = jnp.tanh(GELU_SCALE * (u + GELU_CUBE * squared * u))
        act = (0.5 * u * (1.0 + th)).astype(BF16)
        abuf[where, :] = act
        slope = 0.5 * (1.0 + th) + 0.5 * u * (1.0 - th * th) * (
            GELU_SCALE * (1.0 + 3.0 * GELU_CUBE * squared)
        )
        pull = dot(low, shrink[...], 1, 0) * slope
        tally = jnp.sum(pull, axis=0, keepdims=True)
        column = tally if column is None else column + tally
        pull = pull.astype(BF16)
        ebuf[where, :] = pull
        back = dot(pull, expand[...], 1, 1)
        forth = dot(act, shrink[...], 1, 1)
        if turn < 2:
            sbuf[turn] = back.astype(BF16)
            copy = remote(sbuf.at[turn], rbuf.at[turn], send.at[turn], recv.at[turn], {"tp": partner})
            copy.start()
            copies.append(copy)
            shold[turn] = forth.astype(BF16)
            copy = remote(
                shold.at[turn], shold.at[2 + turn], tsend.at[turn], trecv.at[turn], {"tp": partner}
            )
            copy.start()
            copies.append(copy)
        elif turn == 2:
            copies[0].wait_recv()
            sbuf[2] = (back + rbuf[0].astype(F32)).astype(BF16)
            third = remote(sbuf.at[2], rbuf.at[2], send.at[2], recv.at[2], {"tp": cross})
            third.start()
            copies[1].wait_recv()
            sh_cross[...] = (forth + shold[2].astype(F32)).astype(BF16)
        else:
            copies[2].wait_recv()
            held = back + rbuf[1].astype(F32)
            copies[3].wait_recv()
            sh_own[...] = forth + shold[3].astype(F32)
    hstats[...] = column
    step = 256
    for at in range(0, width, step):
        shrink_grad[at : at + step, :] = dot(
            gbuf[:, at : at + step], abuf[...], 0, 0
        ).astype(BF16)
    third.wait_recv()
    grad_in = held + rbuf[2].astype(F32)
    normed, inverse = centred(middle[...])
    stats[0:1, :] = jnp.sum(grad_in, axis=0, keepdims=True)
    stats[1:2, :] = jnp.sum(grad_in * normed, axis=0, keepdims=True)
    mgrad = cot[aligned(mine * own, own), :].astype(F32) + normal_back(
        grad_in * (1.0 + scale_second), normed, inverse
    )
    mid_grad[...] = mgrad
    agrad = gate_first * mgrad
    attn_low[mine] = agrad.astype(BF16)
    gathers = gather_start(attn_low, mine, partner, cross, gsend, grecv)
    stats[2:3, :] = jnp.sum(mgrad * value[...], axis=0, keepdims=True)
    stats[4:5, :] = jnp.sum(agrad, axis=0, keepdims=True)
    stats[5:8, :] = jnp.zeros((3, width), F32)
    flat = hidden.shape[0] * own
    for at in range(0, width, step):
        expand_grad[at : at + step, :] = dot(
            hidden[:, :, at : at + step].reshape(flat, step), ebuf[...], 0, 0
        ).astype(BF16)
    gather_end(attn_low, gathers, mine, partner, cross, gsend, grecv)
    for copy in copies + [third]:
        copy.wait_send()


def branch(hidden, cot, expand, shrink, hbias, mod, middle, value):
    rows, width = cot.shape
    own = rows // 4
    units = expand.shape[1]
    return call(
        branch_body,
        "branch",
        (
            shape((4, own, width), BF16),
            shape((own, width), F32),
            shape((width, units), BF16),
            shape((width, units), BF16),
            shape((8, width), F32),
            shape((1, units), F32),
            shape((own, width), BF16),
            shape((own, width), F32),
        ),
        [
            pltpu.VMEM((rows, width), BF16),
            pltpu.VMEM((rows, units), BF16),
            pltpu.VMEM((rows, units), BF16),
            pltpu.VMEM((3, own, width), BF16),
            pltpu.VMEM((3, own, width), BF16),
            pltpu.VMEM((4, own, width), BF16),
            DMA((2,)), DMA((2,)), DMA((3,)), DMA((3,)), DMA((3,)), DMA((3,)),
        ],
        4,
        45,
    )(hidden, cot, expand, shrink, hbias, mod, middle, value)


def retreat_body(
    nc, attn_low, weight, att, qkv, out, lse, sh_cross, sh_own, middle, cot, mod, bias,
    joint_grad, weight_grad, bias_grad, mixed, gate_grad,
    dout, dost, keys, vals, dq, stage, rland, wt, delta, send, recv, jsend, jrecv,
    csend, crecv, gsend, grecv,
):
    c = lax.axis_index("ctx")
    mine, partner, cross, far = tp_places()
    own, width = middle.shape
    rows = att.shape[1]
    total = rows * nc
    hd = HEAD_DIM
    bk = bq = 512
    per = rows // bk
    part = mod.shape[1] * 128
    wt[...] = transposed(weight[...])
    low = attn_low[...].reshape(rows, width)
    dost[...] = dot(wt[...], low, 1, 1).astype(BF16)
    greet(
        [{"ctx": lax.rem(c + o, nc)} for o in range(1, nc)]
        + [{"tp": lax.rem(mine + o, 4)} for o in range(1, 4)]
    )
    copies = []
    for o in range(1, nc):
        dst = lax.rem(c + o, nc)
        copy = remote(
            dost.at[aligned(dst * hd, hd), :], dout.at[:, aligned(c * rows, rows)],
            send.at[o], recv.at[o], {"ctx": dst},
        )
        copy.start()
        copies.append(copy)
    crossing = remote(sh_cross, rland, csend, crecv, {"tp": cross})
    crossing.start()
    dout[:, aligned(c * rows, rows)] = dost[aligned(c * hd, hd), :]
    weight_grad[...] = dot(att[...], low, 1, 0).T.astype(BF16)
    for at in range(0, total, 1024):
        keys[at : at + 1024, :] = transposed(qkv[hd : 2 * hd, at : at + 1024])
        vals[at : at + 1024, :] = transposed(qkv[2 * hd : 3 * hd, at : at + 1024])
    dq[...] = jnp.zeros_like(dq)
    for copy in copies:
        copy.wait_recv()
    for at in range(0, total, 1024):
        delta[:, at : at + 1024] = jnp.sum(
            dout[:, at : at + 1024].astype(F32) * out[:, at : at + 1024], axis=0, keepdims=True
        )
    vsum_start = jnp.zeros((hd, 1), F32)

    def block(i, vsum):
        o = 1 + i // per
        owner = lax.rem(c + o, nc)
        sub = lax.rem(i, per)
        where = aligned(owner * rows + sub * bk, bk)
        key, val, key_t = keys[where, :], vals[where, :], qkv[hd : 2 * hd, where]
        dk, dv = None, None
        for at in range(0, total, bq):
            query = qkv[0:hd, at : at + bq] * BF16(hd**-0.5)
            grad = dout[:, at : at + bq]
            p = jnp.exp(dot(key, query, 1, 0) - lse[:, at : at + bq])
            ds = (p * (dot(val, grad, 1, 0) - delta[:, at : at + bq])).astype(BF16)
            tv = dot(grad, p.astype(BF16), 1, 1)
            tk = dot(query, ds, 1, 1)
            dv = tv if dv is None else dv + tv
            dk = tk if dk is None else dk + tk
            dq[:, at : at + bq] += dot(key_t, ds, 1, 0)
        put = aligned(sub * bk, bk)
        stage[owner, hd : 2 * hd, put] = dk.astype(BF16)
        stage[owner, 2 * hd : 3 * hd, put] = dv.astype(BF16)

        @pl.when(jnp.logical_and(sub == per - 1, o < nc))
        def _():
            remote(
                stage.at[owner, pl.ds(hd, 2 * hd), :], joint_grad.at[c, pl.ds(hd, 2 * hd), :],
                jsend.at[0, o], jrecv.at[0, o], {"ctx": owner},
            ).start()

        @pl.when(i == 2)
        def _():
            crossing.wait_recv()
            value = sh_own[...] + rland[...].astype(F32) + bias[1:2, :]
            gate = row_of(mod, 5 * width, width, part)
            mixed[mine] = (middle[...] + gate * value).astype(BF16)
            gather_start(mixed, mine, partner, cross, gsend, grecv)
            gate_grad[...] = jnp.sum(
                cot[aligned(mine * own, own), :].astype(F32) * value, axis=0, keepdims=True
            )

        return vsum + jnp.sum(dv, axis=1, keepdims=True)

    vsum = lax.fori_loop(0, per * nc, block, vsum_start)
    qsum = jnp.zeros((hd, 1), F32)
    dqs = []
    for o in range(1, nc + 1):
        owner = lax.rem(c + o, nc)
        piece = dq[:, aligned(owner * rows, rows)] * (hd**-0.5)
        qsum = qsum + jnp.sum(piece, axis=1, keepdims=True)
        stage[owner, 0:hd, :] = piece.astype(BF16)
        if o < nc:
            copy = remote(
                stage.at[owner, pl.ds(0, hd), :], joint_grad.at[c, pl.ds(0, hd), :],
                jsend.at[1, o], jrecv.at[1, o], {"ctx": owner},
            )
            copy.start()
            dqs.append(copy)
    joint_grad[c] = stage[c]
    bias_grad[0:hd, :] = jnp.broadcast_to(qsum, (hd, 128))
    bias_grad[hd : 2 * hd, :] = jnp.broadcast_to(vsum, (hd, 128))
    over = remote(mixed.at[mine], mixed.at[mine], gsend.at[0], grecv.at[0], {"tp": cross})
    near = remote(mixed.at[mine], mixed.at[mine], gsend.at[1], grecv.at[1], {"tp": partner})
    gather_end(mixed, (over, near), mine, partner, cross, gsend, grecv)
    for o in range(1, nc):
        dst = lax.rem(c + o, nc)
        copy = remote(
            stage.at[dst, pl.ds(hd, 2 * hd), :], joint_grad.at[c, pl.ds(hd, 2 * hd), :],
            jsend.at[0, o], jrecv.at[0, o], {"ctx": dst},
        )
        copy.wait_recv()
        copy.wait_send()
        dqs[o - 1].wait_recv()
        dqs[o - 1].wait_send()
    for copy in copies + [crossing]:
        copy.wait_send()


def retreat(nc, attn_low, weight, att, qkv, out, lse, sh_cross, sh_own, middle, cot, mod, bias):
    rows, width = cot.shape
    own = rows // 4
    total = rows * nc
    hd = HEAD_DIM
    return call(
        partial(retreat_body, nc),
        "retreat",
        (
            shape((nc, 3 * hd, rows), BF16),
            shape((width, nc * hd), BF16),
            shape((2 * hd, 128), F32),
            shape((4, own, width), BF16),
            shape((1, width), F32),
        ),
        [
            pltpu.VMEM((hd, total), BF16),
            pltpu.VMEM((nc * hd, rows), BF16),
            pltpu.VMEM((total, hd), BF16),
            pltpu.VMEM((total, hd), BF16),
            pltpu.VMEM((hd, total), F32),
            pltpu.VMEM((nc, 3 * hd, rows), BF16),
            pltpu.VMEM((own, width), BF16),
            pltpu.VMEM((nc * hd, width), BF16),
            pltpu.VMEM((1, total), F32),
            DMA((nc,)), DMA((nc,)), DMA((2, nc)), DMA((2, nc)),
            DMA, DMA, DMA((3,)), DMA((3,)),
        ],
        5,
        100,
    )(attn_low, weight, att, qkv, out, lse, sh_cross, sh_own, middle, cot, mod, bias)


def leave_body(
    joint_grad, weight_t, hidden, tok, mid_grad, mod,
    weight_grad, tokens_grad, stats,
    sbuf, rbuf, send, recv, gsend, grecv,
):
    mine, partner, cross, far = tp_places()
    own, width = mid_grad.shape
    part = mod.shape[1] * 128
    columns = weight_t.shape[0]

    def piece(at):
        block = joint_grad[:, :, aligned(at * own, own)].reshape(columns, own)
        return dot(block.astype(F32).T.astype(BF16), weight_t[...], 1, 0)

    greet([{"tp": lax.rem(mine + o, 4)} for o in range(1, 4)])
    sbuf[0] = piece(far).astype(BF16)
    first = remote(sbuf.at[0], rbuf.at[0], send.at[0], recv.at[0], {"tp": partner})
    first.start()
    sbuf[1] = piece(partner).astype(BF16)
    second = remote(sbuf.at[1], rbuf.at[1], send.at[1], recv.at[1], {"tp": partner})
    second.start()
    crossing = piece(cross)
    first.wait_recv()
    sbuf[2] = (crossing + rbuf[0].astype(F32)).astype(BF16)
    third = remote(sbuf.at[2], rbuf.at[2], send.at[2], recv.at[2], {"tp": cross})
    third.start()
    held = piece(mine)
    second.wait_recv()
    held = held + rbuf[1].astype(F32)
    normed, inverse = centred(tok[aligned(mine * own, own), :].astype(F32))
    flat = joint_grad[...].reshape(columns, tok.shape[0])
    step = 256
    for at in range(0, width, step):
        weight_grad[at : at + step, :] = dot(flat, hidden[:, at : at + step], 1, 0).T.astype(BF16)
    third.wait_recv()
    grad_in = held + rbuf[2].astype(F32)
    scale = row_of(mod, width, width, part)
    stats[0:1, :] = jnp.sum(grad_in, axis=0, keepdims=True)
    stats[1:2, :] = jnp.sum(grad_in * normed, axis=0, keepdims=True)
    stats[2:8, :] = jnp.zeros((6, width), F32)
    tokens_grad[mine] = (
        mid_grad[...] + normal_back(grad_in * (1.0 + scale), normed, inverse)
    ).astype(BF16)
    copies = gather_start(tokens_grad, mine, partner, cross, gsend, grecv)
    gather_end(tokens_grad, copies, mine, partner, cross, gsend, grecv)
    for copy in (first, second, third):
        copy.wait_send()


def leave(joint_grad, weight_t, hidden, tok, mid_grad, mod):
    rows, width = tok.shape
    own = rows // 4
    return call(
        leave_body,
        "leave",
        (
            shape((width, weight_t.shape[0]), BF16),
            shape((4, own, width), BF16),
            shape((8, width), F32),
        ),
        [
            pltpu.VMEM((3, own, width), BF16),
            pltpu.VMEM((3, own, width), BF16),
            DMA((3,)), DMA((3,)), DMA((3,)), DMA((3,)),
        ],
        6,
        36,
    )(joint_grad, weight_t, hidden, tok, mid_grad, mod)


def tally_body(nf, nc, pieces, gathered, land, total, asend, arecv, bsend, brecv):
    f, c, t = lax.axis_index("fsdp"), lax.axis_index("ctx"), lax.axis_index("tp")
    inner = nc * 4
    group = nf * nc
    here = c * 4 + t
    mine = f * nc + c
    peers = []
    for o in range(1, inner):
        other = lax.rem(here + o, inner)
        peers.append({"ctx": other // 4, "tp": lax.rem(other, 4)})
    outer = []
    for o in range(1, group):
        other = lax.rem(mine + o, group)
        outer.append({"fsdp": other // nc, "ctx": lax.rem(other, nc)})
    greet(peers + outer)
    copies = []
    for o in range(1, inner):
        other = lax.rem(here + o, inner)
        copy = remote(pieces.at[other], land.at[here], asend.at[o], arecv.at[o], peers[o - 1])
        copy.start()
        copies.append(copy)
    land[here] = pieces[here]
    for copy in copies:
        copy.wait_recv()
    acc = land[0]
    for k in range(1, inner):
        acc = acc + land[k]
    total[...] = acc
    gathered[mine] = acc
    second = []
    for o in range(1, group):
        copy = remote(total, gathered.at[mine], bsend.at[o], brecv.at[o], outer[o - 1])
        copy.start()
        second.append(copy)
    for copy in second:
        copy.wait_recv()
    for copy in copies + second:
        copy.wait_send()


def tally(nf, nc, pieces):
    inner, high, lanes = pieces.shape
    group = nf * nc
    return call(
        partial(tally_body, nf, nc),
        "tally",
        (shape((group, high, lanes), F32),),
        [
            pltpu.VMEM((inner, high, lanes), F32),
            pltpu.VMEM((high, lanes), F32),
            DMA((inner,)), DMA((inner,)), DMA((group,)), DMA((group,)),
        ],
        7,
        12,
    )(pieces)[0]


def finish_body(nf, nc, piece, gathered, land, total, asend, arecv, bsend, brecv):
    f, c, t = lax.axis_index("fsdp"), lax.axis_index("ctx"), lax.axis_index("tp")
    group = nf * nc
    mine = f * nc + c
    peers = [{"tp": lax.rem(t + o, 4)} for o in range(1, 4)]
    outer = []
    for o in range(1, group):
        other = lax.rem(mine + o, group)
        outer.append({"fsdp": other // nc, "ctx": lax.rem(other, nc)})
    greet(peers + outer)
    copies = []
    for o in range(1, 4):
        copy = remote(piece, land.at[t], asend.at[o], arecv.at[o], peers[o - 1])
        copy.start()
        copies.append(copy)
    land[t] = piece[...]
    for copy in copies:
        copy.wait_recv()
    acc = land[0] + land[1] + land[2] + land[3]
    total[...] = acc
    gathered[mine] = acc
    second = []
    for o in range(1, group):
        copy = remote(total, gathered.at[mine], bsend.at[o], brecv.at[o], outer[o - 1])
        copy.start()
        second.append(copy)
    for copy in second:
        copy.wait_recv()
    for copy in copies + second:
        copy.wait_send()


def finish(nf, nc, piece):
    high, lanes = piece.shape
    group = nf * nc
    return call(
        partial(finish_body, nf, nc),
        "finish",
        (shape((group, high, lanes), F32),),
        [
            pltpu.VMEM((4, high, lanes), F32),
            pltpu.VMEM((high, lanes), F32),
            DMA((4,)), DMA((4,)), DMA((group,)), DMA((group,)),
        ],
        8,
        10,
    )(piece)[0]


def adam_step(master, moments, gradient, clip_factor, decay_rate):
    scaled = clip_factor * gradient
    first_moment = first_decay * moments[0] + (1.0 - first_decay) * scaled
    second_moment = second_decay * moments[1] * moments[1] + (1.0 - second_decay) * scaled * scaled
    first_hat = first_moment / (1.0 - first_decay**ADAM_STEP)
    second_hat = second_moment / (1.0 - second_decay**ADAM_STEP)
    updated = master - learning_rate * (
        first_hat / (jnp.sqrt(second_hat) + adam_epsilon) + decay_rate * master
    )
    return (updated, jnp.stack([first_moment, jnp.sqrt(second_moment)]))


def local(
    nf,
    nc,
    tokens,
    condition,
    cotangent,
    joint_weight,
    joint_moments,
    output_weight,
    output_moments,
    expand_weight,
    expand_moments,
    shrink_weight,
    shrink_moments,
    modulate_weight,
    modulate_moments,
    attention_bias,
    attention_moments,
    hidden_bias,
    hidden_moments,
    condition_bias,
    condition_moments,
    residual_bias,
    residual_moments,
):
    latent_count, rows, width = tokens.shape
    heads = joint_weight.shape[1] // (3 * HEAD_DIM)
    assert latent_count == 1 and heads == nc and lax.axis_size("tp") == 4
    f, c, t = lax.axis_index("fsdp"), lax.axis_index("ctx"), lax.axis_index("tp")
    mine = f * nc + c
    deep, part = modulate_weight.shape
    units = expand_weight.shape[1]
    tok, cot = tokens[0], cotangent[0]

    def gather(weight):
        return lax.all_gather(weight.astype(BF16), ("fsdp", "ctx"), axis=0, tiled=True)

    output_full, expand_full, shrink_full = (
        gather(output_weight), gather(expand_weight), gather(shrink_weight)
    )

    condition_act, silu_pull = jax.vjp(jax.nn.silu, condition)
    condition_low = condition_act.astype(BF16)
    condition_here = lax.dynamic_slice_in_dim(condition_low, mine * deep, deep, 1)
    condition_pad = jnp.pad(condition_here, ((0, 16 - nf), (0, 0)))
    strips = part // 128
    high = -(-strips // 8) * 8
    bias_strips = jnp.pad(condition_bias.reshape(strips, 128), ((0, high - strips), (0, 0)))
    bias_pairs = attention_bias.reshape(heads, 2, HEAD_DIM)
    offset = jnp.stack(
        [bias_pairs[:, 0], jnp.zeros_like(bias_pairs[:, 0]), bias_pairs[:, 1]], axis=1
    ).reshape(-1, 1)
    joint_t, hidden_first, joint_full_t, mod = entry(
        nf, nc, tok, joint_weight, condition_pad, modulate_weight, bias_strips, offset
    )
    mod = mod[:, :strips]
    att_t, qkv, out, lse = attend(nc, joint_t)
    value, middle, hidden_second = project(att_t, output_full, tok, mod, residual_bias)
    (
        attn_low, mid_grad, shrink_grad, expand_grad, stats_second, hidden_stats, sh_cross, sh_own,
    ) = branch(
        hidden_second, cot, expand_full, shrink_full, hidden_bias[None, :], mod, middle, value
    )

    def scatter(grad):
        return lax.psum_scatter(
            grad, ("fsdp", "ctx"), scatter_dimension=0, tiled=True
        ).astype(F32)

    shrink_sum, expand_sum = scatter(shrink_grad), scatter(expand_grad)
    joint_grad, output_grad, head_bias, mixed, gate_second_grad = retreat(
        nc, attn_low, output_full, att_t, qkv, out, lse, sh_cross, sh_own, middle, cot, mod,
        residual_bias,
    )
    output_sum = scatter(output_grad)
    joint_weight_grad, tokens_grad, stats_first = leave(
        joint_grad, joint_full_t, hidden_first, tok, mid_grad, mod
    )
    joint_sum = scatter(joint_weight_grad)

    stats = jnp.stack(
        [
            stats_first[0], stats_first[1], stats_second[2],
            stats_second[0], stats_second[1], gate_second_grad[0],
        ]
    ).reshape(4, nc, part // nc // 128, 128)
    stats = stats.transpose(1, 0, 2, 3).reshape(nc * 4, -1, 128)
    residual = jnp.stack([stats_second[4], stats_second[3]]).reshape(nc, -1, 128)
    residual = jnp.repeat(residual, 4, axis=0)
    same = (jnp.arange(4) == t).astype(F32)[None, :, None, None]
    hidden_piece = (hidden_stats.reshape(nc, 1, -1, 128) * same).reshape(nc * 4, -1, 128)
    exact = (jnp.arange(nc * 4) == c * 4 + t).astype(F32)[:, None, None]
    head_piece = head_bias[:, 0].reshape(1, -1, 128) * exact
    pieces = jnp.concatenate([stats, residual, hidden_piece, head_piece], axis=1)
    counts = [stats.shape[1], residual.shape[1], hidden_piece.shape[1], head_piece.shape[1]]
    used = sum(counts)
    pieces = jnp.pad(pieces, ((0, 0), (0, -(-used // 8) * 8 - used), (0, 0)))
    sums = tally(nf, nc, pieces).reshape(nf, nc, -1, 128)
    edge = [0]
    for count in counts:
        edge.append(edge[-1] + count)
    modulation_grad = sums[:, :, edge[0] : edge[1]].reshape(nf, part)
    residual_sum = jnp.sum(sums[:, :, edge[1] : edge[2]], axis=0).reshape(2, width)
    hidden_sum = jnp.sum(sums[:, :, edge[2] : edge[3]], axis=0).reshape(units)
    attention_sum = jnp.sum(sums[:, :, edge[3] : edge[4]], axis=0).reshape(-1)
    condition_bias_sum = jnp.sum(modulation_grad, axis=0)
    low_rows = condition_here.astype(F32)
    if nf <= 4:
        modulate_sum = sum(
            low_rows[k][:, None] * modulation_grad[k][None, :] for k in range(nf)
        )
        wide = modulate_weight.astype(BF16).astype(F32)
        condition_part = jnp.stack(
            [jnp.sum(wide * modulation_grad[k][None, :], axis=1) for k in range(nf)]
        )
    else:
        modulate_sum = lax.dot_general(
            low_rows, modulation_grad, (((0,), (0,)), ((), ())),
            precision=lax.Precision.HIGHEST, preferred_element_type=F32,
        )
        condition_part = lax.dot_general(
            modulation_grad, modulate_weight.astype(BF16).astype(F32), (((1,), (1,)), ((), ())),
            precision=lax.Precision.HIGHEST, preferred_element_type=F32,
        )
    lead_flag = (mine == 0).astype(F32)
    tensor_lead = (t == 0).astype(F32)
    weight_squares = (
        jnp.sum(joint_sum * joint_sum)
        + jnp.sum(output_sum * output_sum)
        + jnp.sum(expand_sum * expand_sum)
        + jnp.sum(shrink_sum * shrink_sum)
        + jnp.sum(modulate_sum * modulate_sum)
    )
    bias_squares = (
        jnp.sum(attention_sum * attention_sum)
        + jnp.sum(hidden_sum * hidden_sum)
        + jnp.sum(condition_bias_sum * condition_bias_sum)
        + tensor_lead * jnp.sum(residual_sum * residual_sum)
    )
    squares_part = weight_squares + lead_flag * bias_squares
    tall = -(-(nf + 1) // 8) * 8
    lanes = max(128, deep)
    piece = jnp.concatenate(
        [
            jnp.pad(condition_part, ((0, 0), (0, lanes - deep))),
            jnp.full((1, lanes), squares_part),
            jnp.zeros((tall - nf - 1, lanes), F32),
        ]
    )
    done = finish(nf, nc, piece)
    squares = jnp.sum(done[:, nf, 0])
    grad_norm = jnp.sqrt(squares)
    clip_factor = jnp.minimum(1.0, clip_limit / (grad_norm + 1e-06))
    condition_act_grad = lax.dynamic_slice_in_dim(done, f, 1, 1)[:, 0, :deep].reshape(1, -1)
    condition_all = jnp.broadcast_to(condition_act_grad, condition.shape)
    condition_grad = lax.dynamic_slice_in_dim(silu_pull(condition_all)[0], f, 1, 0)

    joint_updated, joint_averages = adam_step(
        joint_weight, joint_moments, joint_sum, clip_factor, weight_decay
    )
    output_updated, output_averages = adam_step(
        output_weight, output_moments, output_sum, clip_factor, weight_decay
    )
    expand_updated, expand_averages = adam_step(
        expand_weight, expand_moments, expand_sum, clip_factor, weight_decay
    )
    shrink_updated, shrink_averages = adam_step(
        shrink_weight, shrink_moments, shrink_sum, clip_factor, weight_decay
    )
    modulate_updated, modulate_averages = adam_step(
        modulate_weight, modulate_moments, modulate_sum, clip_factor, weight_decay
    )
    attention_updated, attention_averages = adam_step(
        attention_bias, attention_moments, attention_sum, clip_factor, 0.0
    )
    hidden_updated, hidden_averages = adam_step(
        hidden_bias, hidden_moments, hidden_sum, clip_factor, 0.0
    )
    condition_updated, condition_averages = adam_step(
        condition_bias, condition_moments, condition_bias_sum, clip_factor, 0.0
    )
    residual_updated, residual_averages = adam_step(
        residual_bias, residual_moments, residual_sum, clip_factor, 0.0
    )
    return (
        mixed.reshape(1, rows, width),
        tokens_grad.reshape(1, rows, width).astype(F32),
        condition_grad,
        grad_norm,
        joint_updated,
        joint_averages,
        output_updated,
        output_averages,
        expand_updated,
        expand_averages,
        shrink_updated,
        shrink_averages,
        modulate_updated,
        modulate_averages,
        attention_updated,
        attention_averages,
        hidden_updated,
        hidden_averages,
        condition_updated,
        condition_averages,
        residual_updated,
        residual_averages,
    )


def solution(mesh):
    rows = P(("fsdp", "ctx"), "tp")
    pair = P(None, ("fsdp", "ctx"), "tp")
    tokens = P("fsdp", "ctx", None)
    small = (P("tp"), P(None, "tp"))
    return jax.shard_map(
        partial(local, mesh.shape["fsdp"], mesh.shape["ctx"]),
        mesh=mesh,
        in_specs=(tokens, P(), tokens) + (rows, pair) * 5 + small * 3 + (P(), P()),
        out_specs=(tokens, tokens, P("fsdp", None), P())
        + (rows, pair) * 5
        + small * 3
        + (P(), P()),
        check_vma=False,
    )
```

```python
from functools import partial

import jax
import jax.numpy as jnp
from jax import lax
from jax.experimental import pallas as pl
from jax.experimental.pallas import tpu as pltpu
from jax.sharding import PartitionSpec as P

HEAD_DIM = 64
ADAM_STEP = 10
F32 = jnp.float32
BF16 = jnp.bfloat16
MESH = pl.DeviceIdType.MESH
DMA = pltpu.SemaphoreType.DMA

norm_epsilon = 1e-06
first_decay = 0.9
second_decay = 0.999
adam_epsilon = 1e-08
learning_rate = 0.05
weight_decay = 0.1
clip_limit = 1.0
GELU_SCALE = 0.7978845608028654
GELU_CUBE = 0.044715


def dot(a, b, ca, cb):
    return lax.dot_general(a, b, (((ca,), (cb,)), ((), ())), preferred_element_type=F32)


def aligned(start, size):
    return pl.ds(pl.multiple_of(start, size), size)


def greet(peers):
    barrier = pltpu.get_barrier_semaphore()
    for peer in peers:
        pl.semaphore_signal(barrier, inc=1, device_id=peer, device_id_type=MESH)
    pl.semaphore_wait(barrier, len(peers))


def remote(source, target, send_sem, recv_sem, peer):
    return pltpu.make_async_remote_copy(
        src_ref=source,
        dst_ref=target,
        send_sem=send_sem,
        recv_sem=recv_sem,
        device_id=peer,
        device_id_type=MESH,
    )


def vmem(count):
    return [pl.BlockSpec(memory_space=pltpu.VMEM)] * count


def shape(dims, dtype):
    return jax.ShapeDtypeStruct(dims, dtype)


def cost(micros, flops=0):
    return pl.CostEstimate(flops=flops, bytes_accessed=int(micros * 3.0e6), transcendentals=0)


def call(body, name, outs, scratch, ident, micros):
    def run(*args):
        return pl.pallas_call(
            body,
            out_shape=outs,
            in_specs=vmem(len(args)),
            out_specs=vmem(len(outs)),
            scratch_shapes=scratch,
            compiler_params=pltpu.CompilerParams(
                collective_id=ident, has_side_effects=True, vmem_limit_bytes=63000000
            ),
            cost_estimate=cost(micros),
            name=name,
        )(*args)

    return run


def transposed(block):
    return block.astype(F32).T.astype(BF16)


def row_of(mod, start, width, part):
    pieces = []
    for at in range(start, start + width, 128):
        pieces.append(mod[at // part, pl.ds((at % part) // 128, 1), :])
    return jnp.concatenate(pieces, axis=1)


def centred(values):
    center = values - jnp.mean(values, axis=-1, keepdims=True)
    inverse = lax.rsqrt(jnp.mean(center * center, axis=-1, keepdims=True) + norm_epsilon)
    return center * inverse, inverse


def normal_back(grad, normed, inverse):
    return inverse * (
        grad
        - jnp.mean(grad, axis=-1, keepdims=True)
        - normed * jnp.mean(grad * normed, axis=-1, keepdims=True)
    )


def spread_own(buf, nf, nc, zs, zr, xs, xr, lanes=None):
    f, c = lax.axis_index("fsdp"), lax.axis_index("ctx")
    slot = f * nc + c
    view = buf.at[slot] if lanes is None else buf.at[slot, :, lanes]
    copies = [
        remote(view, view, zs.at[o], zr.at[o], {"ctx": lax.rem(c + o, nc)}) for o in (1, 3, 2)
    ]
    return copies, spread_across(buf, nf, nc, 0, xs, xr, lanes)


def spread_across(buf, nf, nc, o, xs, xr, lanes=None):
    f, c = lax.axis_index("fsdp"), lax.axis_index("ctx")
    slot = f * nc + lax.rem(c - o + nc, nc)
    view = buf.at[slot] if lanes is None else buf.at[slot, :, lanes]
    return [
        remote(view, view, xs.at[fo, o], xr.at[fo, o], {"fsdp": lax.rem(f + fo, nf)})
        for fo in range(1, nf)
    ]


def spread_start(*args):
    along, across = spread_own(*args)
    for copy in along + across:
        copy.start()


def spread_relay(buf, nf, nc, zs, zr, xs, xr, lanes=None):
    along, _ = spread_own(buf, nf, nc, zs, zr, xs, xr, lanes)
    for o, copy in zip((1, 3, 2), along):
        copy.wait_recv()
        for relay in spread_across(buf, nf, nc, o, xs, xr, lanes):
            relay.start()


def spread_end(buf, nf, nc, zs, zr, xs, xr, lanes=None):
    along, across = spread_own(buf, nf, nc, zs, zr, xs, xr, lanes)
    for o in (1, 3, 2):
        across = across + spread_across(buf, nf, nc, o, xs, xr, lanes)
    for copy in across:
        copy.wait_recv()
    for copy in along + across:
        copy.wait_send()


def spread_sems(nf, nc):
    return [DMA((nc,)), DMA((nc,)), DMA((nf, nc)), DMA((nf, nc))]


def swap_copies(grad, land, nf, send, recv):
    f = lax.axis_index("fsdp")
    return [
        remote(
            grad.at[lax.rem(f + fo, nf)], land.at[fo - 1], send.at[fo], recv.at[fo],
            {"fsdp": lax.rem(f + fo, nf)},
        )
        for fo in range(1, nf)
    ]


def swap_sum(grad, land, out, nf):
    f = lax.axis_index("fsdp")
    for k in range(out.shape[0]):
        total = grad[f, k].astype(F32)
        for fo in range(1, nf):
            total = total + land[fo - 1, k].astype(F32)
        out[k] = total.astype(BF16)


def deal_copies(parts, land, nc, send, recv):
    c = lax.axis_index("ctx")
    return [
        remote(
            parts.at[lax.rem(c + o, nc)], land.at[o - 1], send.at[o], recv.at[o],
            {"ctx": lax.rem(c + o, nc)},
        )
        for o in (1, 3, 2)
    ]


def deal_sum(parts, land, nc):
    total = parts[lax.axis_index("ctx")].astype(F32)
    for o in range(1, nc):
        total = total + land[o - 1].astype(F32)
    return total


def ring_peers(axis, size):
    here = lax.axis_index(axis)
    return [{axis: lax.rem(here + o, size)} for o in range(1, size)]


def weight_peers(nf, nc):
    f, c = lax.axis_index("fsdp"), lax.axis_index("ctx")
    peers = []
    for o in range(1, nf * nc):
        other = lax.rem(f * nc + c + o, nf * nc)
        peers.append({"fsdp": other // nc, "ctx": lax.rem(other, nc)})
    return peers


def tp_places():
    mine = lax.axis_index("tp")
    partner = mine + 1 - 2 * lax.rem(mine, 2)
    cross = lax.rem(mine + 2, 4)
    far = lax.rem(partner + 2, 4)
    return mine, partner, cross, far


def entry_body(
    nf, nc, tok, weight, cond, modw, cbias, offset, extra,
    joint, hidden, weight_t, mod, ebuf,
    wbuf, pbuf, pland, normed, psend, precv, msend, mrecv, zs, zr, xs, xr, *esems,
):
    f, c, t = lax.axis_index("fsdp"), lax.axis_index("ctx"), lax.axis_index("tp")
    group = nf * nc
    mine = f * nc + c
    rows, width = tok.shape
    part = modw.shape[1]
    strips = part // 128

    def place(offset_):
        other = lax.rem(mine + offset_, group)
        return other // nc, lax.rem(other, nc)

    partial_mod = dot(cond[...], modw[...].astype(BF16), 1, 0)
    for latent in range(nf):
        for k in range(strips):
            pbuf[latent, pl.ds(k, 1), :] = partial_mod[latent : latent + 1, 128 * k : 128 * k + 128]
    wbuf[mine] = weight[...].astype(BF16)
    ebuf[mine] = extra[...].astype(BF16)
    greet(weight_peers(nf, nc) + ring_peers("tp", 4))
    pcopies = []
    for o in range(1, group):
        pf, pc = place(o)
        copy = remote(pbuf.at[pf], pland.at[mine], psend.at[o], precv.at[o], {"fsdp": pf, "ctx": pc})
        copy.start()
        pcopies.append(copy)
    spread_start(wbuf, nf, nc, zs, zr, xs, xr)
    pland[mine] = pbuf[f]
    step = 256
    for at in range(0, rows, step):
        normed[at : at + step, :] = centred(tok[at : at + step, :].astype(F32))[0]
    spread_relay(wbuf, nf, nc, zs, zr, xs, xr)
    spread_start(ebuf, nf, nc, *esems)
    for copy in pcopies:
        copy.wait_recv()
    total = pland[0]
    for k in range(1, group):
        total = total + pland[k]
    mod[t] = total + cbias[...]
    mcopies = []
    for o in range(1, 4):
        copy = remote(
            mod.at[t], mod.at[t], msend.at[o], mrecv.at[o], {"tp": lax.rem(t + o, 4)}
        )
        copy.start()
        mcopies.append(copy)
    for copy in mcopies:
        copy.wait_recv()
    shift = row_of(mod, 0, width, part)
    scale = row_of(mod, width, width, part)
    for at in range(0, rows, step):
        hidden[at : at + step, :] = (
            normed[at : at + step, :] * (1.0 + scale) + shift
        ).astype(BF16)
    spread_end(wbuf, nf, nc, zs, zr, xs, xr)
    spread_relay(ebuf, nf, nc, *esems)
    deep = weight.shape[0]
    for k in range(group):
        weight_t[:, k * deep : (k + 1) * deep] = transposed(wbuf[k])
    for at in range(0, rows, step):
        joint[:, at : at + step] = (
            dot(weight_t[...], hidden[at : at + step, :], 1, 1) + offset[...]
        ).astype(BF16)
    spread_end(ebuf, nf, nc, *esems)
    for copy in pcopies + mcopies:
        copy.wait_send()


def entry(nf, nc, tok, weight, cond, modw, cbias, offset, extra):
    rows, width = tok.shape
    deep, columns = weight.shape
    group = nf * nc
    return call(
        partial(entry_body, nf, nc),
        "entry",
        (
            shape((columns, rows), BF16),
            shape((rows, width), BF16),
            shape((columns, width), BF16),
            shape((4,) + cbias.shape, F32),
            shape((group,) + extra.shape, BF16),
        ),
        [
            pltpu.VMEM((group, deep, columns), BF16),
            pltpu.VMEM((nf,) + cbias.shape, F32),
            pltpu.VMEM((group,) + cbias.shape, F32),
            pltpu.VMEM((rows, width), F32),
            DMA((group,)), DMA((group,)), DMA((4,)), DMA((4,)),
        ]
        + spread_sems(nf, nc) * 2,
        1,
        30,
    )(tok, weight, cond, modw, cbias, offset, extra)


def attend_body(
    nf, nc, x, extra, att, qkv, out, lse, ebuf,
    stage, land, keys, scores, send, recv, osend, orecv, *esems,
):
    c = lax.axis_index("ctx")
    rows = x.shape[1]
    total = rows * nc
    hd = HEAD_DIM
    bq, bk = scores.shape[1], 512
    per = rows // bq
    slot = lax.axis_index("fsdp") * nc + c
    ebuf[slot] = extra[...].astype(BF16)
    greet(ring_peers("ctx", nc) + ring_peers("fsdp", nf))
    copies = []
    for o in range(1, nc):
        dst = lax.rem(c + o, nc)
        copy = remote(
            x.at[aligned(dst * 3 * hd, 3 * hd), :], qkv.at[:, aligned(c * rows, rows)],
            send.at[o], recv.at[o], {"ctx": dst},
        )
        copy.start()
        copies.append(copy)
    qkv[:, aligned(c * rows, rows)] = x[aligned(c * 3 * hd, 3 * hd), :]
    for copy in copies:
        copy.wait_recv()
    spread_start(ebuf, nf, nc, *esems)
    for at in range(0, total, 1024):
        keys[at : at + 1024, :] = transposed(qkv[hd : 2 * hd, at : at + 1024])

    def block(i, carry):
        o = 1 + i // per
        owner = lax.rem(c + o, nc)
        sub = lax.rem(i, per)
        where = aligned(owner * rows + sub * bq, bq)
        query = qkv[0:hd, where] * BF16(hd**-0.5)
        peak = None
        for at in range(0, total, bk):
            s = dot(keys[at : at + bk, :], query, 1, 0)
            scores[at : at + bk, :] = s
            high = jnp.max(s.reshape(bk // 8, 8, bq), axis=0)
            peak = high if peak is None else jnp.maximum(peak, high)
        peak = jnp.max(peak, axis=0, keepdims=True)
        acc, mass = None, None
        for at in range(0, total, bk):
            p = jnp.exp(scores[at : at + bk, :] - peak)
            low = jnp.sum(p.reshape(bk // 8, 8, bq), axis=0)
            mass = low if mass is None else mass + low
            term = dot(qkv[2 * hd : 3 * hd, at : at + bk], p.astype(BF16), 1, 0)
            acc = term if acc is None else acc + term
        mass = jnp.sum(mass, axis=0, keepdims=True)
        acc = acc * (1.0 / mass)
        out[:, where] = acc
        lse[:, where] = peak + jnp.log(mass)
        stage[owner, :, aligned(sub * bq, bq)] = acc.astype(BF16)

        @pl.when(jnp.logical_and(sub == per - 1, o < nc))
        def _():
            remote(
                stage.at[owner], land.at[c], osend.at[o], orecv.at[o], {"ctx": owner}
            ).start()

        @pl.when(i == per * nc - 3)
        def _():
            spread_relay(ebuf, nf, nc, *esems)

        return carry

    lax.fori_loop(0, per * nc, block, 0)
    land[c] = stage[c]
    for o in range(1, nc):
        dst = lax.rem(c + o, nc)
        copy = remote(stage.at[dst], land.at[c], osend.at[o], orecv.at[o], {"ctx": dst})
        copy.wait_recv()
        copy.wait_send()
    for k in range(nc):
        att[k * hd : (k + 1) * hd, :] = land[k]
    for copy in copies:
        copy.wait_send()
    spread_end(ebuf, nf, nc, *esems)


def attend(nf, nc, x, extra):
    rows = x.shape[1]
    total = rows * nc
    hd = HEAD_DIM
    bq = min(512, rows)
    return call(
        partial(attend_body, nf, nc),
        "attend",
        (
            shape((nc * hd, rows), BF16),
            shape((3 * hd, total), BF16),
            shape((hd, total), F32),
            shape((1, total), F32),
            shape((nf * nc,) + extra.shape, BF16),
        ),
        [
            pltpu.VMEM((nc, hd, rows), BF16),
            pltpu.VMEM((nc, hd, rows), BF16),
            pltpu.VMEM((total, hd), BF16),
            pltpu.VMEM((total, bq), F32),
            DMA((nc,)), DMA((nc,)), DMA((nc,)), DMA((nc,)),
        ]
        + spread_sems(nf, nc),
        2,
        70,
    )(x, extra)


def project_body(
    nf, nc, part, att, weight, tok, mod, bias, early, late, other,
    value, middle, hidden, expand, shrink,
    sbuf, rbuf, send, recv, gsend, grecv, *sems,
):
    mine, partner, cross, far = tp_places()
    own = value.shape[0]
    width = tok.shape[1]
    slot = lax.axis_index("fsdp") * nc + lax.axis_index("ctx")
    split = early.shape[2]
    lanes = pl.ds(split, split)
    expand[:, :, 0:split] = early[...]
    expand[slot, :, split : 2 * split] = late[...].astype(BF16)
    shrink[slot] = other[...].astype(BF16)

    def piece(at):
        return dot(
            att[:, aligned(at * own, own)].astype(F32).T.astype(BF16), weight[...], 1, 1
        )

    greet(ring_peers("tp", 4) + ring_peers("ctx", nc) + ring_peers("fsdp", nf))
    spread_start(expand, nf, nc, *sems[0:4], lanes)
    spread_start(shrink, nf, nc, *sems[4:8])
    sbuf[0] = piece(far).astype(BF16)
    first = remote(sbuf.at[0], rbuf.at[0], send.at[0], recv.at[0], {"tp": partner})
    first.start()
    sbuf[1] = piece(partner).astype(BF16)
    second = remote(sbuf.at[1], rbuf.at[1], send.at[1], recv.at[1], {"tp": partner})
    second.start()
    crossing = piece(cross)
    first.wait_recv()
    sbuf[2] = (crossing + rbuf[0].astype(F32)).astype(BF16)
    third = remote(sbuf.at[2], rbuf.at[2], send.at[2], recv.at[2], {"tp": cross})
    third.start()
    held = piece(mine)
    second.wait_recv()
    held = held + rbuf[1].astype(F32) + bias[0:1, :]
    third.wait_recv()
    held = held + rbuf[2].astype(F32)
    value[...] = held
    gate = row_of(mod, 2 * width, width, part)
    shift = row_of(mod, 3 * width, width, part)
    scale = row_of(mod, 4 * width, width, part)
    mid = tok[aligned(mine * own, own), :].astype(F32) + gate * held
    middle[...] = mid
    hidden[mine] = (centred(mid)[0] * (1.0 + scale) + shift).astype(BF16)
    copies = gather_start(hidden, mine, partner, cross, gsend, grecv)
    spread_relay(expand, nf, nc, *sems[0:4], lanes)
    gather_end(hidden, copies, mine, partner, cross, gsend, grecv)
    spread_relay(shrink, nf, nc, *sems[4:8])
    for copy in (first, second, third):
        copy.wait_send()
    spread_end(expand, nf, nc, *sems[0:4], lanes)
    spread_end(shrink, nf, nc, *sems[4:8])


def gather_start(slots, mine, partner, cross, send, recv):
    over = remote(slots.at[mine], slots.at[mine], send.at[0], recv.at[0], {"tp": cross})
    over.start()
    near = remote(slots.at[mine], slots.at[mine], send.at[1], recv.at[1], {"tp": partner})
    near.start()
    return over, near


def gather_end(slots, copies, mine, partner, cross, send, recv):
    over, near = copies
    over.wait_recv()
    relay = remote(slots.at[cross], slots.at[cross], send.at[2], recv.at[2], {"tp": partner})
    relay.start()
    near.wait_recv()
    relay.wait_recv()
    for copy in (over, near, relay):
        copy.wait_send()


def project(nf, nc, part, att, weight, tok, mod, bias, early, late, other):
    rows, width = tok.shape
    own = rows // 4
    return call(
        partial(project_body, nf, nc, part),
        "project",
        (
            shape((own, width), F32), shape((own, width), F32), shape((4, own, width), BF16),
            shape((nf * nc,) + other.shape, BF16), shape((nf * nc,) + other.shape, BF16),
        ),
        [
            pltpu.VMEM((3, own, width), BF16),
            pltpu.VMEM((3, own, width), BF16),
            DMA((3,)), DMA((3,)), DMA((3,)), DMA((3,)),
        ]
        + spread_sems(nf, nc) * 2,
        3,
        36,
    )(att, weight, tok, mod, bias, early, late, other)


def branch_body(
    part, hidden, cot, expand, shrink, hbias, mod, middle, value,
    attn_low, mid_grad, shrink_grad, expand_grad, stats, hstats, sh_cross, sh_own,
    gbuf, abuf, ebuf, sbuf, rbuf, shold, tsend, trecv, send, recv, gsend, grecv,
):
    mine, partner, cross, far = tp_places()
    own, width = middle.shape
    gate_first = row_of(mod, 2 * width, width, part)
    scale_second = row_of(mod, 4 * width, width, part)
    gate_second = row_of(mod, 5 * width, width, part)
    greet([{"tp": lax.rem(mine + o, 4)} for o in range(1, 4)])
    column = None
    copies = []
    held = None
    for turn, at in enumerate((far, partner, cross, mine)):
        where = aligned(at * own, own)
        grad = gate_second * cot[where, :].astype(F32)
        low = grad.astype(BF16)
        gbuf[where, :] = low
        if turn == 3:
            stats[3:4, :] = jnp.sum(grad, axis=0, keepdims=True)
        u = dot(hidden[at], expand[...], 1, 0) + hbias[...]
        squared = u * u
        th = jnp.tanh(GELU_SCALE * (u + GELU_CUBE * squared * u))
        act = (0.5 * u * (1.0 + th)).astype(BF16)
        abuf[where, :] = act
        slope = 0.5 * (1.0 + th) + 0.5 * u * (1.0 - th * th) * (
            GELU_SCALE * (1.0 + 3.0 * GELU_CUBE * squared)
        )
        pull = dot(low, shrink[...], 1, 0) * slope
        tally = jnp.sum(pull, axis=0, keepdims=True)
        column = tally if column is None else column + tally
        pull = pull.astype(BF16)
        ebuf[where, :] = pull
        back = dot(pull, expand[...], 1, 1)
        forth = dot(act, shrink[...], 1, 1)
        if turn < 2:
            sbuf[turn] = back.astype(BF16)
            copy = remote(sbuf.at[turn], rbuf.at[turn], send.at[turn], recv.at[turn], {"tp": partner})
            copy.start()
            copies.append(copy)
            shold[turn] = forth.astype(BF16)
            copy = remote(
                shold.at[turn], shold.at[2 + turn], tsend.at[turn], trecv.at[turn], {"tp": partner}
            )
            copy.start()
            copies.append(copy)
        elif turn == 2:
            copies[0].wait_recv()
            sbuf[2] = (back + rbuf[0].astype(F32)).astype(BF16)
            third = remote(sbuf.at[2], rbuf.at[2], send.at[2], recv.at[2], {"tp": cross})
            third.start()
            copies[1].wait_recv()
            sh_cross[...] = (forth + shold[2].astype(F32)).astype(BF16)
        else:
            copies[2].wait_recv()
            held = back + rbuf[1].astype(F32)
            copies[3].wait_recv()
            sh_own[...] = forth + shold[3].astype(F32)
    hstats[...] = column
    step = 256
    for at in range(0, width, step):
        shrink_grad[at : at + step, :] = dot(
            gbuf[:, at : at + step], abuf[...], 0, 0
        ).astype(BF16)
    third.wait_recv()
    grad_in = held + rbuf[2].astype(F32)
    normed, inverse = centred(middle[...])
    stats[0:1, :] = jnp.sum(grad_in, axis=0, keepdims=True)
    stats[1:2, :] = jnp.sum(grad_in * normed, axis=0, keepdims=True)
    mgrad = cot[aligned(mine * own, own), :].astype(F32) + normal_back(
        grad_in * (1.0 + scale_second), normed, inverse
    )
    mid_grad[...] = mgrad
    agrad = gate_first * mgrad
    attn_low[mine] = agrad.astype(BF16)
    gathers = gather_start(attn_low, mine, partner, cross, gsend, grecv)
    stats[2:3, :] = jnp.sum(mgrad * value[...], axis=0, keepdims=True)
    stats[4:5, :] = jnp.sum(agrad, axis=0, keepdims=True)
    stats[5:8, :] = jnp.zeros((3, width), F32)
    flat = hidden.shape[0] * own
    for at in range(0, width, step):
        expand_grad[at : at + step, :] = dot(
            hidden[:, :, at : at + step].reshape(flat, step), ebuf[...], 0, 0
        ).astype(BF16)
    gather_end(attn_low, gathers, mine, partner, cross, gsend, grecv)
    for copy in copies + [third]:
        copy.wait_send()


def branch(part, hidden, cot, expand, shrink, hbias, mod, middle, value):
    rows, width = cot.shape
    own = rows // 4
    units = expand.shape[1]
    return call(
        partial(branch_body, part),
        "branch",
        (
            shape((4, own, width), BF16),
            shape((own, width), F32),
            shape((width, units), BF16),
            shape((width, units), BF16),
            shape((8, width), F32),
            shape((1, units), F32),
            shape((own, width), BF16),
            shape((own, width), F32),
        ),
        [
            pltpu.VMEM((rows, width), BF16),
            pltpu.VMEM((rows, units), BF16),
            pltpu.VMEM((rows, units), BF16),
            pltpu.VMEM((3, own, width), BF16),
            pltpu.VMEM((3, own, width), BF16),
            pltpu.VMEM((4, own, width), BF16),
            DMA((2,)), DMA((2,)), DMA((3,)), DMA((3,)), DMA((3,)), DMA((3,)),
        ],
        4,
        45,
    )(hidden, cot, expand, shrink, hbias, mod, middle, value)


def retreat_body(
    nf, nc, part, attn_low, weight, att, qkv, out, lse, sh_cross, sh_own, middle, cot, mod, bias,
    shrink_grad, expand_grad,
    joint_grad, bias_grad, mixed, gate_grad, shrink_sum, expand_parts, output_parts,
    dout, dost, keys, vals, dq, stage, rland, wt, delta, output_grad,
    sland, eland, oland, shrink_parts, dland, send, recv, jsend, jrecv,
    csend, crecv, gsend, grecv, ssend, srecv, esend, erecv, osend, orecv, dsend, drecv,
):
    c = lax.axis_index("ctx")
    mine, partner, cross, far = tp_places()
    own, width = middle.shape
    rows = att.shape[1]
    total = rows * nc
    hd = HEAD_DIM
    bk = bq = 512
    per = rows // bk
    wt[...] = transposed(weight[...])
    low = attn_low[...].reshape(rows, width)
    dost[...] = dot(wt[...], low, 1, 1).astype(BF16)
    greet(ring_peers("tp", 4) + ring_peers("ctx", nc) + ring_peers("fsdp", nf))
    shrink_swap = swap_copies(shrink_grad, sland, nf, ssend, srecv)
    expand_swap = swap_copies(expand_grad, eland, nf, esend, erecv)
    output_swap = swap_copies(output_grad, oland, nf, osend, orecv)
    shrink_deal = deal_copies(shrink_parts, dland, nc, dsend, drecv)
    for copy in shrink_swap + expand_swap:
        copy.start()
    copies = []
    for o in range(1, nc):
        dst = lax.rem(c + o, nc)
        copy = remote(
            dost.at[aligned(dst * hd, hd), :], dout.at[:, aligned(c * rows, rows)],
            send.at[o], recv.at[o], {"ctx": dst},
        )
        copy.start()
        copies.append(copy)
    crossing = remote(sh_cross, rland, csend, crecv, {"tp": cross})
    crossing.start()
    dout[:, aligned(c * rows, rows)] = dost[aligned(c * hd, hd), :]
    flat = dot(att[...], low, 1, 0).T.astype(BF16)
    output_grad[...] = flat.reshape(output_grad.shape)
    for copy in output_swap:
        copy.start()
    for at in range(0, total, 1024):
        keys[at : at + 1024, :] = transposed(qkv[hd : 2 * hd, at : at + 1024])
        vals[at : at + 1024, :] = transposed(qkv[2 * hd : 3 * hd, at : at + 1024])
    dq[...] = jnp.zeros_like(dq)
    for copy in copies:
        copy.wait_recv()
    for at in range(0, total, 1024):
        delta[:, at : at + 1024] = jnp.sum(
            dout[:, at : at + 1024].astype(F32) * out[:, at : at + 1024], axis=0, keepdims=True
        )
    vsum_start = jnp.zeros((hd, 1), F32)

    def block(i, vsum):
        o = 1 + i // per
        owner = lax.rem(c + o, nc)
        sub = lax.rem(i, per)
        where = aligned(owner * rows + sub * bk, bk)
        key, val, key_t = keys[where, :], vals[where, :], qkv[hd : 2 * hd, where]
        dk, dv = None, None
        for at in range(0, total, bq):
            query = qkv[0:hd, at : at + bq] * BF16(hd**-0.5)
            grad = dout[:, at : at + bq]
            p = jnp.exp(dot(key, query, 1, 0) - lse[:, at : at + bq])
            ds = (p * (dot(val, grad, 1, 0) - delta[:, at : at + bq])).astype(BF16)
            tv = dot(grad, p.astype(BF16), 1, 1)
            tk = dot(query, ds, 1, 1)
            dv = tv if dv is None else dv + tv
            dk = tk if dk is None else dk + tk
            dq[:, at : at + bq] += dot(key_t, ds, 1, 0)
        put = aligned(sub * bk, bk)
        stage[owner, hd : 2 * hd, put] = dk.astype(BF16)
        stage[owner, 2 * hd : 3 * hd, put] = dv.astype(BF16)

        @pl.when(jnp.logical_and(sub == per - 1, o < nc))
        def _():
            remote(
                stage.at[owner, pl.ds(hd, 2 * hd), :], joint_grad.at[c, pl.ds(hd, 2 * hd), :],
                jsend.at[0, o], jrecv.at[0, o], {"ctx": owner},
            ).start()

        @pl.when(i == 3)
        def _():
            for copy in shrink_swap:
                copy.wait_recv()
            swap_sum(shrink_grad, sland, shrink_parts, nf)
            for copy in shrink_deal:
                copy.start()

        @pl.when(i == 6)
        def _():
            for copy in expand_swap:
                copy.wait_recv()
            swap_sum(expand_grad, eland, expand_parts, nf)

        @pl.when(i == 2)
        def _():
            crossing.wait_recv()
            value = sh_own[...] + rland[...].astype(F32) + bias[1:2, :]
            gate = row_of(mod, 5 * width, width, part)
            mixed[mine] = (middle[...] + gate * value).astype(BF16)
            gather_start(mixed, mine, partner, cross, gsend, grecv)
            gate_grad[...] = jnp.sum(
                cot[aligned(mine * own, own), :].astype(F32) * value, axis=0, keepdims=True
            )

        return vsum + jnp.sum(dv, axis=1, keepdims=True)

    vsum = lax.fori_loop(0, per * nc, block, vsum_start)
    qsum = jnp.zeros((hd, 1), F32)
    dqs = []
    for o in range(1, nc + 1):
        owner = lax.rem(c + o, nc)
        piece = dq[:, aligned(owner * rows, rows)] * (hd**-0.5)
        qsum = qsum + jnp.sum(piece, axis=1, keepdims=True)
        stage[owner, 0:hd, :] = piece.astype(BF16)
        if o < nc:
            copy = remote(
                stage.at[owner, pl.ds(0, hd), :], joint_grad.at[c, pl.ds(0, hd), :],
                jsend.at[1, o], jrecv.at[1, o], {"ctx": owner},
            )
            copy.start()
            dqs.append(copy)
    for copy in output_swap:
        copy.wait_recv()
    swap_sum(output_grad, oland, output_parts, nf)
    for copy in shrink_deal:
        copy.wait_recv()
    shrink_sum[...] = deal_sum(shrink_parts, dland, nc)
    joint_grad[c] = stage[c]
    bias_grad[0:hd, :] = jnp.broadcast_to(qsum, (hd, 128))
    bias_grad[hd : 2 * hd, :] = jnp.broadcast_to(vsum, (hd, 128))
    over = remote(mixed.at[mine], mixed.at[mine], gsend.at[0], grecv.at[0], {"tp": cross})
    near = remote(mixed.at[mine], mixed.at[mine], gsend.at[1], grecv.at[1], {"tp": partner})
    gather_end(mixed, (over, near), mine, partner, cross, gsend, grecv)
    for o in range(1, nc):
        dst = lax.rem(c + o, nc)
        copy = remote(
            stage.at[dst, pl.ds(hd, 2 * hd), :], joint_grad.at[c, pl.ds(hd, 2 * hd), :],
            jsend.at[0, o], jrecv.at[0, o], {"ctx": dst},
        )
        copy.wait_recv()
        copy.wait_send()
        dqs[o - 1].wait_recv()
        dqs[o - 1].wait_send()
    for copy in copies + [crossing] + shrink_swap + expand_swap + output_swap + shrink_deal:
        copy.wait_send()


def retreat(
    nf, nc, part, attn_low, weight, att, qkv, out, lse, sh_cross, sh_own, middle, cot, mod, bias,
    shrink_grad, expand_grad,
):
    rows, width = cot.shape
    own = rows // 4
    total = rows * nc
    hd = HEAD_DIM
    deep = width // (nf * nc)
    units = shrink_grad.shape[1]
    split = (nf, nc, deep, units)
    shrink_grad, expand_grad = shrink_grad.reshape(split), expand_grad.reshape(split)
    return call(
        partial(retreat_body, nf, nc, part),
        "retreat",
        (
            shape((nc, 3 * hd, rows), BF16),
            shape((2 * hd, 128), F32),
            shape((4, own, width), BF16),
            shape((1, width), F32),
            shape((deep, units), F32),
            shape((nc, deep, units), BF16),
            shape((nc, deep, nc * hd), BF16),
        ),
        [
            pltpu.VMEM((hd, total), BF16),
            pltpu.VMEM((nc * hd, rows), BF16),
            pltpu.VMEM((total, hd), BF16),
            pltpu.VMEM((total, hd), BF16),
            pltpu.VMEM((hd, total), F32),
            pltpu.VMEM((nc, 3 * hd, rows), BF16),
            pltpu.VMEM((own, width), BF16),
            pltpu.VMEM((nc * hd, width), BF16),
            pltpu.VMEM((1, total), F32),
            pltpu.VMEM((nf, nc, deep, nc * hd), BF16),
            pltpu.VMEM((nf - 1, nc, deep, units), BF16),
            pltpu.VMEM((nf - 1, nc, deep, units), BF16),
            pltpu.VMEM((nf - 1, nc, deep, nc * hd), BF16),
            pltpu.VMEM((nc, deep, units), BF16),
            pltpu.VMEM((nc - 1, deep, units), BF16),
            DMA((nc,)), DMA((nc,)), DMA((2, nc)), DMA((2, nc)),
            DMA, DMA, DMA((3,)), DMA((3,)),
        ]
        + [DMA((nf,))] * 6
        + [DMA((nc,))] * 2,
        5,
        100,
    )(
        attn_low, weight, att, qkv, out, lse, sh_cross, sh_own, middle, cot, mod, bias,
        shrink_grad, expand_grad,
    )


def leave_body(
    nf, nc, part, joint_grad, weight_t, hidden, tok, mid_grad, mod, expand_parts, output_parts,
    joint_parts, tokens_grad, stats, expand_sum, output_sum,
    sbuf, rbuf, joint_weight_grad, jland, eland, oland,
    send, recv, jsend, jrecv, esend, erecv, osend, orecv,
):
    mine, partner, cross, far = tp_places()
    own, width = mid_grad.shape
    columns = weight_t.shape[0]
    deep = expand_sum.shape[0]

    def piece(at):
        block = joint_grad[:, :, aligned(at * own, own)].reshape(columns, own)
        return dot(block.astype(F32).T.astype(BF16), weight_t[...], 1, 0)

    greet(ring_peers("tp", 4) + ring_peers("ctx", nc) + ring_peers("fsdp", nf))
    expand_deal = deal_copies(expand_parts, eland, nc, esend, erecv)
    output_deal = deal_copies(output_parts, oland, nc, osend, orecv)
    joint_swap = swap_copies(joint_weight_grad, jland, nf, jsend, jrecv)
    for copy in output_deal + expand_deal:
        copy.start()
    sbuf[0] = piece(far).astype(BF16)
    first = remote(sbuf.at[0], rbuf.at[0], send.at[0], recv.at[0], {"tp": partner})
    first.start()
    sbuf[1] = piece(partner).astype(BF16)
    second = remote(sbuf.at[1], rbuf.at[1], send.at[1], recv.at[1], {"tp": partner})
    second.start()
    crossing = piece(cross)
    first.wait_recv()
    sbuf[2] = (crossing + rbuf[0].astype(F32)).astype(BF16)
    third = remote(sbuf.at[2], rbuf.at[2], send.at[2], recv.at[2], {"tp": cross})
    third.start()
    flat = joint_grad[...].reshape(columns, tok.shape[0])
    rows_f = width // nf
    step = max(128, min(256, rows_f))
    for at in range(0, width, step):
        block = dot(flat, hidden[:, at : at + step], 1, 0).T.astype(BF16)
        for k in range(at // deep, (at + step) // deep):
            joint_weight_grad[k // nc, k % nc] = block[k * deep - at : (k + 1) * deep - at, :]
    for copy in joint_swap:
        copy.start()
    held = piece(mine)
    second.wait_recv()
    held = held + rbuf[1].astype(F32)
    normed, inverse = centred(tok[aligned(mine * own, own), :].astype(F32))
    third.wait_recv()
    grad_in = held + rbuf[2].astype(F32)
    scale = row_of(mod, width, width, part)
    stats[0:1, :] = jnp.sum(grad_in, axis=0, keepdims=True)
    stats[1:2, :] = jnp.sum(grad_in * normed, axis=0, keepdims=True)
    stats[2:8, :] = jnp.zeros((6, width), F32)
    tokens_grad[...] = (
        mid_grad[...] + normal_back(grad_in * (1.0 + scale), normed, inverse)
    ).astype(BF16)
    for copy in output_deal:
        copy.wait_recv()
    output_sum[...] = deal_sum(output_parts, oland, nc)
    for copy in expand_deal:
        copy.wait_recv()
    expand_sum[...] = deal_sum(expand_parts, eland, nc)
    for copy in joint_swap:
        copy.wait_recv()
    swap_sum(joint_weight_grad, jland, joint_parts, nf)
    for copy in [first, second, third] + output_deal + expand_deal + joint_swap:
        copy.wait_send()


def leave(nf, nc, part, joint_grad, weight_t, hidden, tok, mid_grad, mod, expand_parts, output_parts):
    rows, width = tok.shape
    own = rows // 4
    columns = weight_t.shape[0]
    deep, units = expand_parts.shape[1:]
    inner = output_parts.shape[2]
    return call(
        partial(leave_body, nf, nc, part),
        "leave",
        (
            shape((nc, deep, columns), BF16),
            shape((own, width), BF16),
            shape((8, width), F32),
            shape((deep, units), F32),
            shape((deep, inner), F32),
        ),
        [
            pltpu.VMEM((3, own, width), BF16),
            pltpu.VMEM((3, own, width), BF16),
            pltpu.VMEM((nf, nc, deep, columns), BF16),
            pltpu.VMEM((nf - 1, nc, deep, columns), BF16),
            pltpu.VMEM((nc - 1, deep, units), BF16),
            pltpu.VMEM((nc - 1, deep, inner), BF16),
            DMA((3,)), DMA((3,)), DMA((nf,)), DMA((nf,)),
            DMA((nc,)), DMA((nc,)), DMA((nc,)), DMA((nc,)),
        ],
        6,
        30,
    )(joint_grad, weight_t, hidden, tok, mid_grad, mod, expand_parts, output_parts)


def settle_body(
    nf, nc, part, joint_parts, own_tokens, stats_first, stats_second, gate_grad, hidden_stats,
    head_bias, shrink_sum, expand_sum, output_sum, modw, low,
    tokens_grad, joint_sum, modulate_sum, bias_rows, done,
    jland, pieces, land, total, gathered, fland, ftotal,
    jsend, jrecv, gsend, grecv, asend, arecv, bsend, brecv, csend, crecv, dsend, drecv,
):
    f, c, t = lax.axis_index("fsdp"), lax.axis_index("ctx"), lax.axis_index("tp")
    mine, partner, cross, far = tp_places()
    inner, group = nc * 4, nf * nc
    here, slot = c * 4 + t, f * nc + c
    width = stats_first.shape[1]
    deep = joint_sum.shape[0]
    slim = part // nc // 128
    share = 2 * width // nc // 128
    hshare = hidden_stats.shape[1] // nc // 128
    tokens_grad[mine] = own_tokens[...]
    rows = [
        stats_first[0:1, :], stats_first[1:2, :], stats_second[2:3, :],
        stats_second[0:1, :], stats_second[1:2, :], gate_grad[...],
    ]

    def strip(k):
        at = k * 128
        return rows[at // width][:, at % width : at % width + 128]

    residual = [stats_second[4:5, :], stats_second[3:4, :]]
    pieces[...] = jnp.zeros_like(pieces)
    for cc in range(nc):
        for tt in range(4):
            k = cc * 4 + tt
            for n in range(slim):
                pieces[k, n : n + 1, :] = strip((tt * part // 128) + cc * slim + n)
            for n in range(share):
                at = (cc * share + n) * 128
                pieces[k, slim + n : slim + n + 1, :] = residual[at // width][
                    :, at % width : at % width + 128
                ]
        for n in range(hshare):
            at = (cc * hshare + n) * 128
            pieces[cc * 4 + t, slim + share + n : slim + share + n + 1, :] = hidden_stats[
                :, at : at + 128
            ]
    last = slim + share + hshare
    pieces[here, last : last + 1, :] = head_bias[...].T[0:1, :]
    greet(
        [
            {"ctx": lax.rem(here + o, inner) // 4, "tp": lax.rem(lax.rem(here + o, inner), 4)}
            for o in range(1, inner)
        ]
        + weight_peers(nf, nc)
    )
    first = []
    for o in range(1, inner):
        other = lax.rem(here + o, inner)
        copy = remote(
            pieces.at[other], land.at[here], asend.at[o], arecv.at[o],
            {"ctx": other // 4, "tp": lax.rem(other, 4)},
        )
        copy.start()
        first.append(copy)
    deals = deal_copies(joint_parts, jland, nc, jsend, jrecv)
    for copy in deals:
        copy.start()
    gathers = gather_start(tokens_grad, mine, partner, cross, gsend, grecv)
    land[here] = pieces[here]
    for copy in first:
        copy.wait_recv()
    acc = land[0]
    for k in range(1, inner):
        acc = acc + land[k]
    total[...] = acc
    gathered[slot] = acc
    second = []
    for o, peer in zip(range(1, group), weight_peers(nf, nc)):
        copy = remote(total, gathered.at[slot], bsend.at[o], brecv.at[o], peer)
        copy.start()
        second.append(copy)
    squares = (
        jnp.sum(shrink_sum[...] * shrink_sum[...])
        + jnp.sum(expand_sum[...] * expand_sum[...])
        + jnp.sum(output_sum[...] * output_sum[...])
    )
    for copy in second:
        copy.wait_recv()
    grads = []
    for latent in range(nf):
        strips = []
        for cc in range(nc):
            for n in range(slim):
                strips.append(gathered[latent * nc + cc, n : n + 1, :])
        grads.append(jnp.concatenate(strips, axis=1))
    condition_bias = grads[0]
    for latent in range(1, nf):
        condition_bias = condition_bias + grads[latent]
    bias_rows[...] = jnp.zeros_like(bias_rows)
    bias_rows[0:1, 0:part] = condition_bias
    factors = low[...].T
    wide = modw[...].astype(BF16).astype(F32)
    outer = None
    ftotal[...] = jnp.zeros_like(ftotal)
    for latent in range(nf):
        term = factors[:, latent : latent + 1] * grads[latent]
        outer = term if outer is None else outer + term
        column = jnp.sum(wide * grads[latent], axis=1, keepdims=True)
        ftotal[latent : latent + 1, 0:deep] = jnp.broadcast_to(column, (deep, 128)).T[0:1, :]
    modulate_sum[...] = outer
    squares = squares + jnp.sum(outer * outer)

    def over(at, count, step):
        found = []
        for cc in range(nc):
            value = None
            for latent in range(nf):
                block = gathered[latent * nc + cc, at : at + count, :]
                value = block if value is None else value + block
            for n in range(count):
                found.append(value[n : n + 1, :])
        return jnp.concatenate(found, axis=1)

    residual_sum = over(slim, share, 0)
    hidden_sum = over(slim + share, hshare, 0)
    head_sum = over(last, 1, 0)
    bias_rows[1:2, 0 : hidden_sum.shape[1]] = hidden_sum
    bias_rows[2:3, 0 : head_sum.shape[1]] = head_sum
    bias_rows[3:4, 0:width] = residual_sum[:, 0:width]
    bias_rows[4:5, 0:width] = residual_sum[:, width : 2 * width]
    lead = (slot == 0).astype(F32)
    tensor_lead = (t == 0).astype(F32)
    squares = squares + lead * (
        jnp.sum(condition_bias * condition_bias)
        + jnp.sum(hidden_sum * hidden_sum)
        + jnp.sum(head_sum * head_sum)
        + tensor_lead * jnp.sum(residual_sum * residual_sum)
    )
    for copy in deals:
        copy.wait_recv()
    joint = deal_sum(joint_parts, jland, nc)
    joint_sum[...] = joint
    squares = squares + jnp.sum(joint * joint)
    ftotal[nf : nf + 1, :] = jnp.full((1, 128), squares)
    third = []
    for o, peer in zip(range(1, 4), ring_peers("tp", 4)):
        copy = remote(ftotal, fland.at[t], csend.at[o], crecv.at[o], peer)
        copy.start()
        third.append(copy)
    fland[t] = ftotal[...]
    for copy in third:
        copy.wait_recv()
    acc = fland[0] + fland[1] + fland[2] + fland[3]
    done[slot] = acc
    fourth = []
    for o, peer in zip(range(1, group), weight_peers(nf, nc)):
        copy = remote(done.at[slot], done.at[slot], dsend.at[o], drecv.at[o], peer)
        copy.start()
        fourth.append(copy)
    gather_end(tokens_grad, gathers, mine, partner, cross, gsend, grecv)
    for copy in fourth:
        copy.wait_recv()
    for copy in first + deals + second + third + fourth:
        copy.wait_send()


def settle(
    nf, nc, part, joint_parts, own_tokens, stats_first, stats_second, gate_grad, hidden_stats,
    head_bias, shrink_sum, expand_sum, output_sum, modw, low,
):
    own, width = own_tokens.shape
    deep, columns = joint_parts.shape[1:]
    inner, group = nc * 4, nf * nc
    high = -(-(part // nc + 2 * width // nc + hidden_stats.shape[1] // nc + 128) // 1024) * 8
    tall = -(-(nf + 1) // 8) * 8
    return call(
        partial(settle_body, nf, nc, part),
        "settle",
        (
            shape((4, own, width), BF16),
            shape((deep, columns), F32),
            shape((deep, part), F32),
            shape((8, max(part, width, hidden_stats.shape[1])), F32),
            shape((group, tall, 128), F32),
        ),
        [
            pltpu.VMEM((nc - 1, deep, columns), BF16),
            pltpu.VMEM((inner, high, 128), F32),
            pltpu.VMEM((inner, high, 128), F32),
            pltpu.VMEM((high, 128), F32),
            pltpu.VMEM((group, high, 128), F32),
            pltpu.VMEM((4, tall, 128), F32),
            pltpu.VMEM((tall, 128), F32),
            DMA((nc,)), DMA((nc,)), DMA((3,)), DMA((3,)),
            DMA((inner,)), DMA((inner,)), DMA((group,)), DMA((group,)),
            DMA((4,)), DMA((4,)), DMA((group,)), DMA((group,)),
        ],
        7,
        30,
    )(
        joint_parts, own_tokens, stats_first, stats_second, gate_grad, hidden_stats,
        head_bias, shrink_sum, expand_sum, output_sum, modw, low,
    )


def update(master, first, root, gradient, clip, decay_rate):
    scaled = clip * gradient
    first_moment = first_decay * first + (1.0 - first_decay) * scaled
    second_moment = second_decay * root * root + (1.0 - second_decay) * scaled * scaled
    new_root = jnp.sqrt(second_moment)
    first_hat = first_moment * (1.0 / (1.0 - first_decay**ADAM_STEP))
    second_hat = second_moment * (1.0 / (1.0 - second_decay**ADAM_STEP))
    updated = master - learning_rate * (
        first_hat / (jnp.sqrt(second_hat) + adam_epsilon) + decay_rate * master
    )
    return updated, first_moment, new_root


def adam_body(count, nf, nc, done, condition, bias_rows, *refs):
    grads = refs[:count]
    masters = refs[count : 2 * count]
    moments = refs[2 * count : 3 * count]
    smalls = refs[3 * count : 3 * count + 8]
    outs = refs[3 * count + 8 :]
    news = outs[:count]
    averages = outs[count : 2 * count]
    small_outs = outs[2 * count : 2 * count + 8]
    condition_grad, norm = outs[2 * count + 8 : 2 * count + 10]
    scratch = outs[2 * count + 10 :]
    wbufs = scratch[:count]
    mbufs = scratch[count : 2 * count]
    gbufs = scratch[2 * count : 3 * count]
    isem, osem = scratch[3 * count :]
    group = nf * nc
    f = lax.axis_index("fsdp")
    loads, stores = [], []
    for k in range(count):
        loads.append(
            (
                pltpu.make_async_copy(masters[k], wbufs[k], isem.at[0, k]),
                pltpu.make_async_copy(moments[k], mbufs[k], isem.at[1, k]),
                pltpu.make_async_copy(grads[k], gbufs[k], isem.at[2, k]),
            )
        )
        stores.append(
            (
                pltpu.make_async_copy(wbufs[k], news[k], osem.at[0, k]),
                pltpu.make_async_copy(mbufs[k], averages[k], osem.at[1, k]),
            )
        )
    for trio in loads:
        for copy in trio:
            copy.start()
    squares = done[0, nf : nf + 1, 0:1]
    for k in range(1, group):
        squares = squares + done[k, nf : nf + 1, 0:1]
    grad_norm = jnp.sqrt(squares)
    norm[...] = grad_norm
    clip = jnp.minimum(1.0, clip_limit / (grad_norm + 1e-06))
    deep = condition.shape[1] // group
    found = [done[k, pl.ds(f, 1), 0:deep] for k in range(group)]
    v = condition[pl.ds(f, 1), :]
    gate = 1.0 / (1.0 + jnp.exp(-v))
    condition_grad[...] = jnp.concatenate(found, axis=1) * (gate * (1.0 + v * (1.0 - gate)))
    for k in range(4):
        master, moment = smalls[2 * k], smalls[2 * k + 1]
        if k < 3:
            row = (2, 1, 0)[k]
            grad = bias_rows[row : row + 1, 0 : master.shape[1]]
            new, first, root = update(master[...], moment[0:1, :], moment[1:2, :], grad, clip, 0.0)
            small_outs[2 * k][...] = new
            small_outs[2 * k + 1][0:1, :] = first
            small_outs[2 * k + 1][1:2, :] = root
        else:
            grad = bias_rows[3:5, 0 : master.shape[1]]
            new, first, root = update(master[...], moment[0], moment[1], grad, clip, 0.0)
            small_outs[2 * k][...] = new
            small_outs[2 * k + 1][0] = first
            small_outs[2 * k + 1][1] = root
    for k in range(count):
        for copy in loads[k]:
            copy.wait()
        deep_k = wbufs[k].shape[0]
        step = min(16, deep_k)

        def rows(i, carry, k=k, step=step):
            at = pl.ds(pl.multiple_of(i * step, step), step)
            new, first, root = update(
                wbufs[k][at, :], mbufs[k][0, at, :], mbufs[k][1, at, :], gbufs[k][at, :],
                clip, weight_decay,
            )
            wbufs[k][at, :] = new
            mbufs[k][0, at, :] = first
            mbufs[k][1, at, :] = root
            return carry

        lax.fori_loop(0, deep_k // step, rows, 0)
        for copy in stores[k]:
            copy.start()
    for pair in stores:
        for copy in pair:
            copy.wait()


def adam(nf, nc, done, condition, bias_rows, grads, masters, moments, smalls):
    count = len(grads)
    anywhere = pl.BlockSpec(memory_space=pl.ANY)
    small_shapes = tuple(shape(a.shape, F32) for a in smalls)
    outs = (
        tuple(shape(m.shape, F32) for m in masters)
        + tuple(shape(m.shape, F32) for m in moments)
        + small_shapes
        + (shape((1, condition.shape[1]), F32), shape((1, 1), F32))
    )
    return pl.pallas_call(
        partial(adam_body, count, nf, nc),
        out_shape=outs,
        in_specs=vmem(3) + [anywhere] * (3 * count) + vmem(8),
        out_specs=[anywhere] * (2 * count) + vmem(10),
        scratch_shapes=[pltpu.VMEM(m.shape, F32) for m in masters]
        + [pltpu.VMEM(m.shape, F32) for m in moments]
        + [pltpu.VMEM(m.shape, F32) for m in masters]
        + [DMA((3, count)), DMA((2, count))],
        compiler_params=pltpu.CompilerParams(vmem_limit_bytes=40000000),
        cost_estimate=cost(10),
        name="adam",
    )(done, condition, bias_rows, *grads, *masters, *moments, *smalls)


def local(
    nf,
    nc,
    tokens,
    condition,
    cotangent,
    joint_weight,
    joint_moments,
    output_weight,
    output_moments,
    expand_weight,
    expand_moments,
    shrink_weight,
    shrink_moments,
    modulate_weight,
    modulate_moments,
    attention_bias,
    attention_moments,
    hidden_bias,
    hidden_moments,
    condition_bias,
    condition_moments,
    residual_bias,
    residual_moments,
):
    latent_count, rows, width = tokens.shape
    heads = joint_weight.shape[1] // (3 * HEAD_DIM)
    assert latent_count == 1 and heads == nc and lax.axis_size("tp") == 4
    f, c, t = lax.axis_index("fsdp"), lax.axis_index("ctx"), lax.axis_index("tp")
    mine = f * nc + c
    deep, part = modulate_weight.shape
    units = expand_weight.shape[1]
    tok, cot = tokens[0], cotangent[0]

    condition_low = jax.nn.silu(condition).astype(BF16)
    condition_here = lax.dynamic_slice_in_dim(condition_low, mine * deep, deep, 1)
    strips = part // 128
    high = -(-strips // 8) * 8
    bias_strips = jnp.pad(condition_bias.reshape(strips, 128), ((0, high - strips), (0, 0)))
    bias_pairs = attention_bias.reshape(heads, 2, HEAD_DIM)
    offset = jnp.stack(
        [bias_pairs[:, 0], jnp.zeros_like(bias_pairs[:, 0]), bias_pairs[:, 1]], axis=1
    ).reshape(-1, 1)
    condition_pad = jnp.pad(condition_here, ((0, 16 - nf), (0, 0)))
    joint_t, hidden_first, joint_full_t, mod, output_full = entry(
        nf, nc, tok, joint_weight, condition_pad, modulate_weight, bias_strips, offset,
        output_weight,
    )
    output_full = output_full.reshape(width, -1)
    half = units // 2
    att_t, qkv, out, lse, expand_early = attend(nf, nc, joint_t, expand_weight[:, :half])
    value, middle, hidden_second, expand_full, shrink_full = project(
        nf, nc, part, att_t, output_full, tok, mod, residual_bias,
        expand_early, expand_weight[:, half:], shrink_weight,
    )
    (
        attn_low, mid_grad, shrink_grad, expand_grad, stats_second, hidden_stats, sh_cross, sh_own,
    ) = branch(
        part, hidden_second, cot, expand_full.reshape(width, units),
        shrink_full.reshape(width, units), hidden_bias[None, :], mod, middle, value,
    )
    joint_grad, head_bias, mixed, gate_second_grad, shrink_sum, expand_parts, output_parts = retreat(
        nf, nc, part, attn_low, output_full, att_t, qkv, out, lse, sh_cross, sh_own, middle, cot,
        mod, residual_bias, shrink_grad, expand_grad,
    )
    joint_parts, own_tokens, stats_first, expand_sum, output_sum = leave(
        nf, nc, part, joint_grad, joint_full_t, hidden_first, tok, mid_grad, mod,
        expand_parts, output_parts,
    )
    tokens_grad, joint_sum, modulate_sum, bias_rows, done = settle(
        nf, nc, part, joint_parts, own_tokens, stats_first, stats_second, gate_second_grad,
        hidden_stats, head_bias, shrink_sum, expand_sum, output_sum, modulate_weight,
        condition_pad.astype(F32),
    )
    weights = (joint_weight, output_weight, expand_weight, shrink_weight, modulate_weight)
    moments = (joint_moments, output_moments, expand_moments, shrink_moments, modulate_moments)
    grads = (joint_sum, output_sum, expand_sum, shrink_sum, modulate_sum)
    smalls = (
        attention_bias[None, :], attention_moments, hidden_bias[None, :], hidden_moments,
        condition_bias[None, :], condition_moments, residual_bias, residual_moments,
    )
    results = adam(nf, nc, done, condition, bias_rows, grads, weights, moments, smalls)
    updated = []
    for k in range(5):
        updated += [results[k], results[5 + k]]
    for k in range(4):
        new = results[10 + 2 * k]
        updated += [new[0] if k < 3 else new, results[11 + 2 * k]]
    return (
        mixed.reshape(1, rows, width),
        tokens_grad.reshape(1, rows, width).astype(F32),
        results[18],
        results[19][0, 0],
    ) + tuple(updated)


def solution(mesh):
    rows = P(("fsdp", "ctx"), "tp")
    pair = P(None, ("fsdp", "ctx"), "tp")
    tokens = P("fsdp", "ctx", None)
    small = (P("tp"), P(None, "tp"))
    return jax.shard_map(
        partial(local, mesh.shape["fsdp"], mesh.shape["ctx"]),
        mesh=mesh,
        in_specs=(tokens, P(), tokens) + (rows, pair) * 5 + small * 3 + (P(), P()),
        out_specs=(tokens, tokens, P("fsdp", None), P())
        + (rows, pair) * 5
        + small * 3
        + (P(), P()),
        check_vma=False,
    )
```

```python
from functools import partial

import jax
import jax.numpy as jnp
from jax import lax
from jax.experimental import pallas as pl
from jax.experimental.pallas import tpu as pltpu
from jax.sharding import PartitionSpec as P

HEAD_DIM = 64
ADAM_STEP = 10
F32 = jnp.float32
BF16 = jnp.bfloat16
MESH = pl.DeviceIdType.MESH
DMA = pltpu.SemaphoreType.DMA

norm_epsilon = 1e-06
first_decay = 0.9
second_decay = 0.999
adam_epsilon = 1e-08
learning_rate = 0.05
weight_decay = 0.1
clip_limit = 1.0
GELU_SCALE = 0.7978845608028654
GELU_CUBE = 0.044715


def dot(a, b, ca, cb):
    return lax.dot_general(a, b, (((ca,), (cb,)), ((), ())), preferred_element_type=F32)


def aligned(start, size):
    return pl.ds(pl.multiple_of(start, size), size)


def greet(peers):
    barrier = pltpu.get_barrier_semaphore()
    for peer in peers:
        pl.semaphore_signal(barrier, inc=1, device_id=peer, device_id_type=MESH)
    pl.semaphore_wait(barrier, len(peers))


def remote(source, target, send_sem, recv_sem, peer):
    return pltpu.make_async_remote_copy(
        src_ref=source,
        dst_ref=target,
        send_sem=send_sem,
        recv_sem=recv_sem,
        device_id=peer,
        device_id_type=MESH,
    )


def vmem(count):
    return [pl.BlockSpec(memory_space=pltpu.VMEM)] * count


def shape(dims, dtype):
    return jax.ShapeDtypeStruct(dims, dtype)


def cost(micros, flops=0):
    return pl.CostEstimate(flops=flops, bytes_accessed=int(micros * 3.0e6), transcendentals=0)


def call(body, name, outs, scratch, ident, micros, megabytes):
    def run(*args):
        return pl.pallas_call(
            body,
            out_shape=outs,
            in_specs=vmem(len(args)),
            out_specs=vmem(len(outs)),
            scratch_shapes=scratch,
            compiler_params=pltpu.CompilerParams(
                collective_id=ident, has_side_effects=True, vmem_limit_bytes=megabytes << 20
            ),
            cost_estimate=cost(micros),
            name=name,
        )(*args)

    return run


def transposed(block):
    return block.astype(F32).T.astype(BF16)


def row_of(mod, start, width, part):
    pieces = []
    for at in range(start, start + width, 128):
        pieces.append(mod[at // part, pl.ds((at % part) // 128, 1), :])
    return jnp.concatenate(pieces, axis=1)


def centred(values):
    center = values - jnp.mean(values, axis=-1, keepdims=True)
    inverse = lax.rsqrt(jnp.mean(center * center, axis=-1, keepdims=True) + norm_epsilon)
    return center * inverse, inverse


def normal_back(grad, normed, inverse):
    return inverse * (
        grad
        - jnp.mean(grad, axis=-1, keepdims=True)
        - normed * jnp.mean(grad * normed, axis=-1, keepdims=True)
    )


class Gather:
    def __init__(self, buf, nf, nc, sems, parts):
        self.buf, self.nf, self.nc, self.sems, self.parts = buf, nf, nc, sems, parts
        self.columns = buf.shape[2] // parts

    def view(self, ctx, part):
        slot = lax.axis_index("fsdp") * self.nc + ctx
        return self.buf.at[slot, :, pl.ds(part * self.columns, self.columns)]

    def along(self, o, part):
        c = lax.axis_index("ctx")
        zs, zr = self.sems[4 * part : 4 * part + 2]
        view = self.view(c, part)
        return remote(view, view, zs.at[o], zr.at[o], {"ctx": lax.rem(c + o, self.nc)})

    def onward(self, part):
        c = lax.axis_index("ctx")
        zs, zr = self.sems[4 * part : 4 * part + 2]
        view = self.view(lax.rem(c + 2, self.nc), part)
        up = remote(view, view, zs.at[0], zr.at[3], {"ctx": lax.rem(c + 1, self.nc)})
        down = remote(view, view, zs.at[0], zr.at[1], {"ctx": lax.rem(c + 3, self.nc)})
        return up, down

    def across(self, o, part):
        f, c = lax.axis_index("fsdp"), lax.axis_index("ctx")
        xs, xr = self.sems[4 * part + 2 : 4 * part + 4]
        view = self.view(lax.rem(c - o + self.nc, self.nc), part)
        return [
            remote(view, view, xs.at[fo, o], xr.at[fo, o], {"fsdp": lax.rem(f + fo, self.nf)})
            for fo in range(1, self.nf)
        ]

    def start(self):
        c = lax.axis_index("ctx")
        for part in range(self.parts):
            self.along(2, part).start()
            pl.when(c != 3)(self.along(1, part).start)
            pl.when(c != 0)(self.along(3, part).start)
            for copy in self.across(0, part):
                copy.start()

    def relay_middle(self, part):
        c = lax.axis_index("ctx")
        self.along(2, part).wait_recv()
        up, down = self.onward(part)
        pl.when(c == 2)(up.start)
        pl.when(c == 1)(down.start)
        for copy in self.across(2, part):
            copy.start()

    def relay_rest(self, part):
        for o in (1, 3):
            self.along(o, part).wait_recv()
            for copy in self.across(o, part):
                copy.start()

    def relay(self):
        for part in range(self.parts):
            self.relay_middle(part)
        for part in range(self.parts):
            self.relay_rest(part)

    def arrive(self):
        for part in range(self.parts):
            for o in range(self.nc):
                for copy in self.across(o, part):
                    copy.wait_recv()

    def drain(self):
        c = lax.axis_index("ctx")
        for part in range(self.parts):
            for o in range(self.nc):
                for copy in self.across(o, part):
                    copy.wait_send()
            up, down = self.onward(part)
            self.along(2, part).wait_send()
            pl.when(c != 3)(self.along(1, part).wait_send)
            pl.when(c != 0)(self.along(3, part).wait_send)
            pl.when(c == 2)(up.wait_send)
            pl.when(c == 1)(down.wait_send)


def gather_sems(nf, nc, parts):
    return [DMA((nc,)), DMA((nc,)), DMA((nf, nc)), DMA((nf, nc))] * parts


class Sum:
    def __init__(self, sbuf, rbuf, send, recv):
        self.sbuf, self.rbuf, self.send, self.recv = sbuf, rbuf, send, recv
        self.places = tp_places()

    def copy(self, k):
        mine, partner, cross, far = self.places
        peer = cross if k == 2 else partner
        return remote(
            self.sbuf.at[k], self.rbuf.at[k], self.send.at[k], self.recv.at[k], {"tp": peer}
        )

    def give(self, k, value):
        self.sbuf[k] = value.astype(BF16)
        self.copy(k).start()

    def pass_on(self, value):
        self.copy(0).wait_recv()
        self.give(2, value + self.rbuf[0].astype(F32))

    def near(self, value):
        self.copy(1).wait_recv()
        return value + self.rbuf[1].astype(F32)

    def total(self, value):
        self.copy(2).wait_recv()
        return value + self.rbuf[2].astype(F32)

    def drain(self):
        for k in range(3):
            self.copy(k).wait_send()


class Share:
    def __init__(self, slots, send, recv):
        self.slots, self.send, self.recv = slots, send, recv
        self.places = tp_places()

    def copy(self, k):
        mine, partner, cross, far = self.places
        slot, peer = ((mine, cross), (mine, partner), (cross, partner))[k]
        view = self.slots.at[slot]
        return remote(view, view, self.send.at[k], self.recv.at[k], {"tp": peer})

    def start(self):
        self.copy(0).start()
        self.copy(1).start()

    def relay(self):
        self.copy(0).wait_recv()
        self.copy(2).start()

    def finish(self):
        self.copy(1).wait_recv()
        self.copy(2).wait_recv()
        for k in range(3):
            self.copy(k).wait_send()


def share_sems():
    return [DMA((3,)), DMA((3,))]


def swap_copies(grad, land, nf, send, recv):
    f = lax.axis_index("fsdp")
    return [
        remote(
            grad.at[lax.rem(f + fo, nf)], land.at[fo - 1], send.at[fo], recv.at[fo],
            {"fsdp": lax.rem(f + fo, nf)},
        )
        for fo in range(1, nf)
    ]


def swap_sum(grad, land, out, nf):
    f = lax.axis_index("fsdp")
    for k in range(out.shape[0]):
        total = grad[f, k].astype(F32)
        for fo in range(1, nf):
            total = total + land[fo - 1, k].astype(F32)
        out[k] = total.astype(BF16)


def deal_copies(parts, land, nc, send, recv):
    c = lax.axis_index("ctx")
    return [
        remote(
            parts.at[lax.rem(c + o, nc)], land.at[o - 1], send.at[o], recv.at[o],
            {"ctx": lax.rem(c + o, nc)},
        )
        for o in (1, 3, 2)
    ]


def deal_sum(parts, land, nc):
    total = parts[lax.axis_index("ctx")].astype(F32)
    for o in range(1, nc):
        total = total + land[o - 1].astype(F32)
    return total


def ring_peers(axis, size):
    here = lax.axis_index(axis)
    return [{axis: lax.rem(here + o, size)} for o in range(1, size)]


def weight_peers(nf, nc):
    f, c = lax.axis_index("fsdp"), lax.axis_index("ctx")
    peers = []
    for o in range(1, nf * nc):
        other = lax.rem(f * nc + c + o, nf * nc)
        peers.append({"fsdp": other // nc, "ctx": lax.rem(other, nc)})
    return peers


def tp_places():
    mine = lax.axis_index("tp")
    partner = mine + 1 - 2 * lax.rem(mine, 2)
    cross = lax.rem(mine + 2, 4)
    far = lax.rem(partner + 2, 4)
    return mine, partner, cross, far


def forward_body(
    nf, nc, part, tok, jweight, cond, modw, cbias, offset, oweight, eweight, sweight, bias,
    hidden, weight_t, mod, obuf, qkv, out, lse, land, ebuf, value, middle, hidden_two, sgat,
    wbuf, pbuf, pland, normed, joint, stage, keys, scores, sbuf, rbuf,
    psend, precv, msend, mrecv, send, recv, osend, orecv, tsend, trecv, gsend, grecv, *gsems,
):
    f, c, t = lax.axis_index("fsdp"), lax.axis_index("ctx"), lax.axis_index("tp")
    mine, partner, cross, far = tp_places()
    group = nf * nc
    slot = f * nc + c
    rows, width = tok.shape
    strips = part // 128
    hd = HEAD_DIM
    step = 256
    partial_mod = dot(cond[...], modw[...].astype(BF16), 1, 0)
    for latent in range(nf):
        for k in range(strips):
            pbuf[latent, pl.ds(k, 1), :] = partial_mod[latent : latent + 1, 128 * k : 128 * k + 128]
    joint_gather = Gather(wbuf, nf, nc, gsems[0:8], 2)
    output_gather = Gather(obuf, nf, nc, gsems[8:12], 1)
    expand_gather = Gather(ebuf, nf, nc, gsems[12:20], 2)
    shrink_gather = Gather(sgat, nf, nc, gsems[20:28], 2)
    wbuf[slot] = jweight[...].astype(BF16)
    greet(weight_peers(nf, nc) + ring_peers("tp", 4))
    pcopies = []
    for o, peer in zip(range(1, group), weight_peers(nf, nc)):
        copy = remote(pbuf.at[peer["fsdp"]], pland.at[slot], psend.at[o], precv.at[o], peer)
        copy.start()
        pcopies.append(copy)
    joint_gather.start()
    pland[slot] = pbuf[f]
    obuf[slot] = oweight[...].astype(BF16)
    ebuf[slot] = eweight[...].astype(BF16)
    sgat[slot] = sweight[...].astype(BF16)
    half = rows // 2
    for at in range(0, half, step):
        normed[at : at + step, :] = centred(tok[at : at + step, :].astype(F32))[0]
    joint_gather.relay_middle(0)
    for at in range(half, rows, step):
        normed[at : at + step, :] = centred(tok[at : at + step, :].astype(F32))[0]
    joint_gather.relay_middle(1)
    for copy in pcopies:
        copy.wait_recv()
    total_mod = pland[0]
    for k in range(1, group):
        total_mod = total_mod + pland[k]
    mod[t] = total_mod + cbias[...]
    mcopies = []
    for o, peer in zip(range(1, 4), ring_peers("tp", 4)):
        copy = remote(mod.at[t], mod.at[t], msend.at[o], mrecv.at[o], peer)
        copy.start()
        mcopies.append(copy)
    joint_gather.relay_rest(0)
    for copy in mcopies:
        copy.wait_recv()
    shift = row_of(mod, 0, width, part)
    scale = row_of(mod, width, width, part)
    for at in range(0, rows, step):
        hidden[at : at + step, :] = (
            normed[at : at + step, :] * (1.0 + scale) + shift
        ).astype(BF16)
    joint_gather.relay_rest(1)
    output_gather.start()
    joint_gather.arrive()
    deep = jweight.shape[0]
    for k in range(group):
        weight_t[:, k * deep : (k + 1) * deep] = transposed(wbuf[k])

    total = rows * nc
    bq, bk = scores.shape[1], 512
    per = rows // bq
    copies = []
    for o in (2, 1, 3, 0):
        dst = lax.rem(c + o, nc)
        where = aligned(dst * 3 * hd, 3 * hd)
        head = (dot(weight_t[where, :], hidden[...], 1, 1) + offset[where, :]).astype(BF16)
        if o == 0:
            qkv[:, aligned(c * rows, rows)] = head
        else:
            joint[where, :] = head
            copy = remote(
                joint.at[where, :], qkv.at[:, aligned(c * rows, rows)],
                send.at[o], recv.at[o], {"ctx": dst},
            )
            copy.start()
            copies.append(copy)
    output_gather.relay()
    for copy in copies:
        copy.wait_recv()
    expand_gather.start()
    for at in range(0, total, 1024):
        keys[at : at + 1024, :] = transposed(qkv[hd : 2 * hd, at : at + 1024])

    def back(o, owner):
        return remote(stage.at[owner], land.at[c], osend.at[o], orecv.at[o], {"ctx": owner})

    def block(i, carry):
        o = 1 + i // per
        owner = lax.rem(c + o, nc)
        sub = lax.rem(i, per)
        where = aligned(owner * rows + sub * bq, bq)
        query = qkv[0:hd, where] * BF16(hd**-0.5)
        peak = None
        for at in range(0, total, bk):
            s = dot(keys[at : at + bk, :], query, 1, 0)
            scores[at : at + bk, :] = s
            high = jnp.max(s.reshape(bk // 8, 8, bq), axis=0)
            peak = high if peak is None else jnp.maximum(peak, high)
        peak = jnp.max(peak, axis=0, keepdims=True)
        acc, mass = None, None
        for at in range(0, total, bk):
            p = jnp.exp(scores[at : at + bk, :] - peak)
            low = jnp.sum(p.reshape(bk // 8, 8, bq), axis=0)
            mass = low if mass is None else mass + low
            term = dot(qkv[2 * hd : 3 * hd, at : at + bk], p.astype(BF16), 1, 0)
            acc = term if acc is None else acc + term
        mass = jnp.sum(mass, axis=0, keepdims=True)
        acc = acc * (1.0 / mass)
        out[:, where] = acc
        lse[:, where] = peak + jnp.log(mass)
        stage[owner, :, aligned(sub * bq, bq)] = acc.astype(BF16)

        @pl.when(jnp.logical_and(sub == per - 1, o < nc))
        def _():
            back(o, owner).start()

        @pl.when(i == 2)
        def _():
            expand_gather.relay_middle(0)
            expand_gather.relay_middle(1)

        @pl.when(i == per * nc - 3)
        def _():
            expand_gather.relay_rest(0)

        @pl.when(i == per * nc - 2)
        def _():
            expand_gather.relay_rest(1)
            shrink_gather.start()

        return carry

    lax.fori_loop(0, per * nc, block, 0)
    land[c] = stage[c]
    for o in range(1, nc):
        back(o, lax.rem(c + o, nc)).wait_recv()

    own = value.shape[0]
    deep_out = obuf.shape[1]
    output_gather.arrive()

    def piece(at):
        block_ = land[:, :, aligned(at * own, own)].reshape(nc * hd, own)
        weight = obuf[...].reshape(group * deep_out, nc * hd)
        return dot(block_.astype(F32).T.astype(BF16), weight, 1, 1)

    summing = Sum(sbuf, rbuf, tsend, trecv)
    summing.give(0, piece(far))
    summing.give(1, piece(partner))
    summing.pass_on(piece(cross))
    held = summing.near(piece(mine)) + bias[0:1, :]
    shrink_gather.relay_middle(0)
    shrink_gather.relay_middle(1)
    held = summing.total(held)
    value[...] = held
    gate = row_of(mod, 2 * width, width, part)
    shift = row_of(mod, 3 * width, width, part)
    scale = row_of(mod, 4 * width, width, part)
    mid = tok[aligned(mine * own, own), :].astype(F32) + gate * held
    middle[...] = mid
    hidden_two[mine] = (centred(mid)[0] * (1.0 + scale) + shift).astype(BF16)
    sharing = Share(hidden_two, gsend, grecv)
    sharing.start()
    shrink_gather.relay_rest(0)
    shrink_gather.relay_rest(1)
    sharing.relay()
    for o in range(1, nc):
        back(o, lax.rem(c + o, nc)).wait_send()
    for copy in pcopies + mcopies + copies:
        copy.wait_send()
    expand_gather.arrive()
    shrink_gather.arrive()
    for gather in (joint_gather, output_gather, expand_gather, shrink_gather):
        gather.drain()
    summing.drain()
    sharing.finish()


def forward(nf, nc, part, tok, jweight, cond, modw, cbias, offset, oweight, eweight, sweight, bias):
    rows, width = tok.shape
    deep, columns = jweight.shape
    group = nf * nc
    own = rows // 4
    total = rows * nc
    hd = HEAD_DIM
    bq = min(512, rows)
    return call(
        partial(forward_body, nf, nc, part),
        "forward",
        (
            shape((rows, width), BF16),
            shape((columns, width), BF16),
            shape((4,) + cbias.shape, F32),
            shape((group,) + oweight.shape, BF16),
            shape((3 * hd, total), BF16),
            shape((hd, total), F32),
            shape((1, total), F32),
            shape((nc, hd, rows), BF16),
            shape((group,) + eweight.shape, BF16),
            shape((own, width), F32),
            shape((own, width), F32),
            shape((4, own, width), BF16),
            shape((group,) + sweight.shape, BF16),
        ),
        [
            pltpu.VMEM((group, deep, columns), BF16),
            pltpu.VMEM((nf,) + cbias.shape, F32),
            pltpu.VMEM((group,) + cbias.shape, F32),
            pltpu.VMEM((rows, width), F32),
            pltpu.VMEM((columns, rows), BF16),
            pltpu.VMEM((nc, hd, rows), BF16),
            pltpu.VMEM((total, hd), BF16),
            pltpu.VMEM((total, bq), F32),
            pltpu.VMEM((3, own, width), BF16),
            pltpu.VMEM((3, own, width), BF16),
            DMA((group,)), DMA((group,)), DMA((4,)), DMA((4,)),
            DMA((nc,)), DMA((nc,)), DMA((nc,)), DMA((nc,)),
        ]
        + share_sems() * 2
        + gather_sems(nf, nc, 7),
        1,
        150,
        50,
    )(tok, jweight, cond, modw, cbias, offset, oweight, eweight, sweight, bias)


def branch_body(
    nf, nc, part, hidden, cot, expand, shrink, hbias, mod, middle, value,
    attn_low, mid_grad, shrink_parts, expand_grad, stats, hstats, sh_cross, sh_own,
    gbuf, abuf, ebuf, slopes, shrink_grad, sland, sbuf, rbuf, shold,
    tsend, trecv, send, recv, gsend, grecv, ssend, srecv,
):
    mine, partner, cross, far = tp_places()
    own, width = middle.shape
    deep = shrink_parts.shape[1]
    gate_first = row_of(mod, 2 * width, width, part)
    scale_second = row_of(mod, 4 * width, width, part)
    gate_second = row_of(mod, 5 * width, width, part)
    greet(ring_peers("tp", 4) + ring_peers("fsdp", nf))
    for at in range(4):
        where = pl.ds(at * own, own)
        grad = gate_second * cot[where, :].astype(F32)
        gbuf[where, :] = grad.astype(BF16)
        u = dot(hidden[at], expand[...], 1, 0) + hbias[...]
        squared = u * u
        th = jnp.tanh(GELU_SCALE * (u + GELU_CUBE * squared * u))
        abuf[where, :] = (0.5 * u * (1.0 + th)).astype(BF16)
        slopes[where, :] = 0.5 * (1.0 + th) + 0.5 * u * (1.0 - th * th) * (
            GELU_SCALE * (1.0 + 3.0 * GELU_CUBE * squared)
        )
    step = 256
    for at in range(0, width, step):
        block = dot(gbuf[:, at : at + step], abuf[...], 0, 0).astype(BF16)
        for k in range(at // deep, (at + step) // deep):
            shrink_grad[k // nc, k % nc] = block[k * deep - at : (k + 1) * deep - at, :]
    swaps = swap_copies(shrink_grad, sland, nf, ssend, srecv)
    for copy in swaps:
        copy.start()
    column = None
    copies = []
    summing = Sum(sbuf, rbuf, send, recv)
    held = None
    for turn, at in enumerate((far, partner, cross, mine)):
        where = aligned(at * own, own)
        pull = dot(gbuf[where, :], shrink[...], 1, 0) * slopes[where, :]
        tally = jnp.sum(pull, axis=0, keepdims=True)
        column = tally if column is None else column + tally
        pull = pull.astype(BF16)
        ebuf[where, :] = pull
        back = dot(pull, expand[...], 1, 1)
        if turn < 2:
            summing.give(turn, back)
        elif turn == 2:
            summing.pass_on(back)
        else:
            held = summing.near(back)
    hstats[...] = column
    for turn, at in enumerate((far, partner, cross, mine)):
        forth = dot(abuf[aligned(at * own, own), :], shrink[...], 1, 1)
        if turn < 2:
            shold[turn] = forth.astype(BF16)
            copy = remote(
                shold.at[turn], shold.at[2 + turn], tsend.at[turn], trecv.at[turn], {"tp": partner}
            )
            copy.start()
            copies.append(copy)
        elif turn == 2:
            copies[0].wait_recv()
            sh_cross[...] = (forth + shold[2].astype(F32)).astype(BF16)
        else:
            copies[1].wait_recv()
            sh_own[...] = forth + shold[3].astype(F32)
    mine_rows = cot[aligned(mine * own, own), :].astype(F32)
    stats[3:4, :] = jnp.sum(gate_second * mine_rows, axis=0, keepdims=True)
    normed, inverse = centred(middle[...])
    grad_in = summing.total(held)
    stats[0:1, :] = jnp.sum(grad_in, axis=0, keepdims=True)
    stats[1:2, :] = jnp.sum(grad_in * normed, axis=0, keepdims=True)
    mgrad = mine_rows + normal_back(grad_in * (1.0 + scale_second), normed, inverse)
    mid_grad[...] = mgrad
    agrad = gate_first * mgrad
    attn_low[mine] = agrad.astype(BF16)
    sharing = Share(attn_low, gsend, grecv)
    sharing.start()
    stats[2:3, :] = jnp.sum(mgrad * value[...], axis=0, keepdims=True)
    stats[4:5, :] = jnp.sum(agrad, axis=0, keepdims=True)
    stats[5:8, :] = jnp.zeros((3, width), F32)
    flat = hidden.shape[0] * own
    for at in range(0, width, step):
        expand_grad[at : at + step, :] = dot(
            hidden[:, :, at : at + step].reshape(flat, step), ebuf[...], 0, 0
        ).astype(BF16)
    sharing.relay()
    for copy in swaps:
        copy.wait_recv()
    swap_sum(shrink_grad, sland, shrink_parts, nf)
    sharing.finish()
    summing.drain()
    for copy in copies + swaps:
        copy.wait_send()


def branch(nf, nc, part, hidden, cot, expand, shrink, hbias, mod, middle, value):
    rows, width = cot.shape
    own = rows // 4
    units = expand.shape[1]
    deep = width // (nf * nc)
    return call(
        partial(branch_body, nf, nc, part),
        "branch",
        (
            shape((4, own, width), BF16),
            shape((own, width), F32),
            shape((nc, deep, units), BF16),
            shape((width, units), BF16),
            shape((8, width), F32),
            shape((1, units), F32),
            shape((own, width), BF16),
            shape((own, width), F32),
        ),
        [
            pltpu.VMEM((rows, width), BF16),
            pltpu.VMEM((rows, units), BF16),
            pltpu.VMEM((rows, units), BF16),
            pltpu.VMEM((rows, units), F32),
            pltpu.VMEM((nf, nc, deep, units), BF16),
            pltpu.VMEM((nf - 1, nc, deep, units), BF16),
            pltpu.VMEM((3, own, width), BF16),
            pltpu.VMEM((3, own, width), BF16),
            pltpu.VMEM((4, own, width), BF16),
            DMA((2,)), DMA((2,)),
        ]
        + share_sems() * 2
        + [DMA((nf,))] * 2,
        2,
        40,
        50,
    )(hidden, cot, expand, shrink, hbias, mod, middle, value)


def backward_body(
    nf, nc, part, attn_low, obuf, att, qkv, out, lse, sh_cross, sh_own, middle, cot, mod, bias,
    shrink_parts, expand_grad, weight_t, hidden, tok, mid_grad, stats_second, hidden_stats,
    modw, low,
    mixed, tokens_grad, shrink_sum, expand_sum, output_sum, joint_sum, modulate_sum,
    bias_rows, done,
    dout, dost, keys, vals, dq, stage, rland, wt, delta, output_grad, eland, oland,
    expand_parts, output_parts, sdeal, edeal, odeal, joint_grad, sbuf, rbuf, jgrad, jland,
    joint_parts, jdeal, pieces, land, total_piece, gathered, fland, ftotal, gate_row,
    send, recv, jsend, jrecv, csend, crecv, gsend, grecv, tsend, trecv, hsend, hrecv,
    esend, erecv, osend, orecv, nsend, nrecv,
    d1s, d1r, d2s, d2r, d3s, d3r, d4s, d4r, asend, arecv, bsend, brecv, f1s, f1r, f2s, f2r,
):
    f, c, t = lax.axis_index("fsdp"), lax.axis_index("ctx"), lax.axis_index("tp")
    mine, partner, cross, far = tp_places()
    own, width = middle.shape
    rows = cot.shape[0]
    total = rows * nc
    hd = HEAD_DIM
    inner, group = nc * 4, nf * nc
    here, slot = c * 4 + t, f * nc + c
    bk = bq = 512
    per = rows // bk
    deep = joint_sum.shape[0]
    heads_wide = nc * hd
    expand_swap = swap_copies(expand_grad, eland, nf, esend, erecv)
    output_swap = swap_copies(output_grad, oland, nf, osend, orecv)
    joint_swap = swap_copies(jgrad, jland, nf, nsend, nrecv)
    shrink_deal = deal_copies(shrink_parts, sdeal, nc, d1s, d1r)
    expand_deal = deal_copies(expand_parts, edeal, nc, d2s, d2r)
    output_deal = deal_copies(output_parts, odeal, nc, d3s, d3r)
    joint_deal = deal_copies(joint_parts, jdeal, nc, d4s, d4r)
    wt[...] = transposed(obuf[...].reshape(width, heads_wide))
    low_grad = attn_low[...].reshape(rows, width)
    dost[...] = dot(wt[...], low_grad, 1, 1).astype(BF16)
    greet(
        [
            {"ctx": lax.rem(here + o, inner) // 4, "tp": lax.rem(lax.rem(here + o, inner), 4)}
            for o in range(1, inner)
        ]
        + weight_peers(nf, nc)
    )
    copies = []
    for o in (2, 1, 3):
        dst = lax.rem(c + o, nc)
        copy = remote(
            dost.at[aligned(dst * hd, hd), :], dout.at[:, aligned(c * rows, rows)],
            send.at[o], recv.at[o], {"ctx": dst},
        )
        copy.start()
        copies.append(copy)
    for copy in expand_swap:
        copy.start()
    crossing = remote(sh_cross, rland, csend, crecv, {"tp": cross})
    crossing.start()
    for copy in shrink_deal:
        copy.start()
    dout[:, aligned(c * rows, rows)] = dost[aligned(c * hd, hd), :]
    flat = dot(att[...].reshape(heads_wide, rows), low_grad, 1, 0).T.astype(BF16)
    output_grad[...] = flat.reshape(output_grad.shape)
    for copy in output_swap:
        copy.start()
    for at in range(0, total, 1024):
        keys[at : at + 1024, :] = transposed(qkv[hd : 2 * hd, at : at + 1024])
        vals[at : at + 1024, :] = transposed(qkv[2 * hd : 3 * hd, at : at + 1024])
    dq[...] = jnp.zeros_like(dq)
    for copy in copies:
        copy.wait_recv()
    for at in range(0, total, 1024):
        delta[:, at : at + 1024] = jnp.sum(
            dout[:, at : at + 1024].astype(F32) * out[:, at : at + 1024], axis=0, keepdims=True
        )
    sharing = Share(mixed, gsend, grecv)

    def kv_back(o, owner):
        return remote(
            stage.at[owner, pl.ds(hd, 2 * hd), :], joint_grad.at[c, pl.ds(hd, 2 * hd), :],
            jsend.at[0, o], jrecv.at[0, o], {"ctx": owner},
        )

    def q_back(o, owner):
        return remote(
            stage.at[owner, pl.ds(0, hd), :], joint_grad.at[c, pl.ds(0, hd), :],
            jsend.at[1, o], jrecv.at[1, o], {"ctx": owner},
        )

    def block(i, vsum):
        o = 1 + i // per
        owner = lax.rem(c + o, nc)
        sub = lax.rem(i, per)
        where = aligned(owner * rows + sub * bk, bk)
        key, val, key_t = keys[where, :], vals[where, :], qkv[hd : 2 * hd, where]
        dk, dv = None, None
        for at in range(0, total, bq):
            query = qkv[0:hd, at : at + bq] * BF16(hd**-0.5)
            grad = dout[:, at : at + bq]
            p = jnp.exp(dot(key, query, 1, 0) - lse[:, at : at + bq])
            ds = (p * (dot(val, grad, 1, 0) - delta[:, at : at + bq])).astype(BF16)
            tv = dot(grad, p.astype(BF16), 1, 1)
            tk = dot(query, ds, 1, 1)
            dv = tv if dv is None else dv + tv
            dk = tk if dk is None else dk + tk
            dq[:, at : at + bq] += dot(key_t, ds, 1, 0)
        put = aligned(sub * bk, bk)
        stage[owner, hd : 2 * hd, put] = dk.astype(BF16)
        stage[owner, 2 * hd : 3 * hd, put] = dv.astype(BF16)

        @pl.when(jnp.logical_and(sub == per - 1, o < nc))
        def _():
            kv_back(o, owner).start()

        @pl.when(i == 2)
        def _():
            crossing.wait_recv()
            value = sh_own[...] + rland[...].astype(F32) + bias[1:2, :]
            gate = row_of(mod, 5 * width, width, part)
            mixed[mine] = (middle[...] + gate * value).astype(BF16)
            sharing.start()
            gate_row[...] = jnp.sum(
                cot[aligned(mine * own, own), :].astype(F32) * value, axis=0, keepdims=True
            )

        @pl.when(i == 5)
        def _():
            for copy in expand_swap + output_swap:
                copy.wait_recv()
            swap_sum(expand_grad, eland, expand_parts, nf)
            swap_sum(output_grad, oland, output_parts, nf)
            sharing.relay()

        return vsum + jnp.sum(dv, axis=1, keepdims=True)

    vsum = lax.fori_loop(0, per * nc, block, jnp.zeros((hd, 1), F32))
    qsum = jnp.zeros((hd, 1), F32)
    for o in (2, 1, 3, 0):
        owner = lax.rem(c + o, nc)
        piece = dq[:, aligned(owner * rows, rows)] * (hd**-0.5)
        qsum = qsum + jnp.sum(piece, axis=1, keepdims=True)
        stage[owner, 0:hd, :] = piece.astype(BF16)
        if o > 0:
            q_back(o, owner).start()
    for copy in output_deal + expand_deal:
        copy.start()
    joint_grad[c] = stage[c]
    bias_column = jnp.concatenate([qsum, vsum], axis=0)
    for copy in shrink_deal:
        copy.wait_recv()
    shrink_total = deal_sum(shrink_parts, sdeal, nc)
    shrink_sum[...] = shrink_total
    squares = jnp.sum(shrink_total * shrink_total)
    for o in range(1, nc):
        owner = lax.rem(c + o, nc)
        kv_back(o, owner).wait_recv()
        q_back(o, owner).wait_recv()

    columns = weight_t.shape[0]
    flat_grad = joint_grad[...].reshape(columns, rows)
    rows_f = width // nf
    step = max(128, min(256, rows_f))
    for o in range(1, nf + 1):
        member = lax.rem(f + o, nf)
        for at in range(0, rows_f, step):
            lanes = aligned(member * rows_f + at, step) if step % 128 == 0 else None
            block_ = dot(flat_grad, hidden[:, lanes], 1, 0).T.astype(BF16)
            for k in range(at // deep, (at + step) // deep):
                jgrad[member, k] = block_[k * deep - at : (k + 1) * deep - at, :]
        if o < nf:
            joint_swap[o - 1].start()

    def piece_of(at):
        block_ = joint_grad[:, :, aligned(at * own, own)].reshape(columns, own)
        return dot(block_.astype(F32).T.astype(BF16), weight_t[...], 1, 0)

    summing = Sum(sbuf, rbuf, tsend, trecv)
    summing.give(0, piece_of(far))
    summing.give(1, piece_of(partner))
    summing.pass_on(piece_of(cross))
    held = summing.near(piece_of(mine))
    normed, inverse = centred(tok[aligned(mine * own, own), :].astype(F32))
    for copy in output_deal:
        copy.wait_recv()
    output_total = deal_sum(output_parts, odeal, nc)
    output_sum[...] = output_total
    squares = squares + jnp.sum(output_total * output_total)
    grad_in = summing.total(held)
    scale = row_of(mod, width, width, part)
    shift_row = jnp.sum(grad_in, axis=0, keepdims=True)
    scale_row = jnp.sum(grad_in * normed, axis=0, keepdims=True)

    slim = part // nc // 128
    share = 2 * width // nc // 128
    hshare = hidden_stats.shape[1] // nc // 128
    last = slim + share + hshare
    vectors = [
        shift_row, scale_row, stats_second[2:3, :],
        stats_second[0:1, :], stats_second[1:2, :], gate_row[...],
    ]
    residual = [stats_second[4:5, :], stats_second[3:4, :]]
    pieces[...] = jnp.zeros_like(pieces)
    for cc in range(nc):
        for tt in range(4):
            k = cc * 4 + tt
            for n in range(slim):
                at = ((tt * part // 128) + cc * slim + n) * 128
                pieces[k, n : n + 1, :] = vectors[at // width][:, at % width : at % width + 128]
            for n in range(share):
                at = (cc * share + n) * 128
                pieces[k, slim + n : slim + n + 1, :] = residual[at // width][
                    :, at % width : at % width + 128
                ]
        for n in range(hshare):
            at = (cc * hshare + n) * 128
            pieces[cc * 4 + t, slim + share + n : slim + share + n + 1, :] = hidden_stats[
                :, at : at + 128
            ]
    pieces[here, last : last + 1, :] = jnp.broadcast_to(bias_column, (2 * hd, 128)).T[0:1, :]
    first = []
    for o in range(1, inner):
        other = lax.rem(here + o, inner)
        copy = remote(
            pieces.at[other], land.at[here], asend.at[o], arecv.at[o],
            {"ctx": other // 4, "tp": lax.rem(other, 4)},
        )
        copy.start()
        first.append(copy)
    tokens_grad[mine] = (
        mid_grad[...] + normal_back(grad_in * (1.0 + scale), normed, inverse)
    ).astype(BF16)
    token_share = Share(tokens_grad, hsend, hrecv)
    token_share.start()
    for copy in joint_swap:
        copy.wait_recv()
    swap_sum(jgrad, jland, joint_parts, nf)
    for copy in joint_deal:
        copy.start()
    land[here] = pieces[here]
    for copy in first:
        copy.wait_recv()
    acc = land[0]
    for k in range(1, inner):
        acc = acc + land[k]
    total_piece[...] = acc
    gathered[slot] = acc
    second = []
    for o, peer in zip(range(1, group), weight_peers(nf, nc)):
        copy = remote(total_piece, gathered.at[slot], bsend.at[o], brecv.at[o], peer)
        copy.start()
        second.append(copy)
    for copy in expand_deal:
        copy.wait_recv()
    expand_total = deal_sum(expand_parts, edeal, nc)
    expand_sum[...] = expand_total
    squares = squares + jnp.sum(expand_total * expand_total)
    for copy in second:
        copy.wait_recv()

    grads = []
    for latent in range(nf):
        strips = []
        for cc in range(nc):
            for n in range(slim):
                strips.append(gathered[latent * nc + cc, n : n + 1, :])
        grads.append(jnp.concatenate(strips, axis=1))
    condition_bias = grads[0]
    for latent in range(1, nf):
        condition_bias = condition_bias + grads[latent]
    bias_rows[...] = jnp.zeros_like(bias_rows)
    bias_rows[0:1, 0:part] = condition_bias
    factors = low[...].T
    wide = modw[...].astype(BF16).astype(F32)
    outer = None
    ftotal[...] = jnp.zeros_like(ftotal)
    for latent in range(nf):
        term = factors[:, latent : latent + 1] * grads[latent]
        outer = term if outer is None else outer + term
        column = jnp.sum(wide * grads[latent], axis=1, keepdims=True)
        ftotal[latent : latent + 1, 0:deep] = jnp.broadcast_to(column, (deep, 128)).T[0:1, :]
    modulate_sum[...] = outer
    squares = squares + jnp.sum(outer * outer)

    def over(at, count):
        found = []
        for cc in range(nc):
            value = None
            for latent in range(nf):
                block_ = gathered[latent * nc + cc, at : at + count, :]
                value = block_ if value is None else value + block_
            for n in range(count):
                found.append(value[n : n + 1, :])
        return jnp.concatenate(found, axis=1)

    residual_sum = over(slim, share)
    hidden_sum = over(slim + share, hshare)
    head_sum = over(last, 1)
    bias_rows[1:2, 0 : hidden_sum.shape[1]] = hidden_sum
    bias_rows[2:3, 0 : head_sum.shape[1]] = head_sum
    bias_rows[3:4, 0:width] = residual_sum[:, 0:width]
    bias_rows[4:5, 0:width] = residual_sum[:, width : 2 * width]
    lead = (slot == 0).astype(F32)
    tensor_lead = (t == 0).astype(F32)
    squares = squares + lead * (
        jnp.sum(condition_bias * condition_bias)
        + jnp.sum(hidden_sum * hidden_sum)
        + jnp.sum(head_sum * head_sum)
        + tensor_lead * jnp.sum(residual_sum * residual_sum)
    )
    token_share.relay()
    for copy in joint_deal:
        copy.wait_recv()
    joint = deal_sum(joint_parts, jdeal, nc)
    joint_sum[...] = joint
    squares = squares + jnp.sum(joint * joint)
    ftotal[nf : nf + 1, :] = jnp.full((1, 128), squares)
    third = []
    for o, peer in zip(range(1, 4), ring_peers("tp", 4)):
        copy = remote(ftotal, fland.at[t], f1s.at[o], f1r.at[o], peer)
        copy.start()
        third.append(copy)
    fland[t] = ftotal[...]
    for copy in third:
        copy.wait_recv()
    done[slot] = fland[0] + fland[1] + fland[2] + fland[3]
    fourth = []
    for o, peer in zip(range(1, group), weight_peers(nf, nc)):
        copy = remote(done.at[slot], done.at[slot], f2s.at[o], f2r.at[o], peer)
        copy.start()
        fourth.append(copy)
    sharing.finish()
    token_share.finish()
    summing.drain()
    for o in range(1, nc):
        owner = lax.rem(c + o, nc)
        kv_back(o, owner).wait_send()
        q_back(o, owner).wait_send()
    deals = shrink_deal + expand_deal + output_deal + joint_deal
    for copy in copies + [crossing] + expand_swap + output_swap + joint_swap + deals:
        copy.wait_send()
    for copy in fourth:
        copy.wait_recv()
    for copy in first + second + third + fourth:
        copy.wait_send()


def backward(
    nf, nc, part, attn_low, obuf, att, qkv, out, lse, sh_cross, sh_own, middle, cot, mod, bias,
    shrink_parts, expand_grad, weight_t, hidden, tok, mid_grad, stats_second, hidden_stats,
    modw, low,
):
    rows, width = cot.shape
    own = rows // 4
    total = rows * nc
    hd = HEAD_DIM
    inner, group = nc * 4, nf * nc
    deep = width // group
    units = expand_grad.shape[1]
    columns = weight_t.shape[0]
    heads_wide = nc * hd
    expand_grad = expand_grad.reshape(nf, nc, deep, units)
    high = -(-(part // nc + 2 * width // nc + hidden_stats.shape[1] // nc + 128) // 1024) * 8
    tall = -(-(nf + 1) // 8) * 8
    return call(
        partial(backward_body, nf, nc, part),
        "backward",
        (
            shape((4, own, width), BF16),
            shape((4, own, width), BF16),
            shape((deep, units), F32),
            shape((deep, units), F32),
            shape((deep, heads_wide), F32),
            shape((deep, columns), F32),
            shape((deep, part), F32),
            shape((8, max(part, width, hidden_stats.shape[1])), F32),
            shape((group, tall, 128), F32),
        ),
        [
            pltpu.VMEM((hd, total), BF16),
            pltpu.VMEM((heads_wide, rows), BF16),
            pltpu.VMEM((total, hd), BF16),
            pltpu.VMEM((total, hd), BF16),
            pltpu.VMEM((hd, total), F32),
            pltpu.VMEM((nc, 3 * hd, rows), BF16),
            pltpu.VMEM((own, width), BF16),
            pltpu.VMEM((heads_wide, width), BF16),
            pltpu.VMEM((1, total), F32),
            pltpu.VMEM((nf, nc, deep, heads_wide), BF16),
            pltpu.VMEM((nf - 1, nc, deep, units), BF16),
            pltpu.VMEM((nf - 1, nc, deep, heads_wide), BF16),
            pltpu.VMEM((nc, deep, units), BF16),
            pltpu.VMEM((nc, deep, heads_wide), BF16),
            pltpu.VMEM((nc - 1, deep, units), BF16),
            pltpu.VMEM((nc - 1, deep, units), BF16),
            pltpu.VMEM((nc - 1, deep, heads_wide), BF16),
            pltpu.VMEM((nc, 3 * hd, rows), BF16),
            pltpu.VMEM((3, own, width), BF16),
            pltpu.VMEM((3, own, width), BF16),
            pltpu.VMEM((nf, nc, deep, columns), BF16),
            pltpu.VMEM((nf - 1, nc, deep, columns), BF16),
            pltpu.VMEM((nc, deep, columns), BF16),
            pltpu.VMEM((nc - 1, deep, columns), BF16),
            pltpu.VMEM((inner, high, 128), F32),
            pltpu.VMEM((inner, high, 128), F32),
            pltpu.VMEM((high, 128), F32),
            pltpu.VMEM((group, high, 128), F32),
            pltpu.VMEM((4, tall, 128), F32),
            pltpu.VMEM((tall, 128), F32),
            pltpu.VMEM((1, width), F32),
            DMA((nc,)), DMA((nc,)), DMA((2, nc)), DMA((2, nc)),
            DMA, DMA,
        ]
        + share_sems() * 3
        + [DMA((nf,))] * 6
        + [DMA((nc,))] * 8
        + [DMA((inner,))] * 2
        + [DMA((group,))] * 2
        + [DMA((4,))] * 2
        + [DMA((group,))] * 2,
        3,
        150,
        56,
    )(
        attn_low, obuf, att, qkv, out, lse, sh_cross, sh_own, middle, cot, mod, bias,
        shrink_parts, expand_grad, weight_t, hidden, tok, mid_grad, stats_second, hidden_stats,
        modw, low,
    )


def update(master, first, root, gradient, clip, decay_rate):
    scaled = clip * gradient
    first_moment = first_decay * first + (1.0 - first_decay) * scaled
    second_moment = second_decay * root * root + (1.0 - second_decay) * scaled * scaled
    new_root = jnp.sqrt(second_moment)
    first_hat = first_moment * (1.0 / (1.0 - first_decay**ADAM_STEP))
    second_hat = second_moment * (1.0 / (1.0 - second_decay**ADAM_STEP))
    updated = master - learning_rate * (
        first_hat / (jnp.sqrt(second_hat) + adam_epsilon) + decay_rate * master
    )
    return updated, first_moment, new_root


def adam_body(count, nf, nc, done, condition, bias_rows, *refs):
    grads = refs[:count]
    masters = refs[count : 2 * count]
    moments = refs[2 * count : 3 * count]
    smalls = refs[3 * count : 3 * count + 8]
    outs = refs[3 * count + 8 :]
    news = outs[:count]
    averages = outs[count : 2 * count]
    small_outs = outs[2 * count : 2 * count + 8]
    condition_grad, norm = outs[2 * count + 8 : 2 * count + 10]
    scratch = outs[2 * count + 10 :]
    wbufs = scratch[:count]
    mbufs = scratch[count : 2 * count]
    gbufs = scratch[2 * count : 3 * count]
    isem, osem = scratch[3 * count :]
    group = nf * nc
    f = lax.axis_index("fsdp")
    loads, stores = [], []
    for k in range(count):
        loads.append(
            (
                pltpu.make_async_copy(masters[k], wbufs[k], isem.at[0, k]),
                pltpu.make_async_copy(moments[k], mbufs[k], isem.at[1, k]),
                pltpu.make_async_copy(grads[k], gbufs[k], isem.at[2, k]),
            )
        )
        stores.append(
            (
                pltpu.make_async_copy(wbufs[k], news[k], osem.at[0, k]),
                pltpu.make_async_copy(mbufs[k], averages[k], osem.at[1, k]),
            )
        )
    for trio in loads:
        for copy in trio:
            copy.start()
    squares = done[0, nf : nf + 1, 0:1]
    for k in range(1, group):
        squares = squares + done[k, nf : nf + 1, 0:1]
    grad_norm = jnp.sqrt(squares)
    norm[...] = grad_norm
    clip = jnp.minimum(1.0, clip_limit / (grad_norm + 1e-06))
    deep = condition.shape[1] // group
    found = [done[k, pl.ds(f, 1), 0:deep] for k in range(group)]
    v = condition[pl.ds(f, 1), :]
    gate = 1.0 / (1.0 + jnp.exp(-v))
    condition_grad[...] = jnp.concatenate(found, axis=1) * (gate * (1.0 + v * (1.0 - gate)))
    for k in range(4):
        master, moment = smalls[2 * k], smalls[2 * k + 1]
        if k < 3:
            row = (2, 1, 0)[k]
            grad = bias_rows[row : row + 1, 0 : master.shape[1]]
            new, first, root = update(master[...], moment[0:1, :], moment[1:2, :], grad, clip, 0.0)
            small_outs[2 * k][...] = new
            small_outs[2 * k + 1][0:1, :] = first
            small_outs[2 * k + 1][1:2, :] = root
        else:
            grad = bias_rows[3:5, 0 : master.shape[1]]
            new, first, root = update(master[...], moment[0], moment[1], grad, clip, 0.0)
            small_outs[2 * k][...] = new
            small_outs[2 * k + 1][0] = first
            small_outs[2 * k + 1][1] = root
    for k in range(count):
        for copy in loads[k]:
            copy.wait()
        deep_k = wbufs[k].shape[0]
        step = min(16, deep_k)

        def rows(i, carry, k=k, step=step):
            at = pl.ds(pl.multiple_of(i * step, step), step)
            new, first, root = update(
                wbufs[k][at, :], mbufs[k][0, at, :], mbufs[k][1, at, :], gbufs[k][at, :],
                clip, weight_decay,
            )
            wbufs[k][at, :] = new
            mbufs[k][0, at, :] = first
            mbufs[k][1, at, :] = root
            return carry

        lax.fori_loop(0, deep_k // step, rows, 0)
        for copy in stores[k]:
            copy.start()
    for pair in stores:
        for copy in pair:
            copy.wait()


def adam(nf, nc, done, condition, bias_rows, grads, masters, moments, smalls):
    count = len(grads)
    anywhere = pl.BlockSpec(memory_space=pl.ANY)
    small_shapes = tuple(shape(a.shape, F32) for a in smalls)
    outs = (
        tuple(shape(m.shape, F32) for m in masters)
        + tuple(shape(m.shape, F32) for m in moments)
        + small_shapes
        + (shape((1, condition.shape[1]), F32), shape((1, 1), F32))
    )
    return pl.pallas_call(
        partial(adam_body, count, nf, nc),
        out_shape=outs,
        in_specs=vmem(3) + [anywhere] * (3 * count) + vmem(8),
        out_specs=[anywhere] * (2 * count) + vmem(10),
        scratch_shapes=[pltpu.VMEM(m.shape, F32) for m in masters]
        + [pltpu.VMEM(m.shape, F32) for m in moments]
        + [pltpu.VMEM(m.shape, F32) for m in masters]
        + [DMA((3, count)), DMA((2, count))],
        compiler_params=pltpu.CompilerParams(vmem_limit_bytes=32 << 20),
        cost_estimate=cost(10),
        name="adam",
    )(done, condition, bias_rows, *grads, *masters, *moments, *smalls)


def local(
    nf,
    nc,
    tokens,
    condition,
    cotangent,
    joint_weight,
    joint_moments,
    output_weight,
    output_moments,
    expand_weight,
    expand_moments,
    shrink_weight,
    shrink_moments,
    modulate_weight,
    modulate_moments,
    attention_bias,
    attention_moments,
    hidden_bias,
    hidden_moments,
    condition_bias,
    condition_moments,
    residual_bias,
    residual_moments,
):
    latent_count, rows, width = tokens.shape
    heads = joint_weight.shape[1] // (3 * HEAD_DIM)
    assert latent_count == 1 and heads == nc and lax.axis_size("tp") == 4
    f, c, t = lax.axis_index("fsdp"), lax.axis_index("ctx"), lax.axis_index("tp")
    mine = f * nc + c
    deep, part = modulate_weight.shape
    units = expand_weight.shape[1]
    tok, cot = tokens[0], cotangent[0]

    condition_low = jax.nn.silu(condition).astype(BF16)
    condition_here = lax.dynamic_slice_in_dim(condition_low, mine * deep, deep, 1)
    strips = part // 128
    high = -(-strips // 8) * 8
    bias_strips = jnp.pad(condition_bias.reshape(strips, 128), ((0, high - strips), (0, 0)))
    bias_pairs = attention_bias.reshape(heads, 2, HEAD_DIM)
    offset = jnp.stack(
        [bias_pairs[:, 0], jnp.zeros_like(bias_pairs[:, 0]), bias_pairs[:, 1]], axis=1
    ).reshape(-1, 1)
    condition_pad = jnp.pad(condition_here, ((0, 16 - nf), (0, 0)))
    (
        hidden_first, joint_full_t, mod, output_full, qkv, out, lse, att, expand_full,
        value, middle, hidden_second, shrink_full,
    ) = forward(
        nf, nc, part, tok, joint_weight, condition_pad, modulate_weight, bias_strips, offset,
        output_weight, expand_weight, shrink_weight, residual_bias,
    )
    (
        attn_low, mid_grad, shrink_parts, expand_grad, stats_second, hidden_stats,
        sh_cross, sh_own,
    ) = branch(
        nf, nc, part, hidden_second, cot, expand_full.reshape(width, units),
        shrink_full.reshape(width, units), hidden_bias[None, :], mod, middle, value,
    )
    (
        mixed, tokens_grad, shrink_sum, expand_sum, output_sum, joint_sum, modulate_sum,
        bias_rows, done,
    ) = backward(
        nf, nc, part, attn_low, output_full, att, qkv, out, lse, sh_cross, sh_own, middle, cot,
        mod, residual_bias, shrink_parts, expand_grad, joint_full_t, hidden_first, tok, mid_grad,
        stats_second, hidden_stats, modulate_weight, condition_pad.astype(F32),
    )
    weights = (joint_weight, output_weight, expand_weight, shrink_weight, modulate_weight)
    moments = (joint_moments, output_moments, expand_moments, shrink_moments, modulate_moments)
    grads = (joint_sum, output_sum, expand_sum, shrink_sum, modulate_sum)
    smalls = (
        attention_bias[None, :], attention_moments, hidden_bias[None, :], hidden_moments,
        condition_bias[None, :], condition_moments, residual_bias, residual_moments,
    )
    results = adam(nf, nc, done, condition, bias_rows, grads, weights, moments, smalls)
    updated = []
    for k in range(5):
        updated += [results[k], results[5 + k]]
    for k in range(4):
        new = results[10 + 2 * k]
        updated += [new[0] if k < 3 else new, results[11 + 2 * k]]
    return (
        mixed.reshape(1, rows, width),
        tokens_grad.reshape(1, rows, width).astype(F32),
        results[18],
        results[19][0, 0],
    ) + tuple(updated)


def solution(mesh):
    rows = P(("fsdp", "ctx"), "tp")
    pair = P(None, ("fsdp", "ctx"), "tp")
    tokens = P("fsdp", "ctx", None)
    small = (P("tp"), P(None, "tp"))
    return jax.shard_map(
        partial(local, mesh.shape["fsdp"], mesh.shape["ctx"]),
        mesh=mesh,
        in_specs=(tokens, P(), tokens) + (rows, pair) * 5 + small * 3 + (P(), P()),
        out_specs=(tokens, tokens, P("fsdp", None), P())
        + (rows, pair) * 5
        + small * 3
        + (P(), P()),
        check_vma=False,
    )
```

```python
from functools import partial

import jax
import jax.numpy as jnp
from jax import lax
from jax.experimental import pallas as pl
from jax.experimental.pallas import tpu as pltpu
from jax.sharding import PartitionSpec as P

HEAD_DIM = 64
ADAM_STEP = 10
F32 = jnp.float32
BF16 = jnp.bfloat16
MESH = pl.DeviceIdType.MESH
DMA = pltpu.SemaphoreType.DMA

norm_epsilon = 1e-06
first_decay = 0.9
second_decay = 0.999
adam_epsilon = 1e-08
learning_rate = 0.05
weight_decay = 0.1
clip_limit = 1.0
GELU_SCALE = 0.7978845608028654
GELU_CUBE = 0.044715


def dot(a, b, ca, cb):
    return lax.dot_general(a, b, (((ca,), (cb,)), ((), ())), preferred_element_type=F32)


def aligned(start, size):
    return pl.ds(pl.multiple_of(start, size), size)


def greet(peers):
    barrier = pltpu.get_barrier_semaphore()
    for peer in peers:
        pl.semaphore_signal(barrier, inc=1, device_id=peer, device_id_type=MESH)
    pl.semaphore_wait(barrier, len(peers))


def remote(source, target, send_sem, recv_sem, peer):
    return pltpu.make_async_remote_copy(
        src_ref=source,
        dst_ref=target,
        send_sem=send_sem,
        recv_sem=recv_sem,
        device_id=peer,
        device_id_type=MESH,
    )


def vmem(count):
    return [pl.BlockSpec(memory_space=pltpu.VMEM)] * count


def shape(dims, dtype):
    return jax.ShapeDtypeStruct(dims, dtype)


def cost(micros, flops=0):
    return pl.CostEstimate(flops=flops, bytes_accessed=int(micros * 3.0e6), transcendentals=0)


def call(body, name, outs, scratch, ident, micros, megabytes, ins=(), to=()):
    def run(*args):
        return pl.pallas_call(
            body,
            out_shape=outs,
            in_specs=[pl.BlockSpec(memory_space=pltpu.HBM if k in ins else pltpu.VMEM) for k in range(len(args))],
            out_specs=[pl.BlockSpec(memory_space=pltpu.HBM if k in to else pltpu.VMEM) for k in range(len(outs))],
            scratch_shapes=scratch,
            compiler_params=pltpu.CompilerParams(
                collective_id=ident, has_side_effects=True, vmem_limit_bytes=megabytes << 20
            ),
            cost_estimate=cost(micros),
            name=name,
        )(*args)

    return run


def transposed(block):
    return block.astype(F32).T.astype(BF16)


def row_of(mod, start, width, part):
    pieces = []
    for at in range(start, start + width, 128):
        pieces.append(mod[at // part, pl.ds((at % part) // 128, 1), :])
    return jnp.concatenate(pieces, axis=1)


def centred(values):
    center = values - jnp.mean(values, axis=-1, keepdims=True)
    inverse = lax.rsqrt(jnp.mean(center * center, axis=-1, keepdims=True) + norm_epsilon)
    return center * inverse, inverse


def normal_back(grad, normed, inverse):
    return inverse * (
        grad
        - jnp.mean(grad, axis=-1, keepdims=True)
        - normed * jnp.mean(grad * normed, axis=-1, keepdims=True)
    )


class Gather:
    def __init__(self, buf, nf, nc, sems, parts, first=0):
        self.buf, self.nf, self.nc, self.sems = buf, nf, nc, sems
        self.first, self.parts = first, range(first, parts)
        self.columns = buf.shape[2] // parts

    def sem(self, part, kind):
        return self.sems[4 * (part - self.first) + kind]

    def view(self, ctx, part):
        slot = lax.axis_index("fsdp") * self.nc + ctx
        return self.buf.at[slot, :, pl.ds(part * self.columns, self.columns)]

    def along(self, o, part):
        c = lax.axis_index("ctx")
        zs, zr = self.sem(part, 0), self.sem(part, 1)
        view = self.view(c, part)
        return remote(view, view, zs.at[o], zr.at[o], {"ctx": lax.rem(c + o, self.nc)})

    def onward(self, part):
        c = lax.axis_index("ctx")
        zs, zr = self.sem(part, 0), self.sem(part, 1)
        view = self.view(lax.rem(c + 2, self.nc), part)
        up = remote(view, view, zs.at[0], zr.at[3], {"ctx": lax.rem(c + 1, self.nc)})
        down = remote(view, view, zs.at[0], zr.at[1], {"ctx": lax.rem(c + 3, self.nc)})
        return up, down

    def across(self, o, part):
        f, c = lax.axis_index("fsdp"), lax.axis_index("ctx")
        xs, xr = self.sem(part, 2), self.sem(part, 3)
        view = self.view(lax.rem(c - o + self.nc, self.nc), part)
        return [
            remote(view, view, xs.at[fo, o], xr.at[fo, o], {"fsdp": lax.rem(f + fo, self.nf)})
            for fo in range(1, self.nf)
        ]

    def start(self):
        c = lax.axis_index("ctx")
        for part in self.parts:
            self.along(2, part).start()
            pl.when(c != 3)(self.along(1, part).start)
            pl.when(c != 0)(self.along(3, part).start)
            for copy in self.across(0, part):
                copy.start()

    def relay_middle(self, part):
        c = lax.axis_index("ctx")
        self.along(2, part).wait_recv()
        up, down = self.onward(part)
        pl.when(c == 2)(up.start)
        pl.when(c == 1)(down.start)
        for copy in self.across(2, part):
            copy.start()

    def relay_rest(self, part):
        for o in (1, 3):
            self.along(o, part).wait_recv()
            for copy in self.across(o, part):
                copy.start()

    def relay(self):
        for part in self.parts:
            self.relay_middle(part)
        for part in self.parts:
            self.relay_rest(part)

    def arrive(self):
        for part in self.parts:
            for o in range(self.nc):
                for copy in self.across(o, part):
                    copy.wait_recv()

    def drain(self):
        c = lax.axis_index("ctx")
        for part in self.parts:
            for o in range(self.nc):
                for copy in self.across(o, part):
                    copy.wait_send()
            up, down = self.onward(part)
            self.along(2, part).wait_send()
            pl.when(c != 3)(self.along(1, part).wait_send)
            pl.when(c != 0)(self.along(3, part).wait_send)
            pl.when(c == 2)(up.wait_send)
            pl.when(c == 1)(down.wait_send)


def gather_sems(nf, nc, parts):
    return [DMA((nc,)), DMA((nc,)), DMA((nf, nc)), DMA((nf, nc))] * parts


class Sum:
    def __init__(self, sbuf, rbuf, send, recv):
        self.sbuf, self.rbuf, self.send, self.recv = sbuf, rbuf, send, recv
        self.places = tp_places()

    def copy(self, k):
        mine, partner, cross, far = self.places
        peer = cross if k == 2 else partner
        return remote(
            self.sbuf.at[k], self.rbuf.at[k], self.send.at[k], self.recv.at[k], {"tp": peer}
        )

    def give(self, k, value):
        self.sbuf[k] = value.astype(BF16)
        self.copy(k).start()

    def pass_on(self, value):
        self.copy(0).wait_recv()
        self.give(2, value + self.rbuf[0].astype(F32))

    def near(self, value):
        self.copy(1).wait_recv()
        return value + self.rbuf[1].astype(F32)

    def total(self, value):
        self.copy(2).wait_recv()
        return value + self.rbuf[2].astype(F32)

    def drain(self):
        for k in range(3):
            self.copy(k).wait_send()


class Share:
    def __init__(self, slots, send, recv):
        self.slots, self.send, self.recv = slots, send, recv
        self.places = tp_places()

    def copy(self, k):
        mine, partner, cross, far = self.places
        slot, peer = ((mine, cross), (mine, partner), (cross, partner))[k]
        view = self.slots.at[slot]
        return remote(view, view, self.send.at[k], self.recv.at[k], {"tp": peer})

    def start(self):
        self.copy(0).start()
        self.copy(1).start()

    def relay(self):
        self.copy(0).wait_recv()
        self.copy(2).start()

    def finish(self):
        self.copy(1).wait_recv()
        self.copy(2).wait_recv()
        for k in range(3):
            self.copy(k).wait_send()


def share_sems():
    return [DMA((3,)), DMA((3,))]


class Scatter:
    def __init__(self, nf, nc, grad, parts, xland, zland, xsend, xrecv, zsend, zrecv, lanes=None):
        f, c = lax.axis_index("fsdp"), lax.axis_index("ctx")
        self.nf, self.nc, self.grad, self.parts, self.xland, self.zland = (
            nf, nc, grad, parts, xland, zland,
        )
        self.lanes = slice(None) if lanes is None else pl.ds(*lanes)
        keep = self.lanes
        self.swaps, self.deals = [], []
        for fo in range(1, nf) if grad is not None else ():
            member = lax.rem(f + fo, nf)
            self.swaps.append(
                remote(
                    grad.at[member, :, :, keep], xland.at[fo - 1, :, :, keep],
                    xsend.at[fo], xrecv.at[fo], {"fsdp": member},
                )
            )
        for o in (2, 1, 3):
            member = lax.rem(c + o, nc)
            self.deals.append(
                remote(
                    parts.at[member, :, keep], zland.at[o - 1, :, keep], zsend.at[o], zrecv.at[o],
                    {"ctx": member},
                )
            )

    def swap(self):
        for copy in self.swaps:
            copy.start()

    def swapped(self):
        f = lax.axis_index("fsdp")
        for copy in self.swaps:
            copy.wait_recv()
        for k in range(self.nc):
            total = self.grad[f, k, :, self.lanes].astype(F32)
            for fo in range(1, self.nf):
                total = total + self.xland[fo - 1, k, :, self.lanes].astype(F32)
            self.parts[k, :, self.lanes] = total.astype(BF16)

    def deal(self):
        for copy in self.deals:
            copy.start()

    def dealt(self):
        for copy in self.deals:
            copy.wait_recv()
        total = self.parts[lax.axis_index("ctx"), :, self.lanes].astype(F32)
        for o in range(1, self.nc):
            total = total + self.zland[o - 1, :, self.lanes].astype(F32)
        return total

    def drain(self, swaps=True, deals=True):
        for copy in (self.swaps if swaps else []) + (self.deals if deals else []):
            copy.wait_send()


def ring_peers(axis, size):
    here = lax.axis_index(axis)
    return [{axis: lax.rem(here + o, size)} for o in range(1, size)]


def weight_peers(nf, nc):
    f, c = lax.axis_index("fsdp"), lax.axis_index("ctx")
    peers = []
    for o in range(1, nf * nc):
        other = lax.rem(f * nc + c + o, nf * nc)
        peers.append({"fsdp": other // nc, "ctx": lax.rem(other, nc)})
    return peers


def all_peers(nf, nc):
    f, c, t = lax.axis_index("fsdp"), lax.axis_index("ctx"), lax.axis_index("tp")
    count = nf * nc * 4
    peers = []
    for o in range(1, count):
        other = lax.rem((f * nc + c) * 4 + t + o, count)
        peers.append(
            {"fsdp": other // (nc * 4), "ctx": lax.rem(other // 4, nc), "tp": lax.rem(other, 4)}
        )
    return peers


def turned(mine, turn):
    high = lax.rem(mine // 2 + turn // 2, 2)
    return high * 2 + lax.rem(mine + turn, 2)


def tp_places():
    mine = lax.axis_index("tp")
    partner = mine + 1 - 2 * lax.rem(mine, 2)
    cross = lax.rem(mine + 2, 4)
    far = lax.rem(partner + 2, 4)
    return mine, partner, cross, far


def load_all(pairs, sems):
    copies = []
    for k, (source, target) in enumerate(pairs):
        copy = pltpu.make_async_copy(source, target, sems.at[k])
        copy.start()
        copies.append(copy)
    return copies


def head_peers(nc):
    c, t = lax.axis_index("ctx"), lax.axis_index("tp")
    inner = nc * 4
    peers = []
    for o in range(1, inner):
        other = lax.rem(c * 4 + t + o, inner)
        peers.append({"ctx": other // 4, "tp": lax.rem(other, 4)})
    return peers


def forward_body(
    nf, nc, part, tok_hbm, jw_hbm, cond, modw_hbm, cbias, offset, ow_hbm, ew_hbm, bias, sw_hbm,
    hidden_hbm, weight_hbm, mod, out_t_hbm, qkv_hbm, out_hbm, lse, land_hbm, ebuf_hbm,
    value, middle, hidden_two_hbm, sbuf_hbm,
    sweight, sbuf, tok, jweight, modw, oweight, eweight, out_t, qkv, out, ebuf, hidden_two,
    hidden, weight_t, wbuf, obuf, oall, pbuf, pland, normed, joint, stage, land, keys, scores,
    lsem, ssem, psend, precv, msend, mrecv, send, recv, osend, orecv, hsend, hrecv, asend, arecv,
    *gsems,
):
    f, c, t = lax.axis_index("fsdp"), lax.axis_index("ctx"), lax.axis_index("tp")
    mine, partner, cross, far = tp_places()
    group = nf * nc
    slot = f * nc + c
    rows, width = tok.shape
    own = rows // 4
    strips = part // 128
    hd = HEAD_DIM
    step = 128
    loads = load_all(
        (
            (jw_hbm, jweight), (modw_hbm, modw), (tok_hbm, tok), (ow_hbm, oweight),
            (ew_hbm, eweight), (sw_hbm.at[:, pl.ds(0, sweight.shape[1])], sweight),
        ),
        lsem,
    )
    joint_gather = Gather(wbuf, nf, nc, gsems[0:8], 2)
    output_gather = Gather(obuf, nf, nc, gsems[8:12], 1)
    expand_gather = Gather(ebuf, nf, nc, gsems[12:20], 2)
    shrink_gather = Gather(sbuf, nf, nc, gsems[20:24], 1)
    loads[0].wait()
    wbuf[slot] = jweight[...].astype(BF16)
    greet(weight_peers(nf, nc) + head_peers(nc))
    joint_gather.start()
    loads[1].wait()
    partial_mod = dot(cond[...], modw[...].astype(BF16), 1, 0)
    for latent in range(nf):
        for k in range(strips):
            pbuf[latent, pl.ds(k, 1), :] = partial_mod[latent : latent + 1, 128 * k : 128 * k + 128]
    pcopies = []
    for o, peer in zip(range(1, group), weight_peers(nf, nc)):
        copy = remote(pbuf.at[peer["fsdp"]], pland.at[slot], psend.at[o], precv.at[o], peer)
        copy.start()
        pcopies.append(copy)
    pland[slot] = pbuf[f]
    loads[2].wait()

    def norm_rows(k, carry):
        at = aligned(k * step, step)
        normed[at, :] = centred(tok[at, :].astype(F32))[0]
        return carry

    lax.fori_loop(0, rows // 2 // step, norm_rows, 0)
    joint_gather.relay_middle(0)
    lax.fori_loop(rows // 2 // step, rows // step, norm_rows, 0)
    joint_gather.relay_middle(1)
    for copy in pcopies:
        copy.wait_recv()
    total_mod = pland[0]
    for k in range(1, group):
        total_mod = total_mod + pland[k]
    mod[t] = total_mod + cbias[...]
    mcopies = []
    for o, peer in zip(range(1, 4), ring_peers("tp", 4)):
        copy = remote(mod.at[t], mod.at[t], msend.at[o], mrecv.at[o], peer)
        copy.start()
        mcopies.append(copy)
    joint_gather.relay_rest(0)
    for copy in loads[3:]:
        copy.wait()
    obuf[slot] = oweight[...].astype(BF16)
    ebuf[slot] = eweight[...].astype(BF16)
    sbuf[slot] = sweight[...].astype(BF16)
    for copy in mcopies:
        copy.wait_recv()
    shift = row_of(mod, 0, width, part)
    scale = row_of(mod, width, width, part)

    def hide_rows(k, carry):
        at = aligned(k * step, step)
        hidden[at, :] = (normed[at, :] * (1.0 + scale) + shift).astype(BF16)
        return carry

    lax.fori_loop(0, rows // step, hide_rows, 0)
    joint_gather.relay_rest(1)
    output_gather.start()
    joint_gather.arrive()
    deep = jweight.shape[0]
    for k in range(group):
        weight_t[:, k * deep : (k + 1) * deep] = transposed(wbuf[k])

    total = rows * nc
    bq, bk = scores.shape[1], 512
    per = rows // bq

    def query_copy(o):
        dst = lax.rem(c + o, nc)
        return remote(
            joint.at[aligned(dst * 3 * hd, hd), :], qkv.at[pl.ds(0, hd), aligned(c * rows, rows)],
            send.at[1, o], recv.at[1, o], {"ctx": dst},
        )

    copies = []
    for o in (2, 1, 3, 0):
        dst = lax.rem(c + o, nc)
        where = aligned(dst * 3 * hd, 3 * hd)
        head = (dot(weight_t[where, :], hidden[...], 1, 1) + offset[where, :]).astype(BF16)
        if o == 0:
            qkv[:, aligned(c * rows, rows)] = head
        else:
            joint[where, :] = head
            copy = remote(
                joint.at[pl.ds(pl.multiple_of(dst * 3 * hd + hd, hd), 2 * hd), :],
                qkv.at[pl.ds(hd, 2 * hd), aligned(c * rows, rows)],
                send.at[0, o], recv.at[0, o], {"ctx": dst},
            )
            copy.start()
            copies.append(copy)
    for o in (2, 1, 3):
        query_copy(o).start()
    saves = [
        pltpu.make_async_copy(source, target, ssem.at[k])
        for k, (source, target) in enumerate(
            (
                (hidden, hidden_hbm), (weight_t, weight_hbm), (out_t, out_t_hbm), (qkv, qkv_hbm),
                (out, out_hbm), (land, land_hbm), (ebuf, ebuf_hbm), (sbuf, sbuf_hbm),
                (hidden_two, hidden_two_hbm),
            )
        )
    ]
    saves[0].start()
    saves[1].start()
    output_gather.relay()
    output_gather.arrive()
    oall[mine] = obuf[...].reshape(width, nc * hd)
    weights_share = Share(oall, asend, arecv)
    weights_share.start()
    for copy in copies:
        copy.wait_recv()
    expand_gather.start()
    for at in range(0, total, 1024):
        keys[at : at + 1024, :] = transposed(qkv[hd : 2 * hd, at : at + 1024])

    def given(o, k):
        owner, tt = lax.rem(c - o + nc, nc), lax.rem(t + k, 4)
        return remote(
            stage.at[owner, :, aligned(tt * own, own)], land.at[t, c],
            osend.at[o, k], orecv.at[o, k], {"ctx": owner, "tp": tt},
        )

    def block(i, carry):
        turn, sub = i // per, lax.rem(i, per)
        o = jnp.where(turn > 0, 1 + lax.rem(turn, 3), 0)
        owner = lax.rem(c - o + nc, nc)

        @pl.when(jnp.logical_and(sub == 0, turn > 0))
        def _():
            query_copy(o).wait_recv()

        @pl.when(i == 2 * per)
        def _():
            expand_gather.relay_middle(0)
            expand_gather.relay_middle(1)

        @pl.when(i == 3 * per)
        def _():
            expand_gather.relay_rest(0)
            expand_gather.relay_rest(1)
            shrink_gather.start()
            saves[3].start()

        where = aligned(owner * rows + sub * bq, bq)
        query = qkv[0:hd, where] * BF16(hd**-0.5)
        peak = None
        for at in range(0, total, bk):
            s = dot(keys[at : at + bk, :], query, 1, 0)
            scores[at : at + bk, :] = s
            high = jnp.max(s.reshape(bk // 8, 8, bq), axis=0)
            peak = high if peak is None else jnp.maximum(peak, high)
        peak = jnp.max(peak, axis=0, keepdims=True)
        acc, mass = None, None
        for at in range(0, total, bk):
            p = jnp.exp(scores[at : at + bk, :] - peak)
            low = jnp.sum(p.reshape(bk // 8, 8, bq), axis=0)
            mass = low if mass is None else mass + low
            term = dot(qkv[2 * hd : 3 * hd, at : at + bk], p.astype(BF16), 1, 0)
            acc = term if acc is None else acc + term
        mass = jnp.sum(mass, axis=0, keepdims=True)
        acc = acc * (1.0 / mass)
        out[:, where] = acc
        lse[:, where] = peak + jnp.log(mass)
        stage[owner, :, aligned(sub * bq, bq)] = acc.astype(BF16)

        @pl.when(sub == per - 1)
        def _():
            pl.when(turn > 0)(given(o, 0).start)
            for k in range(1, 4):
                given(o, k).start()

        @pl.when(i == per - 1)
        def _():
            weights_share.relay()

        @pl.when(i == 2 * per - 1)
        def _():
            weights_share.finish()
            for k in range(4):
                out_t[k] = transposed(oall[k])
            saves[2].start()

        return carry

    lax.fori_loop(0, per * nc, block, 0)
    land[t, c] = stage[c, :, aligned(t * own, own)]
    saves[4].start()
    expand_gather.arrive()
    saves[6].start()
    shrink_gather.relay_middle(0)

    order = [(o, k) for o in (0, 2, 3, 1) for k in range(4) if o or k]
    for o, k in order:
        given(o, k).wait_recv()
    held = bias[0:1, :]
    for k in range(4):
        block_ = land[k].reshape(nc * hd, own)
        held = held + dot(block_.astype(F32).T.astype(BF16), out_t[k], 1, 0)
    value[...] = held
    gate = row_of(mod, 2 * width, width, part)
    shift = row_of(mod, 3 * width, width, part)
    scale = row_of(mod, 4 * width, width, part)
    mid = tok[aligned(mine * own, own), :].astype(F32) + gate * held
    middle[...] = mid
    hidden_two[mine] = (centred(mid)[0] * (1.0 + scale) + shift).astype(BF16)
    sharing = Share(hidden_two, hsend, hrecv)
    sharing.start()
    saves[5].start()
    shrink_gather.relay_rest(0)
    for o, k in order:
        given(o, k).wait_send()
    for o in (2, 1, 3):
        query_copy(o).wait_send()
    for copy in pcopies + mcopies + copies:
        copy.wait_send()
    shrink_gather.arrive()
    saves[7].start()
    sharing.relay()
    sharing.finish()
    saves[8].start()
    for copy in saves:
        copy.wait()
    for gather in (joint_gather, output_gather, expand_gather, shrink_gather):
        gather.drain()


def forward(nf, nc, part, tok, jweight, cond, modw, cbias, offset, oweight, eweight, bias, sweight):
    rows, width = tok.shape
    deep, columns = jweight.shape
    group = nf * nc
    own = rows // 4
    total = rows * nc
    hd = HEAD_DIM
    bq = min(512, rows)
    return call(
        partial(forward_body, nf, nc, part),
        "forward",
        (
            shape((rows, width), BF16),
            shape((columns, width), BF16),
            shape((4,) + cbias.shape, F32),
            shape((4, nc * hd, width), BF16),
            shape((3 * hd, total), BF16),
            shape((hd, total), F32),
            shape((1, total), F32),
            shape((4, nc, hd, own), BF16),
            shape((group,) + eweight.shape, BF16),
            shape((own, width), F32),
            shape((own, width), F32),
            shape((4, own, width), BF16),
            shape((group, deep, sweight.shape[1] // 2), BF16),
        ),
        [
            pltpu.VMEM((deep, sweight.shape[1] // 2), F32),
            pltpu.VMEM((group, deep, sweight.shape[1] // 2), BF16),
            pltpu.VMEM(tok.shape, BF16),
            pltpu.VMEM(jweight.shape, F32),
            pltpu.VMEM(modw.shape, F32),
            pltpu.VMEM(oweight.shape, F32),
            pltpu.VMEM(eweight.shape, F32),
            pltpu.VMEM((4, nc * hd, width), BF16),
            pltpu.VMEM((3 * hd, total), BF16),
            pltpu.VMEM((hd, total), F32),
            pltpu.VMEM((group,) + eweight.shape, BF16),
            pltpu.VMEM((4, own, width), BF16),
            pltpu.VMEM((rows, width), BF16),
            pltpu.VMEM((columns, width), BF16),
            pltpu.VMEM((group, deep, columns), BF16),
            pltpu.VMEM((group,) + oweight.shape, BF16),
            pltpu.VMEM((4, width, nc * hd), BF16),
            pltpu.VMEM((nf,) + cbias.shape, F32),
            pltpu.VMEM((group,) + cbias.shape, F32),
            pltpu.VMEM((rows, width), F32),
            pltpu.VMEM((columns, rows), BF16),
            pltpu.VMEM((nc, hd, rows), BF16),
            pltpu.VMEM((4, nc, hd, own), BF16),
            pltpu.VMEM((total, hd), BF16),
            pltpu.VMEM((total, bq), F32),
            DMA((6,)), DMA((9,)),
            DMA((group,)), DMA((group,)), DMA((4,)), DMA((4,)),
            DMA((2, nc)), DMA((2, nc)), DMA((nc, 4)), DMA((nc, 4)), DMA((3,)), DMA((3,)),
        ]
        + share_sems()
        + gather_sems(nf, nc, 6),
        1,
        150,
        60,
        ins=(0, 1, 3, 6, 7, 9),
        to=(0, 1, 3, 4, 5, 7, 8, 11, 12),
    )(tok, jweight, cond, modw, cbias, offset, oweight, eweight, bias, sweight)


def branch_body(
    nf, nc, part, hidden_hbm, cot_hbm, expand_hbm, sw_hbm, sbuf_hbm, hbias, mod, middle, value,
    attn_own, mid_grad, shrink_half, shrink_rest, expand_grad, stats, hstats, sh_cross, sh_own,
    cot, hidden, expand, sweight, sgat, gbuf, abuf, ebuf, slopes, held_buf,
    shrink_grad, shrink_parts, sland, dland, sbuf, rbuf, shold,
    lsem, tsend, trecv, send, recv, s1s, s1r, s2s, s2r, d1s, d1r, d2s, d2r, *gsems,
):
    mine, partner, cross, far = tp_places()
    own, width = middle.shape
    group = nf * nc
    deep, units = sweight.shape
    slot = lax.axis_index("fsdp") * nc + lax.axis_index("ctx")
    gate_first = row_of(mod, 2 * width, width, part)
    scale_second = row_of(mod, 4 * width, width, part)
    gate_second = row_of(mod, 5 * width, width, part)
    split = units // 2
    loads = load_all(
        (
            (sw_hbm, sweight), (hidden_hbm, hidden), (expand_hbm, expand), (cot_hbm, cot),
            (sbuf_hbm, sgat.at[:, :, pl.ds(0, split)]),
        ),
        lsem,
    )
    loads[0].wait()
    sgat[slot, :, split:units] = sweight[:, split:units].astype(BF16)
    greet(ring_peers("tp", 4) + weight_peers(nf, nc))
    gather = Gather(sgat, nf, nc, gsems, 2, 1)
    gather.start()
    for copy in loads[1:]:
        copy.wait()
    tile = 32

    def ahead(turn, carry):
        at = turned(mine, turn)

        @pl.when(turn == 2)
        def _():
            gather.relay_middle(1)


        where = aligned(at * own, own)
        weight = expand[...].reshape(width, units)
        slopes[where, :] = dot(hidden[at], weight, 1, 0) + hbias[...]

        def curve(k, carry_):
            row = pl.ds(pl.multiple_of(at * own + k * tile, tile), tile)
            u = slopes[row, :]
            squared = u * u
            th = jnp.tanh(GELU_SCALE * (u + GELU_CUBE * squared * u))
            abuf[row, :] = (0.5 * u * (1.0 + th)).astype(BF16)
            slopes[row, :] = 0.5 * (1.0 + th) + 0.5 * u * (1.0 - th * th) * (
                GELU_SCALE * (1.0 + 3.0 * GELU_CUBE * squared)
            )
            gbuf[row, :] = (gate_second * cot[row, :].astype(F32)).astype(BF16)
            return carry_

        lax.fori_loop(0, own // tile, curve, 0)
        return carry

    lax.fori_loop(0, 4, ahead, 0)
    gather.relay_rest(1)
    step = 256
    for at in range(0, width, step):
        block = dot(gbuf[:, at : at + step], abuf[...], 0, 0).astype(BF16)
        for k in range(at // deep, (at + step) // deep):
            shrink_grad[k // nc, k % nc] = block[k * deep - at : (k + 1) * deep - at, :]
    early = Scatter(
        nf, nc, shrink_grad, shrink_parts, sland, dland, s1s, s1r, d1s, d1r, (0, split)
    )
    late = Scatter(
        nf, nc, shrink_grad, shrink_parts, sland, dland, s2s, s2r, d2s, d2r, (split, split)
    )
    early.swap()
    late.swap()
    gather.arrive()
    hstats[...] = jnp.zeros_like(hstats)
    summing = Sum(sbuf, rbuf, send, recv)

    def back_turn(turn, carry):
        at = turned(mine, 3 - turn)
        where = aligned(at * own, own)
        weight = sgat[...].reshape(width, units)
        pull = dot(gbuf[where, :], weight, 1, 0) * slopes[where, :]
        hstats[...] += jnp.sum(pull, axis=0, keepdims=True)
        pull = pull.astype(BF16)
        ebuf[where, :] = pull
        held_buf[...] = dot(pull, expand[...].reshape(width, units), 1, 1)

        @pl.when(turn == 0)
        def _():
            summing.give(0, held_buf[...])

        @pl.when(turn == 1)
        def _():
            summing.pass_on(held_buf[...])

        @pl.when(turn == 2)
        def _():
            summing.give(1, held_buf[...])

        return carry

    lax.fori_loop(0, 4, back_turn, 0)
    copies = []
    for turn, at in enumerate((far, partner)):
        weight = sgat[...].reshape(width, units)
        shold[turn] = dot(abuf[aligned(at * own, own), :], weight, 1, 1).astype(BF16)
        copy = remote(
            shold.at[turn], shold.at[2 + turn], tsend.at[turn], trecv.at[turn], {"tp": partner}
        )
        copy.start()
        copies.append(copy)
    flat = hidden.shape[0] * own
    for at in range(0, width, step):
        expand_grad[at : at + step, :] = dot(
            hidden[:, :, at : at + step].reshape(flat, step), ebuf[...], 0, 0
        ).astype(BF16)
    early.swapped()
    early.deal()
    weight = sgat[...].reshape(width, units)
    forth = dot(abuf[aligned(cross * own, own), :], weight, 1, 1)
    copies[0].wait_recv()
    sh_cross[...] = (forth + shold[2].astype(F32)).astype(BF16)
    forth = dot(abuf[aligned(mine * own, own), :], weight, 1, 1)
    copies[1].wait_recv()
    sh_own[...] = forth + shold[3].astype(F32)
    mine_rows = cot[aligned(mine * own, own), :].astype(F32)
    stats[3:4, :] = jnp.sum(gate_second * mine_rows, axis=0, keepdims=True)
    normed, inverse = centred(middle[...])
    grad_in = summing.total(summing.near(held_buf[...]))
    stats[0:1, :] = jnp.sum(grad_in, axis=0, keepdims=True)
    stats[1:2, :] = jnp.sum(grad_in * normed, axis=0, keepdims=True)
    mgrad = mine_rows + normal_back(grad_in * (1.0 + scale_second), normed, inverse)
    mid_grad[...] = mgrad
    agrad = gate_first * mgrad
    attn_own[...] = agrad.astype(BF16)
    stats[2:3, :] = jnp.sum(mgrad * value[...], axis=0, keepdims=True)
    stats[4:5, :] = jnp.sum(agrad, axis=0, keepdims=True)
    stats[5:8, :] = jnp.zeros((3, width), F32)
    late.swapped()
    shrink_rest[...] = shrink_parts[:, :, split:units]
    shrink_half[...] = early.dealt()
    early.drain()
    late.drain(deals=False)
    summing.drain()
    gather.drain()
    for copy in copies:
        copy.wait_send()


def branch(nf, nc, part, hidden, cot, expand, sweight, sbuf, hbias, mod, middle, value):
    rows, width = cot.shape
    own = rows // 4
    deep, units = sweight.shape
    group = nf * nc
    return call(
        partial(branch_body, nf, nc, part),
        "branch",
        (
            shape((own, width), BF16),
            shape((own, width), F32),
            shape((deep, units // 2), F32),
            shape((nc, deep, units // 2), BF16),
            shape((width, units), BF16),
            shape((8, width), F32),
            shape((1, units), F32),
            shape((own, width), BF16),
            shape((own, width), F32),
        ),
        [
            pltpu.VMEM((rows, width), BF16),
            pltpu.VMEM((4, own, width), BF16),
            pltpu.VMEM((group, deep, units), BF16),
            pltpu.VMEM((deep, units), F32),
            pltpu.VMEM((group, deep, units), BF16),
            pltpu.VMEM((rows, width), BF16),
            pltpu.VMEM((rows, units), BF16),
            pltpu.VMEM((rows, units), BF16),
            pltpu.VMEM((rows, units), F32),
            pltpu.VMEM((own, width), F32),
            pltpu.VMEM((nf, nc, deep, units), BF16),
            pltpu.VMEM((nc, deep, units), BF16),
            pltpu.VMEM((nf - 1, nc, deep, units), BF16),
            pltpu.VMEM((nc - 1, deep, units), BF16),
            pltpu.VMEM((3, own, width), BF16),
            pltpu.VMEM((3, own, width), BF16),
            pltpu.VMEM((4, own, width), BF16),
            DMA((5,)), DMA((2,)), DMA((2,)),
        ]
        + share_sems()
        + [DMA((nf,))] * 4
        + [DMA((nc,))] * 4
        + gather_sems(nf, nc, 1),
        2,
        40,
        60,
        ins=(0, 1, 2, 3, 4),
    )(hidden, cot, expand, sweight, sbuf, hbias, mod, middle, value)


def backward_body(
    nf, nc, part, attn_own, out_t_hbm, heads_hbm, qkv_hbm, out_hbm, lse, sh_cross, sh_own, middle,
    cot_hbm, mod, bias, shrink_half, shrink_parts, expand_grad, weight_hbm, hidden_hbm, tok_hbm,
    mid_grad, stats_second, hidden_stats, modw_hbm, low,
    mixed, tokens_grad, shrink_sum, expand_sum, output_sum, joint_sum, modulate_sum,
    bias_rows, done,
    out_t, qkv, out, heads, att, cot_own, tok_own, weight_t, hidden, modw,
    attn_low, dout, dost, keys, vals, dq, stage, rland, delta, output_grad, eland, oland,
    expand_parts, output_parts, sdeal, edeal, odeal, joint_grad, sbuf, rbuf,
    kvgrad, kvland, kvparts, kvdeal, qgrad, qland, qparts, qdeal, pieces, land, total_piece, gathered, ftotal, gate_row,
    lsem, send, recv, jsend, jrecv, csend, crecv, gsend, grecv, tsend, trecv, hsend, hrecv,
    lowsend, lowrecv, hsend2, hrecv2, x1s, x1r, x2s, x2r, x3s, x3r, x4s, x4r, x5s, x5r,
    d1s, d1r, d2s, d2r, d3s, d3r, d4s, d4r, d5s, d5r, d6s, d6r, asend, arecv, bsend, brecv, f1s, f1r,
):
    f, c, t = lax.axis_index("fsdp"), lax.axis_index("ctx"), lax.axis_index("tp")
    mine, partner, cross, far = tp_places()
    own, width = middle.shape
    rows = 4 * own
    total = rows * nc
    hd = HEAD_DIM
    inner, group = nc * 4, nf * nc
    here, slot = c * 4 + t, f * nc + c
    bk = bq = 512
    per = rows // bk
    deep = joint_sum.shape[0]
    heads_wide = nc * hd
    units = expand_grad.shape[3]
    half = units // 2
    shrink = Scatter(nf, nc, None, shrink_parts, eland, sdeal, None, None, d1s, d1r)
    early = Scatter(
        nf, nc, expand_grad, expand_parts, eland, edeal, x1s, x1r, d2s, d2r, (0, half)
    )
    late = Scatter(
        nf, nc, expand_grad, expand_parts, eland, edeal, x2s, x2r, d3s, d3r, (half, half)
    )
    project = Scatter(nf, nc, output_grad, output_parts, oland, odeal, x3s, x3r, d4s, d4r)
    kv = Scatter(nf, nc, kvgrad, kvparts, kvland, kvdeal, x4s, x4r, d5s, d5r)
    query = Scatter(nf, nc, qgrad, qparts, qland, qdeal, x5s, x5r, d6s, d6r)
    own_rows = aligned(mine * own, own)
    loads = load_all(
        (
            (out_t_hbm, out_t), (qkv_hbm, qkv), (out_hbm, out), (heads_hbm, heads),
            (cot_hbm.at[own_rows, :], cot_own), (tok_hbm.at[own_rows, :], tok_own),
            (weight_hbm, weight_t), (hidden_hbm, hidden), (modw_hbm, modw),
        ),
        lsem,
    )
    attn_low[mine] = attn_own[...]
    loads[0].wait()
    for k in range(4):
        dost[k] = dot(out_t[k], attn_own[...], 1, 1).astype(BF16).reshape(nc, hd, own)
    greet(all_peers(nf, nc))
    where_own = aligned(c * rows + t * own, own)

    def send_out(o, k):
        cc, tt = lax.rem(c + o, nc), lax.rem(t + k, 4)
        return remote(
            dost.at[tt, cc], dout.at[:, where_own], send.at[o, k], recv.at[o, k],
            {"ctx": cc, "tp": tt},
        )

    order = [(o, k) for o in (2, 1, 3, 0) for k in range(4) if o or k]
    for o, k in order:
        send_out(o, k).start()
    low_share = Share(attn_low, lowsend, lowrecv)
    low_share.start()
    early.swap()
    late.swap()
    crossing = remote(sh_cross, rland, csend, crecv, {"tp": cross})
    crossing.start()
    shrink.deal()
    dout[:, where_own] = dost[t, c]
    for copy in loads[1:4]:
        copy.wait()
    for at in range(0, total, 1024):
        keys[at : at + 1024, :] = transposed(qkv[hd : 2 * hd, at : at + 1024])
        vals[at : at + 1024, :] = transposed(qkv[2 * hd : 3 * hd, at : at + 1024])
    dq[...] = jnp.zeros_like(dq)
    for o, k in order:
        send_out(o, k).wait_recv()
    for at in range(0, total, 1024):
        delta[:, at : at + 1024] = jnp.sum(
            dout[:, at : at + 1024].astype(F32) * out[:, at : at + 1024], axis=0, keepdims=True
        )
    sharing = Share(mixed, gsend, grecv)
    exchange = [
        remote(heads.at[peer["tp"]], att.at[:, :, own_rows], hsend2.at[k], hrecv2.at[k], peer)
        for k, peer in zip(range(1, 4), ring_peers("tp", 4))
    ]

    def kv_back(o, owner):
        return remote(
            stage.at[owner, pl.ds(hd, 2 * hd), :], joint_grad.at[c, pl.ds(hd, 2 * hd), :],
            jsend.at[0, o], jrecv.at[0, o], {"ctx": owner},
        )

    def q_back(o, owner):
        return remote(
            stage.at[owner, pl.ds(0, hd), :], joint_grad.at[c, pl.ds(0, hd), :],
            jsend.at[1, o], jrecv.at[1, o], {"ctx": owner},
        )

    def block(i, vsum):
        o = 1 + i // per
        owner = lax.rem(c + o, nc)
        sub = lax.rem(i, per)
        where = aligned(owner * rows + sub * bk, bk)
        key, val, key_t = keys[where, :], vals[where, :], qkv[hd : 2 * hd, where]
        dk, dv = None, None
        for at in range(0, total, bq):
            query = qkv[0:hd, at : at + bq] * BF16(hd**-0.5)
            grad = dout[:, at : at + bq]
            p = jnp.exp(dot(key, query, 1, 0) - lse[:, at : at + bq])
            ds = (p * (dot(val, grad, 1, 0) - delta[:, at : at + bq])).astype(BF16)
            tv = dot(grad, p.astype(BF16), 1, 1)
            tk = dot(query, ds, 1, 1)
            dv = tv if dv is None else dv + tv
            dk = tk if dk is None else dk + tk
            dq[:, at : at + bq] += dot(key_t, ds, 1, 0)
        put = aligned(sub * bk, bk)
        stage[owner, hd : 2 * hd, put] = dk.astype(BF16)
        stage[owner, 2 * hd : 3 * hd, put] = dv.astype(BF16)

        @pl.when(jnp.logical_and(sub == per - 1, o < nc))
        def _():
            kv_back(o, owner).start()

        @pl.when(i == 1)
        def _():
            low_share.relay()
            att[:, :, own_rows] = heads[t]
            for copy in exchange:
                copy.start()

        @pl.when(i == 3)
        def _():
            for k in (1, 2):
                low_share.copy(k).wait_recv()
            for copy in exchange:
                copy.wait_recv()
            flat = dot(
                att[...].reshape(heads_wide, rows), attn_low[...].reshape(rows, width), 1, 0
            ).T.astype(BF16)
            output_grad[...] = flat.reshape(output_grad.shape)
            project.swap()

        @pl.when(i == 2)
        def _():
            crossing.wait_recv()
            loads[4].wait()
            value = sh_own[...] + rland[...].astype(F32) + bias[1:2, :]
            gate = row_of(mod, 5 * width, width, part)
            mixed[mine] = (middle[...] + gate * value).astype(BF16)
            sharing.start()
            gate_row[...] = jnp.sum(
                cot_own[...].astype(F32) * value, axis=0, keepdims=True
            )

        @pl.when(i == 2)
        def _():
            early.swapped()
            early.deal()

        @pl.when(i == 4)
        def _():
            late.swapped()

        @pl.when(i == 6)
        def _():
            project.swapped()
            sharing.relay()

        return vsum + jnp.sum(dv, axis=1, keepdims=True)

    vsum = lax.fori_loop(0, per * nc, block, jnp.zeros((hd, 1), F32))
    qsum = jnp.zeros((hd, 1), F32)
    for o in (2, 1, 3, 0):
        owner = lax.rem(c + o, nc)
        piece = dq[:, aligned(owner * rows, rows)] * (hd**-0.5)
        qsum = qsum + jnp.sum(piece, axis=1, keepdims=True)
        stage[owner, 0:hd, :] = piece.astype(BF16)
        if o > 0:
            q_back(o, owner).start()
    late.deal()
    project.deal()
    joint_grad[c] = stage[c]
    bias_column = jnp.concatenate([qsum, vsum], axis=0)
    for copy in loads[5:]:
        copy.wait()
    rows_f = width // nf

    def weight_grad(scatter, source, into):
        flat_grad = source.reshape(-1, rows)

        def put(lanes, member, first, count):
            block_ = dot(flat_grad, hidden[:, lanes], 1, 0).T.astype(BF16)
            for k in range(count):
                row = (member, first + k) if member is not None else divmod(first + k, nc)
                into[row[0], row[1]] = block_[k * deep : (k + 1) * deep, :]

        if rows_f % 128:
            for at in range(0, width, 256):
                put(pl.ds(at, 256), None, at // deep, 256 // deep)
            scatter.swap()
            return
        wide_step = min(256, rows_f)
        for o in range(1, nf + 1):
            member = lax.rem(f + o, nf)
            for at in range(0, rows_f, wide_step):
                put(
                    aligned(member * rows_f + at, wide_step), member, at // deep, wide_step // deep
                )
            if o < nf:
                scatter.swaps[o - 1].start()

    for o in range(1, nc):
        kv_back(o, lax.rem(c + o, nc)).wait_recv()
    weight_grad(kv, joint_grad[:, hd : 3 * hd, :], kvgrad)
    shrink_total = shrink.dealt()
    shrink_sum[:, 0:half] = shrink_half[...]
    shrink_sum[:, half:units] = shrink_total
    squares = jnp.sum(shrink_total * shrink_total) + jnp.sum(shrink_half[...] * shrink_half[...])
    for o in range(1, nc):
        q_back(o, lax.rem(c + o, nc)).wait_recv()

    columns = weight_t.shape[0]

    def piece_of(at):
        block_ = joint_grad[:, :, aligned(at * own, own)].reshape(columns, own)
        return dot(block_.astype(F32).T.astype(BF16), weight_t[...], 1, 0)

    summing = Sum(sbuf, rbuf, tsend, trecv)
    summing.give(0, piece_of(far))
    summing.give(1, piece_of(partner))
    summing.pass_on(piece_of(cross))
    weight_grad(query, joint_grad[:, 0:hd, :], qgrad)
    held = summing.near(piece_of(mine))
    kv.swapped()
    kv.deal()
    normed, inverse = centred(tok_own[...].astype(F32))
    grad_in = summing.total(held)
    scale = row_of(mod, width, width, part)
    shift_row = jnp.sum(grad_in, axis=0, keepdims=True)
    scale_row = jnp.sum(grad_in * normed, axis=0, keepdims=True)

    slim = part // nc // 128
    share = 2 * width // nc // 128
    hshare = hidden_stats.shape[1] // nc // 128
    last = slim + share + hshare
    vectors = [
        shift_row, scale_row, stats_second[2:3, :],
        stats_second[0:1, :], stats_second[1:2, :], gate_row[...],
    ]
    residual = [stats_second[4:5, :], stats_second[3:4, :]]
    pieces[...] = jnp.zeros_like(pieces)
    for cc in range(nc):
        for tt in range(4):
            k = cc * 4 + tt
            for n in range(slim):
                at = ((tt * part // 128) + cc * slim + n) * 128
                pieces[k, n : n + 1, :] = vectors[at // width][:, at % width : at % width + 128]
            for n in range(share):
                at = (cc * share + n) * 128
                pieces[k, slim + n : slim + n + 1, :] = residual[at // width][
                    :, at % width : at % width + 128
                ]
        for n in range(hshare):
            at = (cc * hshare + n) * 128
            pieces[cc * 4 + t, slim + share + n : slim + share + n + 1, :] = hidden_stats[
                :, at : at + 128
            ]
    pieces[here, last : last + 1, :] = jnp.broadcast_to(bias_column, (2 * hd, 128)).T[0:1, :]
    first = []
    for o in range(1, inner):
        other = lax.rem(here + o, inner)
        copy = remote(
            pieces.at[other], land.at[here], asend.at[o], arecv.at[o],
            {"ctx": other // 4, "tp": lax.rem(other, 4)},
        )
        copy.start()
        first.append(copy)
    tokens_grad[mine] = (
        mid_grad[...] + normal_back(grad_in * (1.0 + scale), normed, inverse)
    ).astype(BF16)
    token_share = Share(tokens_grad, hsend, hrecv)
    token_share.start()
    query.swapped()
    query.deal()
    land[here] = pieces[here]
    for copy in first:
        copy.wait_recv()
    acc = land[0]
    for k in range(1, inner):
        acc = acc + land[k]
    total_piece[...] = acc
    gathered[slot] = acc
    second = []
    for o, peer in zip(range(1, group), weight_peers(nf, nc)):
        copy = remote(total_piece, gathered.at[slot], bsend.at[o], brecv.at[o], peer)
        copy.start()
        second.append(copy)
    expand_total = early.dealt()
    expand_sum[:, 0:half] = expand_total
    squares = squares + jnp.sum(expand_total * expand_total)
    expand_total = late.dealt()
    expand_sum[:, half:units] = expand_total
    squares = squares + jnp.sum(expand_total * expand_total)
    output_total = project.dealt()
    output_sum[...] = output_total
    squares = squares + jnp.sum(output_total * output_total)
    for copy in second:
        copy.wait_recv()

    grads = []
    for latent in range(nf):
        strips = []
        for cc in range(nc):
            for n in range(slim):
                strips.append(gathered[latent * nc + cc, n : n + 1, :])
        grads.append(jnp.concatenate(strips, axis=1))
    condition_bias = grads[0]
    for latent in range(1, nf):
        condition_bias = condition_bias + grads[latent]
    bias_rows[...] = jnp.zeros_like(bias_rows)
    bias_rows[0:1, 0:part] = condition_bias
    factors = low[...].T
    wide = modw[...].astype(BF16).astype(F32)
    outer = None
    ftotal[...] = jnp.zeros_like(ftotal)
    for latent in range(nf):
        term = factors[:, latent : latent + 1] * grads[latent]
        outer = term if outer is None else outer + term
        column = jnp.sum(wide * grads[latent], axis=1, keepdims=True)
        ftotal[latent : latent + 1, 0:deep] = jnp.broadcast_to(column, (deep, 128)).T[0:1, :]
    modulate_sum[...] = outer
    squares = squares + jnp.sum(outer * outer)

    def over(at, count):
        found = []
        for cc in range(nc):
            value = None
            for latent in range(nf):
                block_ = gathered[latent * nc + cc, at : at + count, :]
                value = block_ if value is None else value + block_
            for n in range(count):
                found.append(value[n : n + 1, :])
        return jnp.concatenate(found, axis=1)

    residual_sum = over(slim, share)
    hidden_sum = over(slim + share, hshare)
    head_sum = over(last, 1)
    bias_rows[1:2, 0 : hidden_sum.shape[1]] = hidden_sum
    bias_rows[2:3, 0 : head_sum.shape[1]] = head_sum
    bias_rows[3:4, 0:width] = residual_sum[:, 0:width]
    bias_rows[4:5, 0:width] = residual_sum[:, width : 2 * width]
    lead = (slot == 0).astype(F32)
    tensor_lead = (t == 0).astype(F32)
    squares = squares + lead * (
        jnp.sum(condition_bias * condition_bias)
        + jnp.sum(hidden_sum * hidden_sum)
        + jnp.sum(head_sum * head_sum)
        + tensor_lead * jnp.sum(residual_sum * residual_sum)
    )
    token_share.relay()
    kv_total, q_total = kv.dealt(), query.dealt()
    squares = squares + jnp.sum(kv_total * kv_total) + jnp.sum(q_total * q_total)
    ftotal[nf : nf + 1, :] = jnp.full((1, 128), squares)
    third = []
    for o, peer in zip(range(1, group * 4), all_peers(nf, nc)):
        copy = remote(ftotal, done.at[slot, t], f1s.at[o], f1r.at[o], peer)
        copy.start()
        third.append(copy)
    done[slot, t] = ftotal[...]
    kv_total, q_total = kv_total.T, q_total.T
    blocks = []
    for k in range(nc):
        blocks += [q_total[k * hd : (k + 1) * hd], kv_total[k * 2 * hd : (k + 1) * 2 * hd]]
    joint_sum[...] = jnp.concatenate(blocks, axis=0).T
    sharing.finish()
    token_share.finish()
    summing.drain()
    for o in range(1, nc):
        owner = lax.rem(c + o, nc)
        kv_back(o, owner).wait_send()
        q_back(o, owner).wait_send()
    for o, k in order:
        send_out(o, k).wait_send()
    for k in range(3):
        low_share.copy(k).wait_send()
    for copy in exchange:
        copy.wait_send()
    crossing.wait_send()
    shrink.drain(swaps=False)
    for scatter in (early, late, project, kv, query):
        scatter.drain()
    for copy in third:
        copy.wait_recv()
    for copy in first + second + third:
        copy.wait_send()


def backward(
    nf, nc, part, attn_own, out_t, att, qkv, out, lse, sh_cross, sh_own, middle, cot, mod, bias,
    shrink_half, shrink_parts, expand_grad, weight_t, hidden, tok, mid_grad, stats_second, hidden_stats,
    modw, low,
):
    rows, width = cot.shape
    own = rows // 4
    total = rows * nc
    hd = HEAD_DIM
    inner, group = nc * 4, nf * nc
    deep = width // group
    units = expand_grad.shape[1]
    columns = weight_t.shape[0]
    heads_wide = nc * hd
    expand_grad = expand_grad.reshape(nf, nc, deep, units)
    high = -(-(part // nc + 2 * width // nc + hidden_stats.shape[1] // nc + 128) // 1024) * 8
    tall = -(-(nf + 1) // 8) * 8
    return call(
        partial(backward_body, nf, nc, part),
        "backward",
        (
            shape((4, own, width), BF16),
            shape((4, own, width), BF16),
            shape((deep, units), F32),
            shape((deep, units), F32),
            shape((deep, heads_wide), F32),
            shape((deep, columns), F32),
            shape((deep, part), F32),
            shape((8, max(part, width, hidden_stats.shape[1])), F32),
            shape((group, 4, tall, 128), F32),
        ),
        [
            pltpu.VMEM(out_t.shape, BF16),
            pltpu.VMEM(qkv.shape, BF16),
            pltpu.VMEM(out.shape, F32),
            pltpu.VMEM(att.shape, BF16),
            pltpu.VMEM((nc, hd, rows), BF16),
            pltpu.VMEM((own, width), BF16),
            pltpu.VMEM((own, width), BF16),
            pltpu.VMEM(weight_t.shape, BF16),
            pltpu.VMEM(hidden.shape, BF16),
            pltpu.VMEM(modw.shape, F32),
            pltpu.VMEM((4, own, width), BF16),
            pltpu.VMEM((hd, total), BF16),
            pltpu.VMEM((4, nc, hd, own), BF16),
            pltpu.VMEM((total, hd), BF16),
            pltpu.VMEM((total, hd), BF16),
            pltpu.VMEM((hd, total), F32),
            pltpu.VMEM((nc, 3 * hd, rows), BF16),
            pltpu.VMEM((own, width), BF16),
            pltpu.VMEM((1, total), F32),
            pltpu.VMEM((nf, nc, deep, heads_wide), BF16),
            pltpu.VMEM((nf - 1, nc, deep, units), BF16),
            pltpu.VMEM((nf - 1, nc, deep, heads_wide), BF16),
            pltpu.VMEM((nc, deep, units), BF16),
            pltpu.VMEM((nc, deep, heads_wide), BF16),
            pltpu.VMEM((nc - 1, deep, units // 2), BF16),
            pltpu.VMEM((nc - 1, deep, units), BF16),
            pltpu.VMEM((nc - 1, deep, heads_wide), BF16),
            pltpu.VMEM((nc, 3 * hd, rows), BF16),
            pltpu.VMEM((3, own, width), BF16),
            pltpu.VMEM((3, own, width), BF16),
            pltpu.VMEM((nf, nc, deep, 2 * heads_wide), BF16),
            pltpu.VMEM((nf - 1, nc, deep, 2 * heads_wide), BF16),
            pltpu.VMEM((nc, deep, 2 * heads_wide), BF16),
            pltpu.VMEM((nc - 1, deep, 2 * heads_wide), BF16),
            pltpu.VMEM((nf, nc, deep, heads_wide), BF16),
            pltpu.VMEM((nf - 1, nc, deep, heads_wide), BF16),
            pltpu.VMEM((nc, deep, heads_wide), BF16),
            pltpu.VMEM((nc - 1, deep, heads_wide), BF16),
            pltpu.VMEM((inner, high, 128), F32),
            pltpu.VMEM((inner, high, 128), F32),
            pltpu.VMEM((high, 128), F32),
            pltpu.VMEM((group, high, 128), F32),
            pltpu.VMEM((tall, 128), F32),
            pltpu.VMEM((1, width), F32),
            DMA((9,)), DMA((nc, 4)), DMA((nc, 4)), DMA((2, nc)), DMA((2, nc)),
            DMA, DMA,
        ]
        + share_sems() * 4
        + [DMA((4,))] * 2
        + [DMA((nf,))] * 10
        + [DMA((nc,))] * 12
        + [DMA((inner,))] * 2
        + [DMA((group,))] * 2
        + [DMA((group * 4,))] * 2,
        3,
        150,
        60,
        ins=(1, 2, 3, 4, 9, 15, 16, 17, 21),
    )(
        attn_own, out_t, att, qkv, out, lse, sh_cross, sh_own, middle, cot, mod, bias,
        shrink_half, shrink_parts, expand_grad, weight_t, hidden, tok, mid_grad, stats_second,
        hidden_stats, modw, low,
    )


def update(master, first, root, gradient, clip, decay_rate):
    scaled = clip * gradient
    first_moment = first_decay * first + (1.0 - first_decay) * scaled
    second_moment = second_decay * root * root + (1.0 - second_decay) * scaled * scaled
    new_root = jnp.sqrt(second_moment)
    first_hat = first_moment * (1.0 / (1.0 - first_decay**ADAM_STEP))
    second_hat = second_moment * (1.0 / (1.0 - second_decay**ADAM_STEP))
    updated = master - learning_rate * (
        first_hat / (jnp.sqrt(second_hat) + adam_epsilon) + decay_rate * master
    )
    return updated, first_moment, new_root


def adam_body(count, nf, nc, done, condition, bias_rows, tokens_hbm, mixed_hbm, *refs):
    grads = refs[:count]
    masters = refs[count : 2 * count]
    moments = refs[2 * count : 3 * count]
    smalls = refs[3 * count : 3 * count + 8]
    outs = refs[3 * count + 8 :]
    news = outs[:count]
    averages = outs[count : 2 * count]
    small_outs = outs[2 * count : 2 * count + 8]
    condition_grad, norm, tokens_out, mixed_out = outs[2 * count + 8 : 2 * count + 12]
    scratch = outs[2 * count + 12 :]
    wbufs = scratch[:count]
    mbufs = scratch[count : 2 * count]
    gbufs = scratch[2 * count : 3 * count]
    tokens_low, mixed, wide, isem, osem, tsem = scratch[3 * count :]
    token_load = pltpu.make_async_copy(tokens_hbm, tokens_low, tsem.at[5])
    mixed_load = pltpu.make_async_copy(mixed_hbm, mixed, tsem.at[6])
    group = nf * nc
    f = lax.axis_index("fsdp")
    loads, stores = [], []
    for k in range(count):
        loads.append(
            (
                pltpu.make_async_copy(masters[k], wbufs[k], isem.at[0, k]),
                pltpu.make_async_copy(moments[k], mbufs[k], isem.at[1, k]),
                pltpu.make_async_copy(grads[k], gbufs[k], isem.at[2, k]),
            )
        )
        stores.append(
            (
                pltpu.make_async_copy(wbufs[k], news[k], osem.at[0, k]),
                pltpu.make_async_copy(mbufs[k], averages[k], osem.at[1, k]),
            )
        )
    for copy in loads[0]:
        copy.start()
    token_load.start()
    mixed_load.start()
    for group_ in loads[1:]:
        for copy in group_:
            copy.start()
    token_load.wait()
    mixed_load.wait()
    mixed_copy = pltpu.make_async_copy(mixed, mixed_out, tsem.at[4])
    mixed_copy.start()
    token_copies = []
    for k in range(4):

        def widen(i, carry, k=k):
            at = pl.ds(pl.multiple_of(i * 16, 16), 16)
            wide[k, at, :] = tokens_low[k, at, :].astype(F32)
            return carry

        lax.fori_loop(0, wide.shape[1] // 16, widen, 0)
        copy = pltpu.make_async_copy(wide.at[k], tokens_out.at[k], tsem.at[k])
        copy.start()
        token_copies.append(copy)
    folded = [done[k, 0] + done[k, 1] + done[k, 2] + done[k, 3] for k in range(group)]
    squares = folded[0][nf : nf + 1, 0:1]
    for k in range(1, group):
        squares = squares + folded[k][nf : nf + 1, 0:1]
    grad_norm = jnp.sqrt(squares)
    norm[...] = grad_norm
    clip = jnp.minimum(1.0, clip_limit / (grad_norm + 1e-06))
    deep = condition.shape[1] // group
    found = []
    for k in range(group):
        row = done[k, 0, pl.ds(f, 1), 0:deep]
        for tt in range(1, 4):
            row = row + done[k, tt, pl.ds(f, 1), 0:deep]
        found.append(row)
    v = condition[pl.ds(f, 1), :]
    gate = 1.0 / (1.0 + jnp.exp(-v))
    condition_grad[...] = jnp.concatenate(found, axis=1) * (gate * (1.0 + v * (1.0 - gate)))
    for k in range(4):
        master, moment = smalls[2 * k], smalls[2 * k + 1]
        if k < 3:
            row = (2, 1, 0)[k]
            grad = bias_rows[row : row + 1, 0 : master.shape[1]]
            new, first, root = update(master[...], moment[0:1, :], moment[1:2, :], grad, clip, 0.0)
            small_outs[2 * k][...] = new
            small_outs[2 * k + 1][0:1, :] = first
            small_outs[2 * k + 1][1:2, :] = root
        else:
            grad = bias_rows[3:5, 0 : master.shape[1]]
            new, first, root = update(master[...], moment[0], moment[1], grad, clip, 0.0)
            small_outs[2 * k][...] = new
            small_outs[2 * k + 1][0] = first
            small_outs[2 * k + 1][1] = root
    for k in range(count):
        for copy in loads[k]:
            copy.wait()
        deep_k = wbufs[k].shape[0]
        step = min(16, deep_k)

        def rows(i, carry, k=k, step=step):
            at = pl.ds(pl.multiple_of(i * step, step), step)
            new, first, root = update(
                wbufs[k][at, :], mbufs[k][0, at, :], mbufs[k][1, at, :], gbufs[k][at, :],
                clip, weight_decay,
            )
            wbufs[k][at, :] = new
            mbufs[k][0, at, :] = first
            mbufs[k][1, at, :] = root
            return carry

        lax.fori_loop(0, deep_k // step, rows, 0)
        for copy in stores[k]:
            copy.start()
    for pair in stores:
        for copy in pair:
            copy.wait()
    for copy in token_copies + [mixed_copy]:
        copy.wait()


def adam(nf, nc, done, condition, bias_rows, tokens_low, mixed, grads, masters, moments, smalls):
    count = len(grads)
    anywhere = pl.BlockSpec(memory_space=pltpu.HBM)
    small_shapes = tuple(shape(a.shape, F32) for a in smalls)
    outs = (
        tuple(shape(m.shape, F32) for m in masters)
        + tuple(shape(m.shape, F32) for m in moments)
        + small_shapes
        + (shape((1, condition.shape[1]), F32), shape((1, 1), F32))
        + (shape(tokens_low.shape, F32), shape(mixed.shape, BF16))
    )
    return pl.pallas_call(
        partial(adam_body, count, nf, nc),
        out_shape=outs,
        in_specs=vmem(3) + [anywhere] * (2 + 3 * count) + vmem(8),
        out_specs=[anywhere] * (2 * count) + vmem(10) + [anywhere] * 2,
        scratch_shapes=[pltpu.VMEM(m.shape, F32) for m in masters]
        + [pltpu.VMEM(m.shape, F32) for m in moments]
        + [pltpu.VMEM(m.shape, F32) for m in masters]
        + [
            pltpu.VMEM(tokens_low.shape, BF16), pltpu.VMEM(mixed.shape, BF16),
            pltpu.VMEM(tokens_low.shape, F32),
        ]
        + [DMA((3, count)), DMA((2, count)), DMA((7,))],
        compiler_params=pltpu.CompilerParams(vmem_limit_bytes=63 << 20),
        cost_estimate=cost(10),
        name="adam",
    )(done, condition, bias_rows, tokens_low, mixed, *grads, *masters, *moments, *smalls)


def local(
    nf,
    nc,
    tokens,
    condition,
    cotangent,
    joint_weight,
    joint_moments,
    output_weight,
    output_moments,
    expand_weight,
    expand_moments,
    shrink_weight,
    shrink_moments,
    modulate_weight,
    modulate_moments,
    attention_bias,
    attention_moments,
    hidden_bias,
    hidden_moments,
    condition_bias,
    condition_moments,
    residual_bias,
    residual_moments,
):
    latent_count, rows, width = tokens.shape
    heads = joint_weight.shape[1] // (3 * HEAD_DIM)
    assert latent_count == 1 and heads == nc and lax.axis_size("tp") == 4
    f, c, t = lax.axis_index("fsdp"), lax.axis_index("ctx"), lax.axis_index("tp")
    mine = f * nc + c
    deep, part = modulate_weight.shape
    units = expand_weight.shape[1]
    tok, cot = tokens[0], cotangent[0]

    condition_low = jax.nn.silu(condition).astype(BF16)
    condition_here = lax.dynamic_slice_in_dim(condition_low, mine * deep, deep, 1)
    strips = part // 128
    high = -(-strips // 8) * 8
    bias_strips = jnp.pad(condition_bias.reshape(strips, 128), ((0, high - strips), (0, 0)))
    bias_pairs = attention_bias.reshape(heads, 2, HEAD_DIM)
    offset = jnp.stack(
        [bias_pairs[:, 0], jnp.zeros_like(bias_pairs[:, 0]), bias_pairs[:, 1]], axis=1
    ).reshape(-1, 1)
    condition_pad = jnp.pad(condition_here, ((0, 16 - nf), (0, 0)))
    (
        hidden_first, joint_full_t, mod, out_t, qkv, out, lse, att, expand_full,
        value, middle, hidden_two, shrink_early,
    ) = forward(
        nf, nc, part, tok, joint_weight, condition_pad, modulate_weight, bias_strips, offset,
        output_weight, expand_weight, residual_bias, shrink_weight,
    )
    (
        attn_own, mid_grad, shrink_half, shrink_parts, expand_grad, stats_second, hidden_stats,
        sh_cross, sh_own,
    ) = branch(
        nf, nc, part, hidden_two, cot, expand_full, shrink_weight, shrink_early, hidden_bias[None, :], mod, middle, value,
    )
    (
        mixed, tokens_grad, shrink_sum, expand_sum, output_sum, joint_sum, modulate_sum,
        bias_rows, done,
    ) = backward(
        nf, nc, part, attn_own, out_t, att, qkv, out, lse, sh_cross, sh_own, middle, cot,
        mod, residual_bias, shrink_half, shrink_parts, expand_grad, joint_full_t, hidden_first,
        tok, mid_grad, stats_second, hidden_stats, modulate_weight, condition_pad.astype(F32),
    )
    weights = (joint_weight, output_weight, expand_weight, shrink_weight, modulate_weight)
    moments = (joint_moments, output_moments, expand_moments, shrink_moments, modulate_moments)
    grads = (joint_sum, output_sum, expand_sum, shrink_sum, modulate_sum)
    smalls = (
        attention_bias[None, :], attention_moments, hidden_bias[None, :], hidden_moments,
        condition_bias[None, :], condition_moments, residual_bias, residual_moments,
    )
    results = adam(nf, nc, done, condition, bias_rows, tokens_grad, mixed, grads, weights, moments, smalls)
    updated = []
    for k in range(5):
        updated += [results[k], results[5 + k]]
    for k in range(4):
        new = results[10 + 2 * k]
        updated += [new[0] if k < 3 else new, results[11 + 2 * k]]
    return (
        results[21].reshape(1, rows, width),
        results[20].reshape(1, rows, width),
        results[18],
        results[19][0, 0],
    ) + tuple(updated)


def solution(mesh):
    rows = P(("fsdp", "ctx"), "tp")
    pair = P(None, ("fsdp", "ctx"), "tp")
    tokens = P("fsdp", "ctx", None)
    small = (P("tp"), P(None, "tp"))
    return jax.shard_map(
        partial(local, mesh.shape["fsdp"], mesh.shape["ctx"]),
        mesh=mesh,
        in_specs=(tokens, P(), tokens) + (rows, pair) * 5 + small * 3 + (P(), P()),
        out_specs=(tokens, tokens, P("fsdp", None), P())
        + (rows, pair) * 5
        + small * 3
        + (P(), P()),
        check_vma=False,
    )
```

```python
from functools import partial

import jax
import jax.numpy as jnp
from jax import lax
from jax.experimental import pallas as pl
from jax.experimental.pallas import tpu as pltpu
from jax.sharding import PartitionSpec as P

HEAD_DIM = 64
ADAM_STEP = 10
F32 = jnp.float32
BF16 = jnp.bfloat16
MESH = pl.DeviceIdType.MESH
DMA = pltpu.SemaphoreType.DMA

norm_epsilon = 1e-06
first_decay = 0.9
second_decay = 0.999
adam_epsilon = 1e-08
learning_rate = 0.05
weight_decay = 0.1
clip_limit = 1.0
GELU_SCALE = 0.7978845608028654
GELU_CUBE = 0.044715


def dot(a, b, ca, cb):
    return lax.dot_general(a, b, (((ca,), (cb,)), ((), ())), preferred_element_type=F32)


def aligned(start, size):
    return pl.ds(pl.multiple_of(start, size), size)


def greet(peers):
    barrier = pltpu.get_barrier_semaphore()
    for peer in peers:
        pl.semaphore_signal(barrier, inc=1, device_id=peer, device_id_type=MESH)
    pl.semaphore_wait(barrier, len(peers))


def remote(source, target, send_sem, recv_sem, peer):
    return pltpu.make_async_remote_copy(
        src_ref=source,
        dst_ref=target,
        send_sem=send_sem,
        recv_sem=recv_sem,
        device_id=peer,
        device_id_type=MESH,
    )


def vmem(count):
    return [pl.BlockSpec(memory_space=pltpu.VMEM)] * count


def shape(dims, dtype):
    return jax.ShapeDtypeStruct(dims, dtype)


def cost(micros, flops=0):
    return pl.CostEstimate(flops=flops, bytes_accessed=int(micros * 3.0e6), transcendentals=0)


def call(body, name, outs, scratch, ident, micros, megabytes, ins=(), to=()):
    def run(*args):
        return pl.pallas_call(
            body,
            out_shape=outs,
            in_specs=[pl.BlockSpec(memory_space=pltpu.HBM if k in ins else pltpu.VMEM) for k in range(len(args))],
            out_specs=[pl.BlockSpec(memory_space=pltpu.HBM if k in to else pltpu.VMEM) for k in range(len(outs))],
            scratch_shapes=scratch,
            compiler_params=pltpu.CompilerParams(
                collective_id=ident, has_side_effects=True, vmem_limit_bytes=megabytes << 20
            ),
            cost_estimate=cost(micros),
            name=name,
        )(*args)

    return run


def transposed(block):
    return block.astype(F32).T.astype(BF16)


def row_of(mod, start, width, part):
    pieces = []
    for at in range(start, start + width, 128):
        pieces.append(mod[at // part, pl.ds((at % part) // 128, 1), :])
    return jnp.concatenate(pieces, axis=1)


def centred(values):
    center = values - jnp.mean(values, axis=-1, keepdims=True)
    inverse = lax.rsqrt(jnp.mean(center * center, axis=-1, keepdims=True) + norm_epsilon)
    return center * inverse, inverse


def normal_back(grad, normed, inverse):
    return inverse * (
        grad
        - jnp.mean(grad, axis=-1, keepdims=True)
        - normed * jnp.mean(grad * normed, axis=-1, keepdims=True)
    )


class Gather:
    def __init__(self, buf, nf, nc, sems, parts, first=0):
        self.buf, self.nf, self.nc, self.sems = buf, nf, nc, sems
        self.first, self.parts = first, range(first, parts)
        self.columns = buf.shape[2] // parts

    def sem(self, part, kind):
        return self.sems[4 * (part - self.first) + kind]

    def view(self, ctx, part):
        slot = lax.axis_index("fsdp") * self.nc + ctx
        return self.buf.at[slot, :, pl.ds(part * self.columns, self.columns)]

    def along(self, o, part):
        c = lax.axis_index("ctx")
        zs, zr = self.sem(part, 0), self.sem(part, 1)
        view = self.view(c, part)
        return remote(view, view, zs.at[o], zr.at[o], {"ctx": lax.rem(c + o, self.nc)})

    def onward(self, part):
        c = lax.axis_index("ctx")
        zs, zr = self.sem(part, 0), self.sem(part, 1)
        view = self.view(lax.rem(c + 2, self.nc), part)
        up = remote(view, view, zs.at[0], zr.at[3], {"ctx": lax.rem(c + 1, self.nc)})
        down = remote(view, view, zs.at[0], zr.at[1], {"ctx": lax.rem(c + 3, self.nc)})
        return up, down

    def across(self, o, part):
        f, c = lax.axis_index("fsdp"), lax.axis_index("ctx")
        xs, xr = self.sem(part, 2), self.sem(part, 3)
        view = self.view(lax.rem(c - o + self.nc, self.nc), part)
        return [
            remote(view, view, xs.at[fo, o], xr.at[fo, o], {"fsdp": lax.rem(f + fo, self.nf)})
            for fo in range(1, self.nf)
        ]

    def start(self, only=None):
        c = lax.axis_index("ctx")
        for part in self.parts if only is None else (only,):
            self.along(2, part).start()
            pl.when(c != 3)(self.along(1, part).start)
            pl.when(c != 0)(self.along(3, part).start)
            for copy in self.across(0, part):
                copy.start()

    def relay_middle(self, part):
        c = lax.axis_index("ctx")
        self.along(2, part).wait_recv()
        up, down = self.onward(part)
        pl.when(c == 2)(up.start)
        pl.when(c == 1)(down.start)
        for copy in self.across(2, part):
            copy.start()

    def relay_rest(self, part):
        for o in (1, 3):
            self.along(o, part).wait_recv()
            for copy in self.across(o, part):
                copy.start()

    def relay(self):
        for part in self.parts:
            self.relay_middle(part)
        for part in self.parts:
            self.relay_rest(part)

    def arrive(self):
        for part in self.parts:
            for o in range(self.nc):
                for copy in self.across(o, part):
                    copy.wait_recv()

    def drain(self):
        c = lax.axis_index("ctx")
        for part in self.parts:
            for o in range(self.nc):
                for copy in self.across(o, part):
                    copy.wait_send()
            up, down = self.onward(part)
            self.along(2, part).wait_send()
            pl.when(c != 3)(self.along(1, part).wait_send)
            pl.when(c != 0)(self.along(3, part).wait_send)
            pl.when(c == 2)(up.wait_send)
            pl.when(c == 1)(down.wait_send)


def gather_sems(nf, nc, parts):
    return [DMA((nc,)), DMA((nc,)), DMA((nf, nc)), DMA((nf, nc))] * parts


class Sum:
    def __init__(self, sbuf, rbuf, send, recv):
        self.sbuf, self.rbuf, self.send, self.recv = sbuf, rbuf, send, recv
        self.places = tp_places()

    def copy(self, k):
        mine, partner, cross, far = self.places
        peer = cross if k == 2 else partner
        return remote(
            self.sbuf.at[k], self.rbuf.at[k], self.send.at[k], self.recv.at[k], {"tp": peer}
        )

    def give(self, k, value):
        self.sbuf[k] = value.astype(BF16)
        self.copy(k).start()

    def pass_on(self, value):
        self.copy(0).wait_recv()
        self.give(2, value + self.rbuf[0].astype(F32))

    def near(self, value):
        self.copy(1).wait_recv()
        return value + self.rbuf[1].astype(F32)

    def total(self, value):
        self.copy(2).wait_recv()
        return value + self.rbuf[2].astype(F32)

    def drain(self):
        for k in range(3):
            self.copy(k).wait_send()


class Share:
    def __init__(self, slots, send, recv):
        self.slots, self.send, self.recv = slots, send, recv
        self.places = tp_places()

    def copy(self, k):
        mine, partner, cross, far = self.places
        slot, peer = ((mine, cross), (mine, partner), (cross, partner))[k]
        view = self.slots.at[slot]
        return remote(view, view, self.send.at[k], self.recv.at[k], {"tp": peer})

    def start(self):
        self.copy(0).start()
        self.copy(1).start()

    def relay(self):
        self.copy(0).wait_recv()
        self.copy(2).start()

    def finish(self):
        self.copy(1).wait_recv()
        self.copy(2).wait_recv()
        for k in range(3):
            self.copy(k).wait_send()


def share_sems():
    return [DMA((3,)), DMA((3,))]


class Scatter:
    def __init__(self, nf, nc, grad, parts, xland, zland, xsend, xrecv, zsend, zrecv, lanes=None):
        f, c = lax.axis_index("fsdp"), lax.axis_index("ctx")
        self.nf, self.nc, self.grad, self.parts, self.xland, self.zland = (
            nf, nc, grad, parts, xland, zland,
        )
        self.lanes = slice(None) if lanes is None else pl.ds(*lanes)
        keep = self.lanes
        self.swaps, self.deals = [], []
        for fo in range(1, nf) if grad is not None else ():
            member = lax.rem(f + fo, nf)
            self.swaps.append(
                remote(
                    grad.at[member, :, :, keep], xland.at[fo - 1, :, :, keep],
                    xsend.at[fo], xrecv.at[fo], {"fsdp": member},
                )
            )
        for o in (2, 1, 3):
            member = lax.rem(c + o, nc)
            self.deals.append(
                remote(
                    parts.at[member, :, keep], zland.at[o - 1, :, keep], zsend.at[o], zrecv.at[o],
                    {"ctx": member},
                )
            )

    def swap(self):
        for copy in self.swaps:
            copy.start()

    def swapped(self):
        f = lax.axis_index("fsdp")
        for copy in self.swaps:
            copy.wait_recv()
        for k in range(self.nc):
            total = self.grad[f, k, :, self.lanes].astype(F32)
            for fo in range(1, self.nf):
                total = total + self.xland[fo - 1, k, :, self.lanes].astype(F32)
            self.parts[k, :, self.lanes] = total.astype(BF16)

    def deal(self):
        for copy in self.deals:
            copy.start()

    def dealt(self):
        for copy in self.deals:
            copy.wait_recv()
        total = self.parts[lax.axis_index("ctx"), :, self.lanes].astype(F32)
        for o in range(1, self.nc):
            total = total + self.zland[o - 1, :, self.lanes].astype(F32)
        return total

    def drain(self, swaps=True, deals=True):
        for copy in (self.swaps if swaps else []) + (self.deals if deals else []):
            copy.wait_send()


def ring_peers(axis, size):
    here = lax.axis_index(axis)
    return [{axis: lax.rem(here + o, size)} for o in range(1, size)]


def weight_peers(nf, nc):
    f, c = lax.axis_index("fsdp"), lax.axis_index("ctx")
    peers = []
    for o in range(1, nf * nc):
        other = lax.rem(f * nc + c + o, nf * nc)
        peers.append({"fsdp": other // nc, "ctx": lax.rem(other, nc)})
    return peers


def all_peers(nf, nc):
    f, c, t = lax.axis_index("fsdp"), lax.axis_index("ctx"), lax.axis_index("tp")
    count = nf * nc * 4
    peers = []
    for o in range(1, count):
        other = lax.rem((f * nc + c) * 4 + t + o, count)
        peers.append(
            {"fsdp": other // (nc * 4), "ctx": lax.rem(other // 4, nc), "tp": lax.rem(other, 4)}
        )
    return peers


def turned(mine, turn):
    high = lax.rem(mine // 2 + turn // 2, 2)
    return high * 2 + lax.rem(mine + turn, 2)


def tp_places():
    mine = lax.axis_index("tp")
    partner = mine + 1 - 2 * lax.rem(mine, 2)
    cross = lax.rem(mine + 2, 4)
    far = lax.rem(partner + 2, 4)
    return mine, partner, cross, far


def load_all(pairs, sems):
    copies = []
    for k, (source, target) in enumerate(pairs):
        copy = pltpu.make_async_copy(source, target, sems.at[k])
        copy.start()
        copies.append(copy)
    return copies


def head_peers(nc):
    c, t = lax.axis_index("ctx"), lax.axis_index("tp")
    inner = nc * 4
    peers = []
    for o in range(1, inner):
        other = lax.rem(c * 4 + t + o, inner)
        peers.append({"ctx": other // 4, "tp": lax.rem(other, 4)})
    return peers


def forward_body(
    nf, nc, part, tok_hbm, jw_hbm, cond, modw_hbm, cbias, offset, ow_hbm, ew_hbm, bias, sw_hbm,
    hidden_hbm, weight_hbm, mod, out_t_hbm, qkv_hbm, out_hbm, lse, land_hbm, ebuf_hbm,
    value, middle, hidden_two_hbm, sbuf_hbm,
    sweight, sbuf, tok, jweight, modw, oweight, eweight, out_t, qkv, out, ebuf, hidden_two,
    hidden, weight_t, wbuf, obuf, oall, pbuf, pland, normed, joint, stage, land, keys, scores, columns,
    lsem, ssem, psend, precv, msend, mrecv, send, recv, osend, orecv, hsend, hrecv, asend, arecv,
    *gsems,
):
    f, c, t = lax.axis_index("fsdp"), lax.axis_index("ctx"), lax.axis_index("tp")
    mine, partner, cross, far = tp_places()
    group = nf * nc
    slot = f * nc + c
    rows, width = tok.shape
    own = rows // 4
    strips = part // 128
    hd = HEAD_DIM
    step = 128
    loads = load_all(
        (
            (jw_hbm, jweight), (modw_hbm, modw), (tok_hbm, tok), (ow_hbm, oweight),
            (ew_hbm, eweight), (sw_hbm.at[:, pl.ds(0, sweight.shape[1])], sweight),
        ),
        lsem,
    )
    joint_gather = Gather(wbuf, nf, nc, gsems[0:8], 2)
    output_gather = Gather(obuf, nf, nc, gsems[8:12], 1)
    expand_gather = Gather(ebuf, nf, nc, gsems[12:20], 2)
    shrink_gather = Gather(sbuf, nf, nc, gsems[20:24], 1)
    loads[0].wait()
    wbuf[slot] = jweight[...].astype(BF16)
    greet(weight_peers(nf, nc) + head_peers(nc))
    joint_gather.start()
    loads[1].wait()
    partial_mod = dot(cond[...], modw[...].astype(BF16), 1, 0)
    for latent in range(nf):
        for k in range(strips):
            pbuf[latent, pl.ds(k, 1), :] = partial_mod[latent : latent + 1, 128 * k : 128 * k + 128]
    pcopies = []
    for o, peer in zip(range(1, group), weight_peers(nf, nc)):
        copy = remote(pbuf.at[peer["fsdp"]], pland.at[slot], psend.at[o], precv.at[o], peer)
        copy.start()
        pcopies.append(copy)
    pland[slot] = pbuf[f]
    loads[2].wait()

    def norm_rows(k, carry):
        at = aligned(k * step, step)
        normed[at, :] = centred(tok[at, :].astype(F32))[0]
        return carry

    lax.fori_loop(0, rows // 2 // step, norm_rows, 0)
    joint_gather.relay_middle(0)
    lax.fori_loop(rows // 2 // step, rows // step, norm_rows, 0)
    joint_gather.relay_middle(1)
    for copy in pcopies:
        copy.wait_recv()
    total_mod = pland[0]
    for k in range(1, group):
        total_mod = total_mod + pland[k]
    for k in range(strips):
        mod[t, pl.ds(k, 1), :] = total_mod[k : k + 1, :] + cbias[:, 128 * k : 128 * k + 128]
    mcopies = []
    for o, peer in zip(range(1, 4), ring_peers("tp", 4)):
        copy = remote(mod.at[t], mod.at[t], msend.at[o], mrecv.at[o], peer)
        copy.start()
        mcopies.append(copy)
    joint_gather.relay_rest(0)
    for copy in loads[3:]:
        copy.wait()
    obuf[slot] = oweight[...].astype(BF16)
    ebuf[slot] = eweight[...].astype(BF16)
    sbuf[slot] = sweight[...].astype(BF16)
    for copy in mcopies:
        copy.wait_recv()
    shift = row_of(mod, 0, width, part)
    scale = row_of(mod, width, width, part)

    def hide_rows(k, carry):
        at = aligned(k * step, step)
        hidden[at, :] = (normed[at, :] * (1.0 + scale) + shift).astype(BF16)
        return carry

    lax.fori_loop(0, rows // step, hide_rows, 0)
    joint_gather.relay_rest(1)
    joint_gather.arrive()
    deep = jweight.shape[0]
    for k in range(group):
        weight_t[:, k * deep : (k + 1) * deep] = transposed(wbuf[k])

    total = rows * nc
    bq, bk = scores.shape[1], 512
    per = rows // bq

    def query_copy(o):
        dst = lax.rem(c + o, nc)
        return remote(
            joint.at[aligned(dst * 3 * hd, hd), :], qkv.at[pl.ds(0, hd), aligned(c * rows, rows)],
            send.at[1, o], recv.at[1, o], {"ctx": dst},
        )

    copies = []
    biases = offset.shape[1]
    columns[...] = jnp.broadcast_to(offset[...], (128, biases)).T
    for o in (2, 1, 3, 0):
        dst = lax.rem(c + o, nc)
        where = aligned(dst * 3 * hd, 3 * hd)
        pair = columns[aligned(dst * 2 * hd, 2 * hd), 0:1]
        added = jnp.concatenate([pair[0:hd], jnp.zeros((hd, 1), F32), pair[hd : 2 * hd]], axis=0)
        head = (dot(weight_t[where, :], hidden[...], 1, 1) + added).astype(BF16)
        if o == 0:
            qkv[:, aligned(c * rows, rows)] = head
        else:
            joint[where, :] = head
            copy = remote(
                joint.at[pl.ds(pl.multiple_of(dst * 3 * hd + hd, hd), 2 * hd), :],
                qkv.at[pl.ds(hd, 2 * hd), aligned(c * rows, rows)],
                send.at[0, o], recv.at[0, o], {"ctx": dst},
            )
            copy.start()
            copies.append(copy)
    output_gather.start()
    for o in (2, 1, 3):
        query_copy(o).start()
    saves = [
        pltpu.make_async_copy(source, target, ssem.at[k])
        for k, (source, target) in enumerate(
            (
                (hidden, hidden_hbm), (weight_t, weight_hbm), (out_t, out_t_hbm), (qkv, qkv_hbm),
                (out, out_hbm), (land, land_hbm), (ebuf, ebuf_hbm), (sbuf, sbuf_hbm),
                (hidden_two, hidden_two_hbm),
            )
        )
    ]
    saves[0].start()
    saves[1].start()
    weights_share = Share(oall, asend, arecv)
    for copy in copies:
        copy.wait_recv()
    expand_gather.start(0)
    for at in range(0, total, 1024):
        keys[at : at + 1024, :] = transposed(qkv[hd : 2 * hd, at : at + 1024])

    def given(o, k):
        owner, tt = lax.rem(c - o + nc, nc), lax.rem(t + k, 4)
        return remote(
            stage.at[owner, :, aligned(tt * own, own)], land.at[t, c],
            osend.at[o, k], orecv.at[o, k], {"ctx": owner, "tp": tt},
        )

    def block(i, carry):
        turn, sub = i // per, lax.rem(i, per)
        o = jnp.where(turn > 0, 1 + lax.rem(turn, 3), 0)
        owner = lax.rem(c - o + nc, nc)

        @pl.when(jnp.logical_and(sub == 0, turn > 0))
        def _():
            query_copy(o).wait_recv()

        @pl.when(i == per)
        def _():
            output_gather.relay()

        @pl.when(i == per + 1)
        def _():
            output_gather.arrive()
            oall[mine] = obuf[...].reshape(width, nc * hd)
            weights_share.start()

        @pl.when(i == per * nc - 1)
        def _():
            weights_share.relay()

        @pl.when(i == 3 * per)
        def _():
            expand_gather.relay_middle(0)
            saves[3].start()

        where = aligned(owner * rows + sub * bq, bq)
        query = qkv[0:hd, where] * BF16(hd**-0.5)
        peak = None
        for at in range(0, total, bk):
            s = dot(keys[at : at + bk, :], query, 1, 0)
            scores[at : at + bk, :] = s
            high = jnp.max(s.reshape(bk // 8, 8, bq), axis=0)
            peak = high if peak is None else jnp.maximum(peak, high)
        peak = jnp.max(peak, axis=0, keepdims=True)
        acc, mass = None, None
        for at in range(0, total, bk):
            p = jnp.exp(scores[at : at + bk, :] - peak)
            low = jnp.sum(p.reshape(bk // 8, 8, bq), axis=0)
            mass = low if mass is None else mass + low
            term = dot(qkv[2 * hd : 3 * hd, at : at + bk], p.astype(BF16), 1, 0)
            acc = term if acc is None else acc + term
        mass = jnp.sum(mass, axis=0, keepdims=True)
        acc = acc * (1.0 / mass)
        out[:, where] = acc
        lse[:, where] = peak + jnp.log(mass)
        stage[owner, :, aligned(sub * bq, bq)] = acc.astype(BF16)

        @pl.when(sub == per - 1)
        def _():
            pl.when(turn > 0)(given(o, 0).start)
            for k in range(1, 4):
                given(o, k).start()

        return carry

    lax.fori_loop(0, per * nc, block, 0)
    expand_gather.start(1)
    shrink_gather.start()
    land[t, c] = stage[c, :, aligned(t * own, own)]
    expand_gather.relay_rest(0)
    weights_share.finish()
    for k in range(4):
        out_t[k] = transposed(oall[k])
    saves[2].start()
    saves[4].start()

    order = [(o, k) for o in (0, 2, 3, 1) for k in range(4) if o or k]
    for o, k in order:
        given(o, k).wait_recv()
    held = bias[0:1, :]
    for k in range(4):
        block_ = land[k].reshape(nc * hd, own)
        held = held + dot(block_.astype(F32).T.astype(BF16), out_t[k], 1, 0)
    value[...] = held
    gate = row_of(mod, 2 * width, width, part)
    shift = row_of(mod, 3 * width, width, part)
    scale = row_of(mod, 4 * width, width, part)
    mid = tok[aligned(mine * own, own), :].astype(F32) + gate * held
    middle[...] = mid
    hidden_two[mine] = (centred(mid)[0] * (1.0 + scale) + shift).astype(BF16)
    sharing = Share(hidden_two, hsend, hrecv)
    sharing.start()
    saves[5].start()
    expand_gather.relay_middle(1)
    shrink_gather.relay_middle(0)
    expand_gather.relay_rest(1)
    shrink_gather.relay_rest(0)
    sharing.relay()
    for o, k in order:
        given(o, k).wait_send()
    for o in (2, 1, 3):
        query_copy(o).wait_send()
    for copy in pcopies + mcopies + copies:
        copy.wait_send()
    expand_gather.arrive()
    saves[6].start()
    sharing.finish()
    saves[8].start()
    shrink_gather.arrive()
    saves[7].start()
    for copy in saves:
        copy.wait()
    for gather in (joint_gather, output_gather, expand_gather, shrink_gather):
        gather.drain()


def forward(nf, nc, part, tok, jweight, cond, modw, cbias, offset, oweight, eweight, bias, sweight):
    rows, width = tok.shape
    deep, columns = jweight.shape
    group = nf * nc
    own = rows // 4
    total = rows * nc
    hd = HEAD_DIM
    bq = min(512, rows)
    high = -(-part // 1024) * 8
    return call(
        partial(forward_body, nf, nc, part),
        "forward",
        (
            shape((rows, width), BF16),
            shape((columns, width), BF16),
            shape((4, high, 128), F32),
            shape((4, nc * hd, width), BF16),
            shape((3 * hd, total), BF16),
            shape((hd, total), F32),
            shape((1, total), F32),
            shape((4, nc, hd, own), BF16),
            shape((group,) + eweight.shape, BF16),
            shape((own, width), F32),
            shape((own, width), F32),
            shape((4, own, width), BF16),
            shape((group, deep, sweight.shape[1] // 2), BF16),
        ),
        [
            pltpu.VMEM((deep, sweight.shape[1] // 2), F32),
            pltpu.VMEM((group, deep, sweight.shape[1] // 2), BF16),
            pltpu.VMEM(tok.shape, BF16),
            pltpu.VMEM(jweight.shape, F32),
            pltpu.VMEM(modw.shape, F32),
            pltpu.VMEM(oweight.shape, F32),
            pltpu.VMEM(eweight.shape, F32),
            pltpu.VMEM((4, nc * hd, width), BF16),
            pltpu.VMEM((3 * hd, total), BF16),
            pltpu.VMEM((hd, total), F32),
            pltpu.VMEM((group,) + eweight.shape, BF16),
            pltpu.VMEM((4, own, width), BF16),
            pltpu.VMEM((rows, width), BF16),
            pltpu.VMEM((columns, width), BF16),
            pltpu.VMEM((group, deep, columns), BF16),
            pltpu.VMEM((group,) + oweight.shape, BF16),
            pltpu.VMEM((4, width, nc * hd), BF16),
            pltpu.VMEM((nf, high, 128), F32),
            pltpu.VMEM((group, high, 128), F32),
            pltpu.VMEM((rows, width), F32),
            pltpu.VMEM((columns, rows), BF16),
            pltpu.VMEM((nc, hd, rows), BF16),
            pltpu.VMEM((4, nc, hd, own), BF16),
            pltpu.VMEM((total, hd), BF16),
            pltpu.VMEM((total, bq), F32),
            pltpu.VMEM((offset.shape[1], 128), F32),
            DMA((6,)), DMA((9,)),
            DMA((group,)), DMA((group,)), DMA((4,)), DMA((4,)),
            DMA((2, nc)), DMA((2, nc)), DMA((nc, 4)), DMA((nc, 4)), DMA((3,)), DMA((3,)),
        ]
        + share_sems()
        + gather_sems(nf, nc, 6),
        1,
        150,
        60,
        ins=(0, 1, 3, 6, 7, 9),
        to=(0, 1, 3, 4, 5, 7, 8, 11, 12),
    )(tok, jweight, cond, modw, cbias, offset, oweight, eweight, bias, sweight)


def branch_body(
    nf, nc, part, hidden_hbm, cot_hbm, expand_hbm, sw_hbm, sbuf_hbm, hbias, mod, middle, value,
    attn_own, mid_grad, shrink_half, shrink_late, expand_grad, stats, hstats, sh_cross, sh_own,
    cot, hidden, expand, sweight, sgat, gbuf, abuf, ebuf, slopes, held_buf,
    shrink_grad, shrink_parts, sland, dland, sbuf, rbuf, shold,
    lsem, tsend, trecv, send, recv, s1s, s1r, d1s, d1r, *gsems,
):
    mine, partner, cross, far = tp_places()
    own, width = middle.shape
    group = nf * nc
    deep, units = sweight.shape
    slot = lax.axis_index("fsdp") * nc + lax.axis_index("ctx")
    gate_first = row_of(mod, 2 * width, width, part)
    scale_second = row_of(mod, 4 * width, width, part)
    gate_second = row_of(mod, 5 * width, width, part)
    split = units // 2
    loads = load_all(
        (
            (sw_hbm, sweight), (hidden_hbm, hidden), (expand_hbm, expand), (cot_hbm, cot),
            (sbuf_hbm, sgat.at[:, :, pl.ds(0, split)]),
        ),
        lsem,
    )
    loads[0].wait()
    sgat[slot, :, split:units] = sweight[:, split:units].astype(BF16)
    greet(ring_peers("tp", 4) + weight_peers(nf, nc))
    gather = Gather(sgat, nf, nc, gsems, 2, 1)
    gather.start()
    for copy in loads[1:]:
        copy.wait()
    tile = 32

    def ahead(turn, carry):
        at = turned(mine, turn)

        @pl.when(turn == 2)
        def _():
            gather.relay_middle(1)


        where = aligned(at * own, own)
        weight = expand[...].reshape(width, units)
        slopes[where, :] = dot(hidden[at], weight, 1, 0) + hbias[...]

        def curve(k, carry_):
            row = pl.ds(pl.multiple_of(at * own + k * tile, tile), tile)
            u = slopes[row, :]
            squared = u * u
            th = jnp.tanh(GELU_SCALE * (u + GELU_CUBE * squared * u))
            abuf[row, :] = (0.5 * u * (1.0 + th)).astype(BF16)
            slopes[row, :] = 0.5 * (1.0 + th) + 0.5 * u * (1.0 - th * th) * (
                GELU_SCALE * (1.0 + 3.0 * GELU_CUBE * squared)
            )
            gbuf[row, :] = (gate_second * cot[row, :].astype(F32)).astype(BF16)
            return carry_

        lax.fori_loop(0, own // tile, curve, 0)
        return carry

    lax.fori_loop(0, 4, ahead, 0)
    gather.relay_rest(1)
    step = 256
    for at in range(0, width, step):
        block = dot(gbuf[:, at : at + step], abuf[...], 0, 0).astype(BF16)
        for k in range(at // deep, (at + step) // deep):
            rows_k = slice(k * deep - at, (k + 1) * deep - at)
            shrink_grad[k // nc, k % nc] = block[rows_k, 0:split]
            shrink_late[k // nc, k % nc] = block[rows_k, split:units]
    early = Scatter(nf, nc, shrink_grad, shrink_parts, sland, dland, s1s, s1r, d1s, d1r)
    early.swap()
    gather.arrive()
    hstats[...] = jnp.zeros_like(hstats)
    summing = Sum(sbuf, rbuf, send, recv)

    def back_turn(turn, carry):
        at = turned(mine, 3 - turn)
        where = aligned(at * own, own)
        weight = sgat[...].reshape(width, units)
        pull = dot(gbuf[where, :], weight, 1, 0) * slopes[where, :]
        hstats[...] += jnp.sum(pull, axis=0, keepdims=True)
        pull = pull.astype(BF16)
        ebuf[where, :] = pull
        held_buf[...] = dot(pull, expand[...].reshape(width, units), 1, 1)

        @pl.when(turn == 0)
        def _():
            summing.give(0, held_buf[...])

        @pl.when(turn == 1)
        def _():
            summing.pass_on(held_buf[...])

        @pl.when(turn == 2)
        def _():
            summing.give(1, held_buf[...])

        return carry

    lax.fori_loop(0, 4, back_turn, 0)
    copies = []
    for turn, at in enumerate((far, partner)):
        weight = sgat[...].reshape(width, units)
        shold[turn] = dot(abuf[aligned(at * own, own), :], weight, 1, 1).astype(BF16)
        copy = remote(
            shold.at[turn], shold.at[2 + turn], tsend.at[turn], trecv.at[turn], {"tp": partner}
        )
        copy.start()
        copies.append(copy)
    flat = hidden.shape[0] * own
    for at in range(0, width, step):
        expand_grad[at : at + step, :] = dot(
            hidden[:, :, at : at + step].reshape(flat, step), ebuf[...], 0, 0
        ).astype(BF16)
    early.swapped()
    early.deal()
    weight = sgat[...].reshape(width, units)
    forth = dot(abuf[aligned(cross * own, own), :], weight, 1, 1)
    copies[0].wait_recv()
    sh_cross[...] = (forth + shold[2].astype(F32)).astype(BF16)
    forth = dot(abuf[aligned(mine * own, own), :], weight, 1, 1)
    copies[1].wait_recv()
    sh_own[...] = forth + shold[3].astype(F32)
    mine_rows = cot[aligned(mine * own, own), :].astype(F32)
    stats[3:4, :] = jnp.sum(gate_second * mine_rows, axis=0, keepdims=True)
    normed, inverse = centred(middle[...])
    grad_in = summing.total(summing.near(held_buf[...]))
    stats[0:1, :] = jnp.sum(grad_in, axis=0, keepdims=True)
    stats[1:2, :] = jnp.sum(grad_in * normed, axis=0, keepdims=True)
    mgrad = mine_rows + normal_back(grad_in * (1.0 + scale_second), normed, inverse)
    mid_grad[...] = mgrad
    agrad = gate_first * mgrad
    attn_own[...] = agrad.astype(BF16)
    stats[2:3, :] = jnp.sum(mgrad * value[...], axis=0, keepdims=True)
    stats[4:5, :] = jnp.sum(agrad, axis=0, keepdims=True)
    stats[5:8, :] = jnp.zeros((3, width), F32)
    shrink_half[...] = early.dealt()
    early.drain()
    summing.drain()
    gather.drain()
    for copy in copies:
        copy.wait_send()


def branch(nf, nc, part, hidden, cot, expand, sweight, sbuf, hbias, mod, middle, value):
    rows, width = cot.shape
    own = rows // 4
    deep, units = sweight.shape
    group = nf * nc
    return call(
        partial(branch_body, nf, nc, part),
        "branch",
        (
            shape((own, width), BF16),
            shape((own, width), F32),
            shape((deep, units // 2), F32),
            shape((nf, nc, deep, units // 2), BF16),
            shape((width, units), BF16),
            shape((8, width), F32),
            shape((1, units), F32),
            shape((own, width), BF16),
            shape((own, width), F32),
        ),
        [
            pltpu.VMEM((rows, width), BF16),
            pltpu.VMEM((4, own, width), BF16),
            pltpu.VMEM((group, deep, units), BF16),
            pltpu.VMEM((deep, units), F32),
            pltpu.VMEM((group, deep, units), BF16),
            pltpu.VMEM((rows, width), BF16),
            pltpu.VMEM((rows, units), BF16),
            pltpu.VMEM((rows, units), BF16),
            pltpu.VMEM((rows, units), F32),
            pltpu.VMEM((own, width), F32),
            pltpu.VMEM((nf, nc, deep, units // 2), BF16),
            pltpu.VMEM((nc, deep, units // 2), BF16),
            pltpu.VMEM((nf - 1, nc, deep, units // 2), BF16),
            pltpu.VMEM((nc - 1, deep, units // 2), BF16),
            pltpu.VMEM((3, own, width), BF16),
            pltpu.VMEM((3, own, width), BF16),
            pltpu.VMEM((4, own, width), BF16),
            DMA((5,)), DMA((2,)), DMA((2,)),
        ]
        + share_sems()
        + [DMA((nf,))] * 2
        + [DMA((nc,))] * 2
        + gather_sems(nf, nc, 1),
        2,
        40,
        60,
        ins=(0, 1, 2, 3, 4),
    )(hidden, cot, expand, sweight, sbuf, hbias, mod, middle, value)


def backward_body(
    nf, nc, part, attn_own, out_t_hbm, heads_hbm, qkv_hbm, out_hbm, lse, sh_cross, sh_own, middle,
    cot_hbm, mod, bias, shrink_half, shrink_grad, expand_grad, weight_hbm, hidden_hbm, tok_hbm,
    mid_grad, stats_second, hidden_stats, modw_hbm, low,
    mixed, tokens_grad, shrink_sum, expand_sum, output_sum, joint_sum, modulate_sum,
    bias_rows, done,
    out_t, qkv, out, heads, att, cot_own, tok_own, weight_t, hidden, modw,
    attn_low, dout, dost, keys, vals, dq, dkv, stage, rland, delta, output_grad,
    sland, shrink_parts, eland, oland, expand_parts, output_parts, sdeal, edeal, odeal, joint_grad, sbuf, rbuf,
    kvgrad, kvland, kvparts, kvdeal, qgrad, qland, qparts, qdeal, pieces, land, total_piece, gathered, ftotal, gate_row,
    lsem, send, recv, jsend, jrecv, csend, crecv, gsend, grecv, tsend, trecv, hsend, hrecv,
    lowsend, lowrecv, hsend2, hrecv2, x1s, x1r, x2s, x2r, x3s, x3r, x4s, x4r, x5s, x5r, x6s, x6r,
    d1s, d1r, d2s, d2r, d3s, d3r, d4s, d4r, d5s, d5r, d6s, d6r, asend, arecv, bsend, brecv, f1s, f1r,
):
    f, c, t = lax.axis_index("fsdp"), lax.axis_index("ctx"), lax.axis_index("tp")
    mine, partner, cross, far = tp_places()
    own, width = middle.shape
    rows = 4 * own
    total = rows * nc
    hd = HEAD_DIM
    inner, group = nc * 4, nf * nc
    here, slot = c * 4 + t, f * nc + c
    bk = bq = 512
    per = rows // bk
    deep = joint_sum.shape[0]
    heads_wide = nc * hd
    units = expand_grad.shape[3]
    half = units // 2
    shrink = Scatter(nf, nc, shrink_grad, shrink_parts, sland, sdeal, x6s, x6r, d1s, d1r)
    early = Scatter(
        nf, nc, expand_grad, expand_parts, eland, edeal, x1s, x1r, d2s, d2r, (0, half)
    )
    late = Scatter(
        nf, nc, expand_grad, expand_parts, eland, edeal, x2s, x2r, d3s, d3r, (half, half)
    )
    project = Scatter(nf, nc, output_grad, output_parts, oland, odeal, x3s, x3r, d4s, d4r)
    kv = Scatter(nf, nc, kvgrad, kvparts, kvland, kvdeal, x4s, x4r, d5s, d5r)
    query = Scatter(nf, nc, qgrad, qparts, qland, qdeal, x5s, x5r, d6s, d6r)
    own_rows = aligned(mine * own, own)
    loads = load_all(
        (
            (out_t_hbm, out_t), (qkv_hbm, qkv), (out_hbm, out), (heads_hbm, heads),
            (cot_hbm.at[own_rows, :], cot_own), (tok_hbm.at[own_rows, :], tok_own),
            (weight_hbm, weight_t), (hidden_hbm, hidden), (modw_hbm, modw),
        ),
        lsem,
    )
    attn_low[mine] = attn_own[...]
    loads[0].wait()
    for k in range(4):
        dost[k] = dot(out_t[k], attn_own[...], 1, 1).astype(BF16).reshape(nc, hd, own)
    greet(all_peers(nf, nc))
    where_own = aligned(c * rows + t * own, own)

    def send_out(o, k):
        cc, tt = lax.rem(c + o, nc), lax.rem(t + k, 4)
        return remote(
            dost.at[tt, cc], dout.at[:, where_own], send.at[o, k], recv.at[o, k],
            {"ctx": cc, "tp": tt},
        )

    order = [(o, k) for o in (0, 2, 1, 3) for k in range(4) if o or k]
    shrink.swap()
    for o, k in order:
        send_out(o, k).start()
    low_share = Share(attn_low, lowsend, lowrecv)
    low_share.start()
    crossing = remote(sh_cross, rland, csend, crecv, {"tp": cross})
    early.swap()
    dout[:, where_own] = dost[t, c]
    for copy in loads[1:4]:
        copy.wait()
    for at in range(0, total, 1024):
        keys[at : at + 1024, :] = transposed(qkv[hd : 2 * hd, at : at + 1024])
        vals[at : at + 1024, :] = transposed(qkv[2 * hd : 3 * hd, at : at + 1024])
    dq[...] = jnp.zeros_like(dq)
    dkv[...] = jnp.zeros_like(dkv)
    sharing = Share(mixed, gsend, grecv)
    exchange = [
        remote(heads.at[peer["tp"]], att.at[:, :, own_rows], hsend2.at[k], hrecv2.at[k], peer)
        for k, peer in zip(range(1, 4), ring_peers("tp", 4))
    ]

    def kv_back(o, owner):
        return remote(
            stage.at[owner, pl.ds(hd, 2 * hd), :], joint_grad.at[c, pl.ds(hd, 2 * hd), :],
            jsend.at[0, o], jrecv.at[0, o], {"ctx": owner},
        )

    def q_back(o, owner):
        return remote(
            stage.at[owner, pl.ds(0, hd), :], joint_grad.at[c, pl.ds(0, hd), :],
            jsend.at[1, o], jrecv.at[1, o], {"ctx": owner},
        )

    count = per * nc

    def block(i, vsum):
        turn, step = i // count, lax.rem(i, count)
        owners = (lax.rem(c + turn * (nc - 1), nc), lax.rem(c + 2 + turn * (nc - 1), nc))

        @pl.when(i == 0)
        def _():
            for o, k in order:
                if o in (0, 2):
                    send_out(o, k).wait_recv()

        @pl.when(i == count)
        def _():
            for o, k in order:
                if o in (1, 3):
                    send_out(o, k).wait_recv()

        @pl.when(step == 0)
        def _():
            for owner in owners:
                where_q = aligned(owner * rows, rows)
                delta[:, where_q] = jnp.sum(
                    dout[:, where_q].astype(F32) * out[:, where_q], axis=0, keepdims=True
                )

        o = 1 + step // per
        owner = lax.rem(c + o, nc)
        sub = lax.rem(step, per)
        where = aligned(owner * rows + sub * bk, bk)
        key, val, key_t = keys[where, :], vals[where, :], qkv[hd : 2 * hd, where]
        dk, dv = dkv[0:hd, where], dkv[hd : 2 * hd, where]
        for source in owners:
            for half_ in range(rows // bq):
                at = aligned(source * rows + half_ * bq, bq)
                query = qkv[0:hd, at] * BF16(hd**-0.5)
                grad = dout[:, at]
                p = jnp.exp(dot(key, query, 1, 0) - lse[:, at])
                ds = (p * (dot(val, grad, 1, 0) - delta[:, at])).astype(BF16)
                dv = dv + dot(grad, p.astype(BF16), 1, 1)
                dk = dk + dot(query, ds, 1, 1)
                dq[:, at] += dot(key_t, ds, 1, 0)
        dkv[0:hd, where] = dk
        dkv[hd : 2 * hd, where] = dv
        put = aligned(sub * bk, bk)

        @pl.when(turn == 1)
        def _():
            stage[owner, hd : 2 * hd, put] = dkv[0:hd, where].astype(BF16)
            stage[owner, 2 * hd : 3 * hd, put] = dkv[hd : 2 * hd, where].astype(BF16)

        @pl.when(jnp.logical_and(turn == 1, jnp.logical_and(sub == per - 1, o < nc)))
        def _():
            kv_back(o, owner).start()

        @pl.when(i == 1)
        def _():
            shrink.swapped()
            shrink.deal()

        @pl.when(i == 0)
        def _():
            att[:, :, own_rows] = heads[t]
            for copy in exchange:
                copy.start()

        @pl.when(i == 2)
        def _():
            low_share.relay()
            crossing.start()

        @pl.when(i == 8)
        def _():
            crossing.wait_recv()
            loads[4].wait()
            value = sh_own[...] + rland[...].astype(F32) + bias[1:2, :]
            gate = row_of(mod, 5 * width, width, part)
            mixed[mine] = (middle[...] + gate * value).astype(BF16)
            sharing.start()
            gate_row[...] = jnp.sum(
                cot_own[...].astype(F32) * value, axis=0, keepdims=True
            )

        @pl.when(i == 3)
        def _():
            early.swapped()
            early.deal()
            late.swap()

        @pl.when(i == 6)
        def _():
            for k in (1, 2):
                low_share.copy(k).wait_recv()
            for copy in exchange:
                copy.wait_recv()
            flat = dot(
                att[...].reshape(heads_wide, rows), attn_low[...].reshape(rows, width), 1, 0
            ).T.astype(BF16)
            output_grad[...] = flat.reshape(output_grad.shape)
            project.swap()

        @pl.when(i == count - 1)
        def _():
            for source in owners:
                stage[source, 0:hd, :] = (
                    dq[:, aligned(source * rows, rows)] * (hd**-0.5)
                ).astype(BF16)
            q_back(2, owners[1]).start()

        @pl.when(i == 9)
        def _():
            late.swapped()

        @pl.when(i == 11)
        def _():
            project.swapped()

        @pl.when(i == 14)
        def _():
            sharing.relay()

        return vsum

    lax.fori_loop(0, 2 * count, block, 0)
    for o in (1, 3):
        owner = lax.rem(c + o, nc)
        stage[owner, 0:hd, :] = (dq[:, aligned(owner * rows, rows)] * (hd**-0.5)).astype(BF16)
        q_back(o, owner).start()
    qsum = jnp.sum(dq[...] * (hd**-0.5), axis=1, keepdims=True)
    vsum = jnp.sum(dkv[hd : 2 * hd, :], axis=1, keepdims=True)
    late.deal()
    project.deal()
    joint_grad[c] = stage[c]
    bias_column = jnp.concatenate([qsum, vsum], axis=0)
    for copy in loads[5:]:
        copy.wait()
    rows_f = width // nf

    def weight_grad(scatter, source, into):
        flat_grad = source.reshape(-1, rows)

        def put(lanes, member, first, count):
            block_ = dot(flat_grad, hidden[:, lanes], 1, 0).T.astype(BF16)
            for k in range(count):
                row = (member, first + k) if member is not None else divmod(first + k, nc)
                into[row[0], row[1]] = block_[k * deep : (k + 1) * deep, :]

        if rows_f % 128:
            for at in range(0, width, 256):
                put(pl.ds(at, 256), None, at // deep, 256 // deep)
            scatter.swap()
            return
        wide_step = min(256, rows_f)
        for o in range(1, nf + 1):
            member = lax.rem(f + o, nf)
            for at in range(0, rows_f, wide_step):
                put(
                    aligned(member * rows_f + at, wide_step), member, at // deep, wide_step // deep
                )
            if o < nf:
                scatter.swaps[o - 1].start()

    for o in range(1, nc):
        kv_back(o, lax.rem(c + o, nc)).wait_recv()
    weight_grad(kv, joint_grad[:, hd : 3 * hd, :], kvgrad)
    shrink_total = shrink.dealt()
    shrink_sum[:, 0:half] = shrink_half[...]
    shrink_sum[:, half:units] = shrink_total
    squares = jnp.sum(shrink_total * shrink_total) + jnp.sum(shrink_half[...] * shrink_half[...])
    for o in range(1, nc):
        q_back(o, lax.rem(c + o, nc)).wait_recv()

    columns = weight_t.shape[0]

    def piece_of(at):
        block_ = joint_grad[:, :, aligned(at * own, own)].reshape(columns, own)
        return dot(block_.astype(F32).T.astype(BF16), weight_t[...], 1, 0)

    summing = Sum(sbuf, rbuf, tsend, trecv)
    summing.give(0, piece_of(far))
    summing.give(1, piece_of(partner))
    summing.pass_on(piece_of(cross))
    weight_grad(query, joint_grad[:, 0:hd, :], qgrad)
    held = summing.near(piece_of(mine))
    kv.swapped()
    kv.deal()
    normed, inverse = centred(tok_own[...].astype(F32))
    grad_in = summing.total(held)
    scale = row_of(mod, width, width, part)
    shift_row = jnp.sum(grad_in, axis=0, keepdims=True)
    scale_row = jnp.sum(grad_in * normed, axis=0, keepdims=True)

    slim = part // nc // 128
    share = 2 * width // nc // 128
    hshare = hidden_stats.shape[1] // nc // 128
    last = slim + share + hshare
    vectors = [
        shift_row, scale_row, stats_second[2:3, :],
        stats_second[0:1, :], stats_second[1:2, :], gate_row[...],
    ]
    residual = [stats_second[4:5, :], stats_second[3:4, :]]
    pieces[...] = jnp.zeros_like(pieces)
    for cc in range(nc):
        for tt in range(4):
            k = cc * 4 + tt
            for n in range(slim):
                at = ((tt * part // 128) + cc * slim + n) * 128
                pieces[k, n : n + 1, :] = vectors[at // width][:, at % width : at % width + 128]
            for n in range(share):
                at = (cc * share + n) * 128
                pieces[k, slim + n : slim + n + 1, :] = residual[at // width][
                    :, at % width : at % width + 128
                ]
        for n in range(hshare):
            at = (cc * hshare + n) * 128
            pieces[cc * 4 + t, slim + share + n : slim + share + n + 1, :] = hidden_stats[
                :, at : at + 128
            ]
    pieces[here, last : last + 1, :] = jnp.broadcast_to(bias_column, (2 * hd, 128)).T[0:1, :]
    first = []
    for o in range(1, inner):
        other = lax.rem(here + o, inner)
        copy = remote(
            pieces.at[other], land.at[here], asend.at[o], arecv.at[o],
            {"ctx": other // 4, "tp": lax.rem(other, 4)},
        )
        copy.start()
        first.append(copy)
    tokens_grad[mine] = (
        mid_grad[...] + normal_back(grad_in * (1.0 + scale), normed, inverse)
    ).astype(BF16)
    token_share = Share(tokens_grad, hsend, hrecv)
    token_share.start()
    query.swapped()
    query.deal()
    land[here] = pieces[here]
    for copy in first:
        copy.wait_recv()
    acc = land[0]
    for k in range(1, inner):
        acc = acc + land[k]
    total_piece[...] = acc
    gathered[slot] = acc
    second = []
    for o, peer in zip(range(1, group), weight_peers(nf, nc)):
        copy = remote(total_piece, gathered.at[slot], bsend.at[o], brecv.at[o], peer)
        copy.start()
        second.append(copy)
    expand_total = early.dealt()
    expand_sum[:, 0:half] = expand_total
    squares = squares + jnp.sum(expand_total * expand_total)
    expand_total = late.dealt()
    expand_sum[:, half:units] = expand_total
    squares = squares + jnp.sum(expand_total * expand_total)
    output_total = project.dealt()
    output_sum[...] = output_total
    squares = squares + jnp.sum(output_total * output_total)
    for copy in second:
        copy.wait_recv()

    grads = []
    for latent in range(nf):
        strips = []
        for cc in range(nc):
            for n in range(slim):
                strips.append(gathered[latent * nc + cc, n : n + 1, :])
        grads.append(jnp.concatenate(strips, axis=1))
    condition_bias = grads[0]
    for latent in range(1, nf):
        condition_bias = condition_bias + grads[latent]
    bias_rows[...] = jnp.zeros_like(bias_rows)
    bias_rows[0:1, 0:part] = condition_bias
    factors = low[...].T
    wide = modw[...].astype(BF16).astype(F32)
    outer = None
    ftotal[...] = jnp.zeros_like(ftotal)
    for latent in range(nf):
        term = factors[:, latent : latent + 1] * grads[latent]
        outer = term if outer is None else outer + term
        column = jnp.sum(wide * grads[latent], axis=1, keepdims=True)
        ftotal[latent : latent + 1, 0:deep] = jnp.broadcast_to(column, (deep, 128)).T[0:1, :]
    modulate_sum[...] = outer
    squares = squares + jnp.sum(outer * outer)

    def over(at, count):
        found = []
        for cc in range(nc):
            value = None
            for latent in range(nf):
                block_ = gathered[latent * nc + cc, at : at + count, :]
                value = block_ if value is None else value + block_
            for n in range(count):
                found.append(value[n : n + 1, :])
        return jnp.concatenate(found, axis=1)

    residual_sum = over(slim, share)
    hidden_sum = over(slim + share, hshare)
    head_sum = over(last, 1)
    bias_rows[1:2, 0 : hidden_sum.shape[1]] = hidden_sum
    bias_rows[2:3, 0 : head_sum.shape[1]] = head_sum
    bias_rows[3:4, 0:width] = residual_sum[:, 0:width]
    bias_rows[4:5, 0:width] = residual_sum[:, width : 2 * width]
    lead = (slot == 0).astype(F32)
    tensor_lead = (t == 0).astype(F32)
    squares = squares + lead * (
        jnp.sum(condition_bias * condition_bias)
        + jnp.sum(hidden_sum * hidden_sum)
        + jnp.sum(head_sum * head_sum)
        + tensor_lead * jnp.sum(residual_sum * residual_sum)
    )
    token_share.relay()
    kv_total, q_total = kv.dealt(), query.dealt()
    squares = squares + jnp.sum(kv_total * kv_total) + jnp.sum(q_total * q_total)
    ftotal[nf : nf + 1, :] = jnp.full((1, 128), squares)
    third = []
    for o, peer in zip(range(1, group * 4), all_peers(nf, nc)):
        copy = remote(ftotal, done.at[slot, t], f1s.at[o], f1r.at[o], peer)
        copy.start()
        third.append(copy)
    done[slot, t] = ftotal[...]
    kv_total, q_total = kv_total.T, q_total.T
    blocks = []
    for k in range(nc):
        blocks += [q_total[k * hd : (k + 1) * hd], kv_total[k * 2 * hd : (k + 1) * 2 * hd]]
    joint_sum[...] = jnp.concatenate(blocks, axis=0).T
    sharing.finish()
    token_share.finish()
    summing.drain()
    for o in range(1, nc):
        owner = lax.rem(c + o, nc)
        kv_back(o, owner).wait_send()
        q_back(o, owner).wait_send()
    for o, k in order:
        send_out(o, k).wait_send()
    for k in range(3):
        low_share.copy(k).wait_send()
    for copy in exchange:
        copy.wait_send()
    crossing.wait_send()
    for scatter in (shrink, early, late, project, kv, query):
        scatter.drain()
    for copy in third:
        copy.wait_recv()
    for copy in first + second + third:
        copy.wait_send()


def backward(
    nf, nc, part, attn_own, out_t, att, qkv, out, lse, sh_cross, sh_own, middle, cot, mod, bias,
    shrink_half, shrink_grad, expand_grad, weight_t, hidden, tok, mid_grad, stats_second, hidden_stats,
    modw, low,
):
    rows, width = cot.shape
    own = rows // 4
    total = rows * nc
    hd = HEAD_DIM
    inner, group = nc * 4, nf * nc
    deep = width // group
    units = expand_grad.shape[1]
    columns = weight_t.shape[0]
    heads_wide = nc * hd
    expand_grad = expand_grad.reshape(nf, nc, deep, units)
    high = -(-(part // nc + 2 * width // nc + hidden_stats.shape[1] // nc + 128) // 1024) * 8
    tall = -(-(nf + 1) // 8) * 8
    return call(
        partial(backward_body, nf, nc, part),
        "backward",
        (
            shape((4, own, width), BF16),
            shape((4, own, width), BF16),
            shape((deep, units), F32),
            shape((deep, units), F32),
            shape((deep, heads_wide), F32),
            shape((deep, columns), F32),
            shape((deep, part), F32),
            shape((8, max(part, width, hidden_stats.shape[1])), F32),
            shape((group, 4, tall, 128), F32),
        ),
        [
            pltpu.VMEM(out_t.shape, BF16),
            pltpu.VMEM(qkv.shape, BF16),
            pltpu.VMEM(out.shape, F32),
            pltpu.VMEM(att.shape, BF16),
            pltpu.VMEM((nc, hd, rows), BF16),
            pltpu.VMEM((own, width), BF16),
            pltpu.VMEM((own, width), BF16),
            pltpu.VMEM(weight_t.shape, BF16),
            pltpu.VMEM(hidden.shape, BF16),
            pltpu.VMEM(modw.shape, F32),
            pltpu.VMEM((4, own, width), BF16),
            pltpu.VMEM((hd, total), BF16),
            pltpu.VMEM((4, nc, hd, own), BF16),
            pltpu.VMEM((total, hd), BF16),
            pltpu.VMEM((total, hd), BF16),
            pltpu.VMEM((hd, total), F32),
            pltpu.VMEM((2 * hd, total), F32),
            pltpu.VMEM((nc, 3 * hd, rows), BF16),
            pltpu.VMEM((own, width), BF16),
            pltpu.VMEM((1, total), F32),
            pltpu.VMEM((nf, nc, deep, heads_wide), BF16),
            pltpu.VMEM((nf - 1, nc, deep, units // 2), BF16),
            pltpu.VMEM((nc, deep, units // 2), BF16),
            pltpu.VMEM((nf - 1, nc, deep, units), BF16),
            pltpu.VMEM((nf - 1, nc, deep, heads_wide), BF16),
            pltpu.VMEM((nc, deep, units), BF16),
            pltpu.VMEM((nc, deep, heads_wide), BF16),
            pltpu.VMEM((nc - 1, deep, units // 2), BF16),
            pltpu.VMEM((nc - 1, deep, units), BF16),
            pltpu.VMEM((nc - 1, deep, heads_wide), BF16),
            pltpu.VMEM((nc, 3 * hd, rows), BF16),
            pltpu.VMEM((3, own, width), BF16),
            pltpu.VMEM((3, own, width), BF16),
            pltpu.VMEM((nf, nc, deep, 2 * heads_wide), BF16),
            pltpu.VMEM((nf - 1, nc, deep, 2 * heads_wide), BF16),
            pltpu.VMEM((nc, deep, 2 * heads_wide), BF16),
            pltpu.VMEM((nc - 1, deep, 2 * heads_wide), BF16),
            pltpu.VMEM((nf, nc, deep, heads_wide), BF16),
            pltpu.VMEM((nf - 1, nc, deep, heads_wide), BF16),
            pltpu.VMEM((nc, deep, heads_wide), BF16),
            pltpu.VMEM((nc - 1, deep, heads_wide), BF16),
            pltpu.VMEM((inner, high, 128), F32),
            pltpu.VMEM((inner, high, 128), F32),
            pltpu.VMEM((high, 128), F32),
            pltpu.VMEM((group, high, 128), F32),
            pltpu.VMEM((tall, 128), F32),
            pltpu.VMEM((1, width), F32),
            DMA((9,)), DMA((nc, 4)), DMA((nc, 4)), DMA((2, nc)), DMA((2, nc)),
            DMA, DMA,
        ]
        + share_sems() * 4
        + [DMA((4,))] * 2
        + [DMA((nf,))] * 12
        + [DMA((nc,))] * 12
        + [DMA((inner,))] * 2
        + [DMA((group,))] * 2
        + [DMA((group * 4,))] * 2,
        3,
        150,
        60,
        ins=(1, 2, 3, 4, 9, 15, 16, 17, 21),
    )(
        attn_own, out_t, att, qkv, out, lse, sh_cross, sh_own, middle, cot, mod, bias,
        shrink_half, shrink_grad, expand_grad, weight_t, hidden, tok, mid_grad, stats_second,
        hidden_stats, modw, low,
    )


def update(master, first, root, gradient, clip, decay_rate):
    scaled = clip * gradient
    first_moment = first_decay * first + (1.0 - first_decay) * scaled
    second_moment = second_decay * root * root + (1.0 - second_decay) * scaled * scaled
    new_root = jnp.sqrt(second_moment)
    first_hat = first_moment * (1.0 / (1.0 - first_decay**ADAM_STEP))
    second_hat = second_moment * (1.0 / (1.0 - second_decay**ADAM_STEP))
    updated = master - learning_rate * (
        first_hat / (jnp.sqrt(second_hat) + adam_epsilon) + decay_rate * master
    )
    return updated, first_moment, new_root


def adam_body(count, nf, nc, done, condition, bias_rows, tokens_hbm, mixed_hbm, *refs):
    grads = refs[:count]
    masters = refs[count : 2 * count]
    moments = refs[2 * count : 3 * count]
    smalls = refs[3 * count : 3 * count + 8]
    outs = refs[3 * count + 8 :]
    news = outs[:count]
    averages = outs[count : 2 * count]
    small_outs = outs[2 * count : 2 * count + 8]
    condition_grad, norm, tokens_out, mixed_out = outs[2 * count + 8 : 2 * count + 12]
    scratch = outs[2 * count + 12 :]
    wbufs = scratch[:count]
    mbufs = scratch[count : 2 * count]
    gbufs = scratch[2 * count : 3 * count]
    tokens_low, mixed, wide, isem, osem, tsem = scratch[3 * count :]
    token_load = pltpu.make_async_copy(tokens_hbm, tokens_low, tsem.at[5])
    mixed_load = pltpu.make_async_copy(mixed_hbm, mixed, tsem.at[6])
    group = nf * nc
    f = lax.axis_index("fsdp")
    loads, stores = [], []
    for k in range(count):
        loads.append(
            (
                pltpu.make_async_copy(masters[k], wbufs[k], isem.at[0, k]),
                pltpu.make_async_copy(moments[k], mbufs[k], isem.at[1, k]),
                pltpu.make_async_copy(grads[k], gbufs[k], isem.at[2, k]),
            )
        )
        stores.append(
            (
                pltpu.make_async_copy(wbufs[k], news[k], osem.at[0, k]),
                pltpu.make_async_copy(mbufs[k], averages[k], osem.at[1, k]),
            )
        )
    for copy in loads[0]:
        copy.start()
    token_load.start()
    mixed_load.start()
    for group_ in loads[1:]:
        for copy in group_:
            copy.start()
    token_load.wait()
    mixed_load.wait()
    mixed_copy = pltpu.make_async_copy(mixed, mixed_out, tsem.at[4])
    mixed_copy.start()
    token_copies = []
    for k in range(4):

        def widen(i, carry, k=k):
            at = pl.ds(pl.multiple_of(i * 16, 16), 16)
            wide[k, at, :] = tokens_low[k, at, :].astype(F32)
            return carry

        lax.fori_loop(0, wide.shape[1] // 16, widen, 0)
        copy = pltpu.make_async_copy(wide.at[k], tokens_out.at[k], tsem.at[k])
        copy.start()
        token_copies.append(copy)
    folded = [done[k, 0] + done[k, 1] + done[k, 2] + done[k, 3] for k in range(group)]
    squares = folded[0][nf : nf + 1, 0:1]
    for k in range(1, group):
        squares = squares + folded[k][nf : nf + 1, 0:1]
    grad_norm = jnp.sqrt(squares)
    norm[...] = grad_norm
    clip = jnp.minimum(1.0, clip_limit / (grad_norm + 1e-06))
    deep = condition.shape[1] // group
    found = []
    for k in range(group):
        row = done[k, 0, pl.ds(f, 1), 0:deep]
        for tt in range(1, 4):
            row = row + done[k, tt, pl.ds(f, 1), 0:deep]
        found.append(row)
    v = condition[pl.ds(f, 1), :]
    gate = 1.0 / (1.0 + jnp.exp(-v))
    condition_grad[...] = jnp.concatenate(found, axis=1) * (gate * (1.0 + v * (1.0 - gate)))
    for k in range(4):
        master, moment = smalls[2 * k], smalls[2 * k + 1]
        if k < 3:
            row = (2, 1, 0)[k]
            grad = bias_rows[row : row + 1, 0 : master.shape[1]]
            new, first, root = update(master[...], moment[0:1, :], moment[1:2, :], grad, clip, 0.0)
            small_outs[2 * k][...] = new
            small_outs[2 * k + 1][0:1, :] = first
            small_outs[2 * k + 1][1:2, :] = root
        else:
            grad = bias_rows[3:5, 0 : master.shape[1]]
            new, first, root = update(master[...], moment[0], moment[1], grad, clip, 0.0)
            small_outs[2 * k][...] = new
            small_outs[2 * k + 1][0] = first
            small_outs[2 * k + 1][1] = root
    for k in range(count):
        for copy in loads[k]:
            copy.wait()
        deep_k = wbufs[k].shape[0]
        step = min(16, deep_k)

        def rows(i, carry, k=k, step=step):
            at = pl.ds(pl.multiple_of(i * step, step), step)
            new, first, root = update(
                wbufs[k][at, :], mbufs[k][0, at, :], mbufs[k][1, at, :], gbufs[k][at, :],
                clip, weight_decay,
            )
            wbufs[k][at, :] = new
            mbufs[k][0, at, :] = first
            mbufs[k][1, at, :] = root
            return carry

        lax.fori_loop(0, deep_k // step, rows, 0)
        for copy in stores[k]:
            copy.start()
    for pair in stores:
        for copy in pair:
            copy.wait()
    for copy in token_copies + [mixed_copy]:
        copy.wait()


def adam(nf, nc, done, condition, bias_rows, tokens_low, mixed, grads, masters, moments, smalls):
    count = len(grads)
    anywhere = pl.BlockSpec(memory_space=pltpu.HBM)
    small_shapes = tuple(shape(a.shape, F32) for a in smalls)
    outs = (
        tuple(shape(m.shape, F32) for m in masters)
        + tuple(shape(m.shape, F32) for m in moments)
        + small_shapes
        + (shape((1, condition.shape[1]), F32), shape((1, 1), F32))
        + (shape(tokens_low.shape, F32), shape(mixed.shape, BF16))
    )
    return pl.pallas_call(
        partial(adam_body, count, nf, nc),
        out_shape=outs,
        in_specs=vmem(3) + [anywhere] * (2 + 3 * count) + vmem(8),
        out_specs=[anywhere] * (2 * count) + vmem(10) + [anywhere] * 2,
        scratch_shapes=[pltpu.VMEM(m.shape, F32) for m in masters]
        + [pltpu.VMEM(m.shape, F32) for m in moments]
        + [pltpu.VMEM(m.shape, F32) for m in masters]
        + [
            pltpu.VMEM(tokens_low.shape, BF16), pltpu.VMEM(mixed.shape, BF16),
            pltpu.VMEM(tokens_low.shape, F32),
        ]
        + [DMA((3, count)), DMA((2, count)), DMA((7,))],
        compiler_params=pltpu.CompilerParams(vmem_limit_bytes=63 << 20),
        cost_estimate=cost(10),
        name="adam",
    )(done, condition, bias_rows, tokens_low, mixed, *grads, *masters, *moments, *smalls)


def local(
    nf,
    nc,
    tokens,
    condition,
    cotangent,
    joint_weight,
    joint_moments,
    output_weight,
    output_moments,
    expand_weight,
    expand_moments,
    shrink_weight,
    shrink_moments,
    modulate_weight,
    modulate_moments,
    attention_bias,
    attention_moments,
    hidden_bias,
    hidden_moments,
    condition_bias,
    condition_moments,
    residual_bias,
    residual_moments,
):
    latent_count, rows, width = tokens.shape
    heads = joint_weight.shape[1] // (3 * HEAD_DIM)
    assert latent_count == 1 and heads == nc and lax.axis_size("tp") == 4
    f, c, t = lax.axis_index("fsdp"), lax.axis_index("ctx"), lax.axis_index("tp")
    mine = f * nc + c
    deep, part = modulate_weight.shape
    units = expand_weight.shape[1]
    tok, cot = tokens[0], cotangent[0]

    condition_low = jax.nn.silu(condition).astype(BF16)
    condition_here = lax.dynamic_slice_in_dim(condition_low, mine * deep, deep, 1)
    condition_pad = jnp.pad(condition_here, ((0, 16 - nf), (0, 0)))
    (
        hidden_first, joint_full_t, mod, out_t, qkv, out, lse, att, expand_full,
        value, middle, hidden_two, shrink_early,
    ) = forward(
        nf, nc, part, tok, joint_weight, condition_pad, modulate_weight, condition_bias[None, :],
        attention_bias[None, :],
        output_weight, expand_weight, residual_bias, shrink_weight,
    )
    (
        attn_own, mid_grad, shrink_half, shrink_late, expand_grad, stats_second, hidden_stats,
        sh_cross, sh_own,
    ) = branch(
        nf, nc, part, hidden_two, cot, expand_full, shrink_weight, shrink_early, hidden_bias[None, :], mod, middle, value,
    )
    (
        mixed, tokens_grad, shrink_sum, expand_sum, output_sum, joint_sum, modulate_sum,
        bias_rows, done,
    ) = backward(
        nf, nc, part, attn_own, out_t, att, qkv, out, lse, sh_cross, sh_own, middle, cot,
        mod, residual_bias, shrink_half, shrink_late, expand_grad, joint_full_t, hidden_first,
        tok, mid_grad, stats_second, hidden_stats, modulate_weight, condition_pad.astype(F32),
    )
    weights = (joint_weight, output_weight, expand_weight, shrink_weight, modulate_weight)
    moments = (joint_moments, output_moments, expand_moments, shrink_moments, modulate_moments)
    grads = (joint_sum, output_sum, expand_sum, shrink_sum, modulate_sum)
    smalls = (
        attention_bias[None, :], attention_moments, hidden_bias[None, :], hidden_moments,
        condition_bias[None, :], condition_moments, residual_bias, residual_moments,
    )
    results = adam(nf, nc, done, condition, bias_rows, tokens_grad, mixed, grads, weights, moments, smalls)
    updated = []
    for k in range(5):
        updated += [results[k], results[5 + k]]
    for k in range(4):
        new = results[10 + 2 * k]
        updated += [new[0] if k < 3 else new, results[11 + 2 * k]]
    return (
        results[21].reshape(1, rows, width),
        results[20].reshape(1, rows, width),
        results[18],
        results[19][0, 0],
    ) + tuple(updated)


def solution(mesh):
    rows = P(("fsdp", "ctx"), "tp")
    pair = P(None, ("fsdp", "ctx"), "tp")
    tokens = P("fsdp", "ctx", None)
    small = (P("tp"), P(None, "tp"))
    return jax.shard_map(
        partial(local, mesh.shape["fsdp"], mesh.shape["ctx"]),
        mesh=mesh,
        in_specs=(tokens, P(), tokens) + (rows, pair) * 5 + small * 3 + (P(), P()),
        out_specs=(tokens, tokens, P("fsdp", None), P())
        + (rows, pair) * 5
        + small * 3
        + (P(), P()),
        check_vma=False,
    )
```

```python
from functools import partial

import jax
import jax.numpy as jnp
from jax import lax
from jax.experimental import pallas as pl
from jax.experimental.pallas import tpu as pltpu
from jax.sharding import PartitionSpec as P

HEAD_DIM = 64
ADAM_STEP = 10
F32 = jnp.float32
BF16 = jnp.bfloat16
MESH = pl.DeviceIdType.MESH
DMA = pltpu.SemaphoreType.DMA

norm_epsilon = 1e-06
first_decay = 0.9
second_decay = 0.999
adam_epsilon = 1e-08
learning_rate = 0.05
weight_decay = 0.1
clip_limit = 1.0
GELU_SCALE = 0.7978845608028654
GELU_CUBE = 0.044715


def dot(a, b, ca, cb):
    return lax.dot_general(a, b, (((ca,), (cb,)), ((), ())), preferred_element_type=F32)


def aligned(start, size):
    return pl.ds(pl.multiple_of(start, size), size)


def greet(peers):
    for peer in peers:
        pl.semaphore_signal(
            pltpu.get_barrier_semaphore(), inc=1, device_id=peer, device_id_type=MESH
        )
    return len(peers)


def meet(count):
    pl.semaphore_wait(pltpu.get_barrier_semaphore(), count)


def remote(source, target, send_sem, recv_sem, peer):
    return pltpu.make_async_remote_copy(
        src_ref=source,
        dst_ref=target,
        send_sem=send_sem,
        recv_sem=recv_sem,
        device_id=peer,
        device_id_type=MESH,
    )


def vmem(count):
    return [pl.BlockSpec(memory_space=pltpu.VMEM)] * count


def shape(dims, dtype):
    return jax.ShapeDtypeStruct(dims, dtype)


def cost(micros, flops=0):
    return pl.CostEstimate(flops=flops, bytes_accessed=int(micros * 3.0e6), transcendentals=0)


def call(body, name, outs, scratch, ident, micros, megabytes, ins=(), to=()):
    def run(*args):
        return pl.pallas_call(
            body,
            out_shape=outs,
            in_specs=[pl.BlockSpec(memory_space=pltpu.HBM if k in ins else pltpu.VMEM) for k in range(len(args))],
            out_specs=[pl.BlockSpec(memory_space=pltpu.HBM if k in to else pltpu.VMEM) for k in range(len(outs))],
            scratch_shapes=scratch,
            compiler_params=pltpu.CompilerParams(
                collective_id=ident, has_side_effects=True, vmem_limit_bytes=megabytes << 20
            ),
            cost_estimate=cost(micros),
            name=name,
        )(*args)

    return run


def transposed(block):
    return block.astype(F32).T.astype(BF16)


def row_of(mod, start, width, part):
    pieces = []
    for at in range(start, start + width, 128):
        pieces.append(mod[at // part, pl.ds((at % part) // 128, 1), :])
    return jnp.concatenate(pieces, axis=1)


def centred(values):
    center = values - jnp.mean(values, axis=-1, keepdims=True)
    inverse = lax.rsqrt(jnp.mean(center * center, axis=-1, keepdims=True) + norm_epsilon)
    return center * inverse, inverse


def normal_back(grad, normed, inverse):
    return inverse * (
        grad
        - jnp.mean(grad, axis=-1, keepdims=True)
        - normed * jnp.mean(grad * normed, axis=-1, keepdims=True)
    )


class Gather:
    def __init__(self, buf, nf, nc, sems, parts, first=0):
        self.buf, self.nf, self.nc, self.sems = buf, nf, nc, sems
        self.first, self.parts = first, range(first, parts)
        self.columns = buf.shape[2] // parts

    def sem(self, part, kind):
        return self.sems[4 * (part - self.first) + kind]

    def view(self, ctx, part):
        slot = lax.axis_index("fsdp") * self.nc + ctx
        return self.buf.at[slot, :, pl.ds(part * self.columns, self.columns)]

    def along(self, o, part):
        c = lax.axis_index("ctx")
        zs, zr = self.sem(part, 0), self.sem(part, 1)
        view = self.view(c, part)
        return remote(view, view, zs.at[o], zr.at[o], {"ctx": lax.rem(c + o, self.nc)})

    def onward(self, part):
        c = lax.axis_index("ctx")
        zs, zr = self.sem(part, 0), self.sem(part, 1)
        view = self.view(lax.rem(c + 2, self.nc), part)
        up = remote(view, view, zs.at[0], zr.at[3], {"ctx": lax.rem(c + 1, self.nc)})
        down = remote(view, view, zs.at[0], zr.at[1], {"ctx": lax.rem(c + 3, self.nc)})
        return up, down

    def across(self, o, part):
        f, c = lax.axis_index("fsdp"), lax.axis_index("ctx")
        xs, xr = self.sem(part, 2), self.sem(part, 3)
        view = self.view(lax.rem(c - o + self.nc, self.nc), part)
        return [
            remote(view, view, xs.at[fo, o], xr.at[fo, o], {"fsdp": lax.rem(f + fo, self.nf)})
            for fo in range(1, self.nf)
        ]

    def start(self, only=None):
        c = lax.axis_index("ctx")
        for part in self.parts if only is None else (only,):
            self.along(2, part).start()
            pl.when(c != 3)(self.along(1, part).start)
            pl.when(c != 0)(self.along(3, part).start)
            for copy in self.across(0, part):
                copy.start()

    def relay_middle(self, part):
        c = lax.axis_index("ctx")
        self.along(2, part).wait_recv()
        up, down = self.onward(part)
        pl.when(c == 2)(up.start)
        pl.when(c == 1)(down.start)
        for copy in self.across(2, part):
            copy.start()

    def relay_rest(self, part):
        for o in (1, 3):
            self.along(o, part).wait_recv()
            for copy in self.across(o, part):
                copy.start()

    def relay(self):
        for part in self.parts:
            self.relay_middle(part)
        for part in self.parts:
            self.relay_rest(part)

    def arrive(self):
        for part in self.parts:
            for o in range(self.nc):
                for copy in self.across(o, part):
                    copy.wait_recv()

    def drain(self):
        c = lax.axis_index("ctx")
        for part in self.parts:
            for o in range(self.nc):
                for copy in self.across(o, part):
                    copy.wait_send()
            up, down = self.onward(part)
            self.along(2, part).wait_send()
            pl.when(c != 3)(self.along(1, part).wait_send)
            pl.when(c != 0)(self.along(3, part).wait_send)
            pl.when(c == 2)(up.wait_send)
            pl.when(c == 1)(down.wait_send)


def gather_sems(nf, nc, parts):
    return [DMA((nc,)), DMA((nc,)), DMA((nf, nc)), DMA((nf, nc))] * parts


class Sum:
    def __init__(self, sbuf, rbuf, send, recv):
        self.sbuf, self.rbuf, self.send, self.recv = sbuf, rbuf, send, recv
        self.places = tp_places()

    def copy(self, k):
        mine, partner, cross, far = self.places
        peer = cross if k == 2 else partner
        return remote(
            self.sbuf.at[k], self.rbuf.at[k], self.send.at[k], self.recv.at[k], {"tp": peer}
        )

    def give(self, k, value):
        self.sbuf[k] = value.astype(BF16)
        self.copy(k).start()

    def pass_on(self, value):
        self.copy(0).wait_recv()
        self.give(2, value + self.rbuf[0].astype(F32))

    def near(self, value):
        self.copy(1).wait_recv()
        return value + self.rbuf[1].astype(F32)

    def total(self, value):
        self.copy(2).wait_recv()
        return value + self.rbuf[2].astype(F32)

    def drain(self):
        for k in range(3):
            self.copy(k).wait_send()


class Share:
    def __init__(self, slots, send, recv):
        self.slots, self.send, self.recv = slots, send, recv
        self.places = tp_places()

    def copy(self, k):
        mine, partner, cross, far = self.places
        slot, peer = ((mine, cross), (mine, partner), (cross, partner))[k]
        view = self.slots.at[slot]
        return remote(view, view, self.send.at[k], self.recv.at[k], {"tp": peer})

    def start(self):
        self.copy(0).start()
        self.copy(1).start()

    def relay(self):
        self.copy(0).wait_recv()
        self.copy(2).start()

    def finish(self):
        self.copy(1).wait_recv()
        self.copy(2).wait_recv()
        for k in range(3):
            self.copy(k).wait_send()


def share_sems():
    return [DMA((3,)), DMA((3,))]


class Scatter:
    def __init__(self, nf, nc, grad, parts, xland, zland, xsend, xrecv, zsend, zrecv, lanes=None):
        f, c = lax.axis_index("fsdp"), lax.axis_index("ctx")
        self.nf, self.nc, self.grad, self.parts, self.xland, self.zland = (
            nf, nc, grad, parts, xland, zland,
        )
        self.lanes = slice(None) if lanes is None else pl.ds(*lanes)
        keep = self.lanes
        self.swaps, self.deals = [], []
        for fo in range(1, nf) if grad is not None else ():
            member = lax.rem(f + fo, nf)
            self.swaps.append(
                remote(
                    grad.at[member, :, :, keep], xland.at[fo - 1, :, :, keep],
                    xsend.at[fo], xrecv.at[fo], {"fsdp": member},
                )
            )
        for o in (2, 1, 3):
            member = lax.rem(c + o, nc)
            self.deals.append(
                remote(
                    parts.at[member, :, keep], zland.at[o - 1, :, keep], zsend.at[o], zrecv.at[o],
                    {"ctx": member},
                )
            )

    def swap(self):
        for copy in self.swaps:
            copy.start()

    def swapped(self):
        f = lax.axis_index("fsdp")
        for copy in self.swaps:
            copy.wait_recv()
        for k in range(self.nc):
            total = self.grad[f, k, :, self.lanes].astype(F32)
            for fo in range(1, self.nf):
                total = total + self.xland[fo - 1, k, :, self.lanes].astype(F32)
            self.parts[k, :, self.lanes] = total.astype(BF16)

    def deal(self):
        for copy in self.deals:
            copy.start()

    def dealt(self):
        for copy in self.deals:
            copy.wait_recv()
        total = self.parts[lax.axis_index("ctx"), :, self.lanes].astype(F32)
        for o in range(1, self.nc):
            total = total + self.zland[o - 1, :, self.lanes].astype(F32)
        return total

    def drain(self, swaps=True, deals=True):
        for copy in (self.swaps if swaps else []) + (self.deals if deals else []):
            copy.wait_send()


def ring_peers(axis, size):
    here = lax.axis_index(axis)
    return [{axis: lax.rem(here + o, size)} for o in range(1, size)]


def weight_peers(nf, nc):
    f, c = lax.axis_index("fsdp"), lax.axis_index("ctx")
    peers = []
    for o in range(1, nf * nc):
        other = lax.rem(f * nc + c + o, nf * nc)
        peers.append({"fsdp": other // nc, "ctx": lax.rem(other, nc)})
    return peers


def all_peers(nf, nc):
    f, c, t = lax.axis_index("fsdp"), lax.axis_index("ctx"), lax.axis_index("tp")
    count = nf * nc * 4
    peers = []
    for o in range(1, count):
        other = lax.rem((f * nc + c) * 4 + t + o, count)
        peers.append(
            {"fsdp": other // (nc * 4), "ctx": lax.rem(other // 4, nc), "tp": lax.rem(other, 4)}
        )
    return peers


def turned(mine, turn):
    high = lax.rem(mine // 2 + turn // 2, 2)
    return high * 2 + lax.rem(mine + turn, 2)


def tp_places():
    mine = lax.axis_index("tp")
    partner = mine + 1 - 2 * lax.rem(mine, 2)
    cross = lax.rem(mine + 2, 4)
    far = lax.rem(partner + 2, 4)
    return mine, partner, cross, far


def load_all(pairs, sems):
    copies = []
    for k, (source, target) in enumerate(pairs):
        copy = pltpu.make_async_copy(source, target, sems.at[k])
        copy.start()
        copies.append(copy)
    return copies


def head_peers(nc):
    c, t = lax.axis_index("ctx"), lax.axis_index("tp")
    inner = nc * 4
    peers = []
    for o in range(1, inner):
        other = lax.rem(c * 4 + t + o, inner)
        peers.append({"ctx": other // 4, "tp": lax.rem(other, 4)})
    return peers


def forward_body(
    nf, nc, part, tok_hbm, jw_hbm, cond, modw_hbm, cbias, offset, ow_hbm, ew_hbm, bias, sw_hbm,
    hidden_hbm, weight_hbm, mod, out_t_hbm, qkv_hbm, out_hbm, lse, land_hbm, ebuf_hbm,
    value, middle, hidden_two_hbm, sbuf_hbm,
    sweight, sbuf, tok, jweight, modw, oweight, eweight, out_t, qkv, out, ebuf, hidden_two,
    hidden, weight_t, wbuf, obuf, oall, pbuf, pland, normed, joint, stage, land, keys, scores, columns,
    lsem, ssem, psend, precv, msend, mrecv, send, recv, osend, orecv, hsend, hrecv, asend, arecv,
    *gsems,
):
    f, c, t = lax.axis_index("fsdp"), lax.axis_index("ctx"), lax.axis_index("tp")
    mine, partner, cross, far = tp_places()
    group = nf * nc
    slot = f * nc + c
    rows, width = tok.shape
    own = rows // 4
    strips = part // 128
    hd = HEAD_DIM
    step = 128
    greeted = greet(weight_peers(nf, nc) + head_peers(nc))
    loads = load_all(
        (
            (jw_hbm, jweight), (modw_hbm, modw), (tok_hbm, tok), (ow_hbm, oweight),
            (ew_hbm, eweight), (sw_hbm.at[:, pl.ds(0, sweight.shape[1])], sweight),
        ),
        lsem,
    )
    joint_gather = Gather(wbuf, nf, nc, gsems[0:8], 2)
    output_gather = Gather(obuf, nf, nc, gsems[8:12], 1)
    expand_gather = Gather(ebuf, nf, nc, gsems[12:20], 2)
    shrink_gather = Gather(sbuf, nf, nc, gsems[20:24], 1)
    loads[0].wait()
    wbuf[slot] = jweight[...].astype(BF16)
    meet(greeted)
    joint_gather.start()
    loads[1].wait()
    partial_mod = dot(cond[...], modw[...].astype(BF16), 1, 0)
    for latent in range(nf):
        for k in range(strips):
            pbuf[latent, pl.ds(k, 1), :] = partial_mod[latent : latent + 1, 128 * k : 128 * k + 128]
    pcopies = []
    for o, peer in zip(range(1, group), weight_peers(nf, nc)):
        copy = remote(pbuf.at[peer["fsdp"]], pland.at[slot], psend.at[o], precv.at[o], peer)
        copy.start()
        pcopies.append(copy)
    pland[slot] = pbuf[f]
    loads[2].wait()

    def norm_rows(k, carry):
        at = aligned(k * step, step)
        normed[at, :] = centred(tok[at, :].astype(F32))[0]
        return carry

    lax.fori_loop(0, rows // 2 // step, norm_rows, 0)
    joint_gather.relay_middle(0)
    lax.fori_loop(rows // 2 // step, rows // step, norm_rows, 0)
    joint_gather.relay_middle(1)
    for copy in pcopies:
        copy.wait_recv()
    total_mod = pland[0]
    for k in range(1, group):
        total_mod = total_mod + pland[k]
    for k in range(strips):
        mod[t, pl.ds(k, 1), :] = total_mod[k : k + 1, :] + cbias[:, 128 * k : 128 * k + 128]
    mcopies = []
    for o, peer in zip(range(1, 4), ring_peers("tp", 4)):
        copy = remote(mod.at[t], mod.at[t], msend.at[o], mrecv.at[o], peer)
        copy.start()
        mcopies.append(copy)
    joint_gather.relay_rest(0)
    for copy in loads[3:]:
        copy.wait()
    obuf[slot] = oweight[...].astype(BF16)
    ebuf[slot] = eweight[...].astype(BF16)
    sbuf[slot] = sweight[...].astype(BF16)
    for copy in mcopies:
        copy.wait_recv()
    shift = row_of(mod, 0, width, part)
    scale = row_of(mod, width, width, part)

    def hide_rows(k, carry):
        at = aligned(k * step, step)
        hidden[at, :] = (normed[at, :] * (1.0 + scale) + shift).astype(BF16)
        return carry

    lax.fori_loop(0, rows // step, hide_rows, 0)
    joint_gather.relay_rest(1)
    joint_gather.arrive()
    deep = jweight.shape[0]
    for k in range(group):
        weight_t[:, k * deep : (k + 1) * deep] = transposed(wbuf[k])

    total = rows * nc
    bq, bk = scores.shape[1], 512
    per = rows // bq

    def query_copy(o):
        dst = lax.rem(c + o, nc)
        return remote(
            joint.at[aligned(dst * 3 * hd, hd), :], qkv.at[pl.ds(0, hd), aligned(c * rows, rows)],
            send.at[1, o], recv.at[1, o], {"ctx": dst},
        )

    copies = []
    biases = offset.shape[1]
    columns[...] = jnp.broadcast_to(offset[...], (128, biases)).T
    for o in (2, 1, 3, 0):
        dst = lax.rem(c + o, nc)
        where = aligned(dst * 3 * hd, 3 * hd)
        pair = columns[aligned(dst * 2 * hd, 2 * hd), 0:1]
        added = jnp.concatenate([pair[0:hd], jnp.zeros((hd, 1), F32), pair[hd : 2 * hd]], axis=0)
        head = (dot(weight_t[where, :], hidden[...], 1, 1) + added).astype(BF16)
        if o == 0:
            qkv[:, aligned(c * rows, rows)] = head
        else:
            joint[where, :] = head
            copy = remote(
                joint.at[pl.ds(pl.multiple_of(dst * 3 * hd + hd, hd), 2 * hd), :],
                qkv.at[pl.ds(hd, 2 * hd), aligned(c * rows, rows)],
                send.at[0, o], recv.at[0, o], {"ctx": dst},
            )
            copy.start()
            copies.append(copy)
    output_gather.start()
    for o in (2, 1, 3):
        query_copy(o).start()
    saves = [
        pltpu.make_async_copy(source, target, ssem.at[k])
        for k, (source, target) in enumerate(
            (
                (hidden, hidden_hbm), (weight_t, weight_hbm), (out_t, out_t_hbm), (qkv, qkv_hbm),
                (out, out_hbm), (land, land_hbm), (ebuf, ebuf_hbm), (sbuf, sbuf_hbm),
                (hidden_two, hidden_two_hbm),
            )
        )
    ]
    saves[0].start()
    saves[1].start()
    weights_share = Share(oall, asend, arecv)
    for copy in copies:
        copy.wait_recv()
    expand_gather.start(0)
    for at in range(0, total, 1024):
        keys[at : at + 1024, :] = transposed(qkv[hd : 2 * hd, at : at + 1024])

    def given(o, k):
        owner, tt = lax.rem(c - o + nc, nc), lax.rem(t + k, 4)
        return remote(
            stage.at[owner, :, aligned(tt * own, own)], land.at[t, c],
            osend.at[o, k], orecv.at[o, k], {"ctx": owner, "tp": tt},
        )

    def block(i, carry):
        turn, sub = i // per, lax.rem(i, per)
        o = jnp.where(turn > 0, 1 + lax.rem(turn, 3), 0)
        owner = lax.rem(c - o + nc, nc)

        @pl.when(jnp.logical_and(sub == 0, turn > 0))
        def _():
            query_copy(o).wait_recv()

        @pl.when(i == per)
        def _():
            output_gather.relay()

        @pl.when(i == per + 1)
        def _():
            output_gather.arrive()
            oall[mine] = obuf[...].reshape(width, nc * hd)
            weights_share.start()

        @pl.when(i == per * nc - 1)
        def _():
            weights_share.relay()

        @pl.when(i == 3 * per)
        def _():
            expand_gather.relay_middle(0)
            saves[3].start()

        where = aligned(owner * rows + sub * bq, bq)
        query = qkv[0:hd, where] * BF16(hd**-0.5)
        peak = None
        for at in range(0, total, bk):
            s = dot(keys[at : at + bk, :], query, 1, 0)
            scores[at : at + bk, :] = s
            high = jnp.max(s.reshape(bk // 8, 8, bq), axis=0)
            peak = high if peak is None else jnp.maximum(peak, high)
        peak = jnp.max(peak, axis=0, keepdims=True)
        acc, mass = None, None
        for at in range(0, total, bk):
            p = jnp.exp(scores[at : at + bk, :] - peak)
            low = jnp.sum(p.reshape(bk // 8, 8, bq), axis=0)
            mass = low if mass is None else mass + low
            term = dot(qkv[2 * hd : 3 * hd, at : at + bk], p.astype(BF16), 1, 0)
            acc = term if acc is None else acc + term
        mass = jnp.sum(mass, axis=0, keepdims=True)
        acc = acc * (1.0 / mass)
        out[:, where] = acc
        lse[:, where] = peak + jnp.log(mass)
        stage[owner, :, aligned(sub * bq, bq)] = acc.astype(BF16)

        @pl.when(sub == per - 1)
        def _():
            pl.when(turn > 0)(given(o, 0).start)
            for k in range(1, 4):
                given(o, k).start()

        return carry

    lax.fori_loop(0, per * nc, block, 0)
    expand_gather.start(1)
    shrink_gather.start()
    land[t, c] = stage[c, :, aligned(t * own, own)]
    expand_gather.relay_rest(0)
    weights_share.finish()
    for k in range(4):
        out_t[k] = transposed(oall[k])
    saves[2].start()
    saves[4].start()

    order = [(o, k) for o in (0, 2, 3, 1) for k in range(4) if o or k]
    for o, k in order:
        given(o, k).wait_recv()
    held = bias[0:1, :]
    for k in range(4):
        block_ = land[k].reshape(nc * hd, own)
        held = held + dot(block_.astype(F32).T.astype(BF16), out_t[k], 1, 0)
    value[...] = held
    gate = row_of(mod, 2 * width, width, part)
    shift = row_of(mod, 3 * width, width, part)
    scale = row_of(mod, 4 * width, width, part)
    mid = tok[aligned(mine * own, own), :].astype(F32) + gate * held
    middle[...] = mid
    hidden_two[mine] = (centred(mid)[0] * (1.0 + scale) + shift).astype(BF16)
    sharing = Share(hidden_two, hsend, hrecv)
    sharing.start()
    saves[5].start()
    expand_gather.relay_middle(1)
    shrink_gather.relay_middle(0)
    expand_gather.relay_rest(1)
    shrink_gather.relay_rest(0)
    sharing.relay()
    for o, k in order:
        given(o, k).wait_send()
    for o in (2, 1, 3):
        query_copy(o).wait_send()
    for copy in pcopies + mcopies + copies:
        copy.wait_send()
    expand_gather.arrive()
    saves[6].start()
    sharing.finish()
    saves[8].start()
    shrink_gather.arrive()
    saves[7].start()
    for copy in saves:
        copy.wait()
    for gather in (joint_gather, output_gather, expand_gather, shrink_gather):
        gather.drain()


def forward(nf, nc, part, tok, jweight, cond, modw, cbias, offset, oweight, eweight, bias, sweight):
    rows, width = tok.shape
    deep, columns = jweight.shape
    group = nf * nc
    own = rows // 4
    total = rows * nc
    hd = HEAD_DIM
    bq = min(512, rows)
    high = -(-part // 1024) * 8
    return call(
        partial(forward_body, nf, nc, part),
        "forward",
        (
            shape((rows, width), BF16),
            shape((columns, width), BF16),
            shape((4, high, 128), F32),
            shape((4, nc * hd, width), BF16),
            shape((3 * hd, total), BF16),
            shape((hd, total), F32),
            shape((1, total), F32),
            shape((4, nc, hd, own), BF16),
            shape((group,) + eweight.shape, BF16),
            shape((own, width), F32),
            shape((own, width), F32),
            shape((4, own, width), BF16),
            shape((group, deep, sweight.shape[1] // 2), BF16),
        ),
        [
            pltpu.VMEM((deep, sweight.shape[1] // 2), F32),
            pltpu.VMEM((group, deep, sweight.shape[1] // 2), BF16),
            pltpu.VMEM(tok.shape, BF16),
            pltpu.VMEM(jweight.shape, F32),
            pltpu.VMEM(modw.shape, F32),
            pltpu.VMEM(oweight.shape, F32),
            pltpu.VMEM(eweight.shape, F32),
            pltpu.VMEM((4, nc * hd, width), BF16),
            pltpu.VMEM((3 * hd, total), BF16),
            pltpu.VMEM((hd, total), F32),
            pltpu.VMEM((group,) + eweight.shape, BF16),
            pltpu.VMEM((4, own, width), BF16),
            pltpu.VMEM((rows, width), BF16),
            pltpu.VMEM((columns, width), BF16),
            pltpu.VMEM((group, deep, columns), BF16),
            pltpu.VMEM((group,) + oweight.shape, BF16),
            pltpu.VMEM((4, width, nc * hd), BF16),
            pltpu.VMEM((nf, high, 128), F32),
            pltpu.VMEM((group, high, 128), F32),
            pltpu.VMEM((rows, width), F32),
            pltpu.VMEM((columns, rows), BF16),
            pltpu.VMEM((nc, hd, rows), BF16),
            pltpu.VMEM((4, nc, hd, own), BF16),
            pltpu.VMEM((total, hd), BF16),
            pltpu.VMEM((total, bq), F32),
            pltpu.VMEM((offset.shape[1], 128), F32),
            DMA((6,)), DMA((9,)),
            DMA((group,)), DMA((group,)), DMA((4,)), DMA((4,)),
            DMA((2, nc)), DMA((2, nc)), DMA((nc, 4)), DMA((nc, 4)), DMA((3,)), DMA((3,)),
        ]
        + share_sems()
        + gather_sems(nf, nc, 6),
        1,
        150,
        60,
        ins=(0, 1, 3, 6, 7, 9),
        to=(0, 1, 3, 4, 5, 7, 8, 11, 12),
    )(tok, jweight, cond, modw, cbias, offset, oweight, eweight, bias, sweight)


def branch_body(
    nf, nc, part, hidden_hbm, cot_hbm, expand_hbm, sw_hbm, sbuf_hbm, hbias, mod, middle, value,
    attn_own, mid_grad, shrink_half, shrink_late, expand_grad, stats, hstats, sh_cross, sh_own,
    cot, hidden, expand, sweight, sgat, gbuf, abuf, ebuf, slopes, held_buf,
    shrink_grad, shrink_parts, sland, dland, sbuf, rbuf, shold,
    lsem, tsend, trecv, send, recv, s1s, s1r, d1s, d1r, *gsems,
):
    mine, partner, cross, far = tp_places()
    own, width = middle.shape
    group = nf * nc
    deep, units = sweight.shape
    slot = lax.axis_index("fsdp") * nc + lax.axis_index("ctx")
    greeted = greet(ring_peers("tp", 4) + weight_peers(nf, nc))
    gate_first = row_of(mod, 2 * width, width, part)
    scale_second = row_of(mod, 4 * width, width, part)
    gate_second = row_of(mod, 5 * width, width, part)
    split = units // 2
    loads = load_all(
        (
            (sw_hbm, sweight), (hidden_hbm, hidden), (expand_hbm, expand), (cot_hbm, cot),
            (sbuf_hbm, sgat.at[:, :, pl.ds(0, split)]),
        ),
        lsem,
    )
    loads[0].wait()
    sgat[slot, :, split:units] = sweight[:, split:units].astype(BF16)
    meet(greeted)
    gather = Gather(sgat, nf, nc, gsems, 2, 1)
    gather.start()
    for copy in loads[1:]:
        copy.wait()
    tile = 32

    def ahead(turn, carry):
        at = turned(mine, turn)

        @pl.when(turn == 2)
        def _():
            gather.relay_middle(1)


        where = aligned(at * own, own)
        weight = expand[...].reshape(width, units)
        slopes[where, :] = dot(hidden[at], weight, 1, 0) + hbias[...]

        def curve(k, carry_):
            row = pl.ds(pl.multiple_of(at * own + k * tile, tile), tile)
            u = slopes[row, :]
            squared = u * u
            th = jnp.tanh(GELU_SCALE * (u + GELU_CUBE * squared * u))
            abuf[row, :] = (0.5 * u * (1.0 + th)).astype(BF16)
            slopes[row, :] = 0.5 * (1.0 + th) + 0.5 * u * (1.0 - th * th) * (
                GELU_SCALE * (1.0 + 3.0 * GELU_CUBE * squared)
            )
            gbuf[row, :] = (gate_second * cot[row, :].astype(F32)).astype(BF16)
            return carry_

        lax.fori_loop(0, own // tile, curve, 0)
        return carry

    lax.fori_loop(0, 4, ahead, 0)
    gather.relay_rest(1)
    step = 256
    for at in range(0, width, step):
        block = dot(gbuf[:, at : at + step], abuf[...], 0, 0).astype(BF16)
        for k in range(at // deep, (at + step) // deep):
            rows_k = slice(k * deep - at, (k + 1) * deep - at)
            shrink_grad[k // nc, k % nc] = block[rows_k, 0:split]
            shrink_late[k // nc, k % nc] = block[rows_k, split:units]
    early = Scatter(nf, nc, shrink_grad, shrink_parts, sland, dland, s1s, s1r, d1s, d1r)
    early.swap()
    gather.arrive()
    hstats[...] = jnp.zeros_like(hstats)
    summing = Sum(sbuf, rbuf, send, recv)

    def back_turn(turn, carry):
        at = turned(mine, 3 - turn)
        where = aligned(at * own, own)
        weight = sgat[...].reshape(width, units)
        pull = dot(gbuf[where, :], weight, 1, 0) * slopes[where, :]
        hstats[...] += jnp.sum(pull, axis=0, keepdims=True)
        pull = pull.astype(BF16)
        ebuf[where, :] = pull
        held_buf[...] = dot(pull, expand[...].reshape(width, units), 1, 1)

        @pl.when(turn == 0)
        def _():
            summing.give(0, held_buf[...])

        @pl.when(turn == 1)
        def _():
            summing.pass_on(held_buf[...])

        @pl.when(turn == 2)
        def _():
            summing.give(1, held_buf[...])

        return carry

    lax.fori_loop(0, 4, back_turn, 0)
    copies = []
    for turn, at in enumerate((far, partner)):
        weight = sgat[...].reshape(width, units)
        shold[turn] = dot(abuf[aligned(at * own, own), :], weight, 1, 1).astype(BF16)
        copy = remote(
            shold.at[turn], shold.at[2 + turn], tsend.at[turn], trecv.at[turn], {"tp": partner}
        )
        copy.start()
        copies.append(copy)
    flat = hidden.shape[0] * own
    for at in range(0, width, step):
        expand_grad[at : at + step, :] = dot(
            hidden[:, :, at : at + step].reshape(flat, step), ebuf[...], 0, 0
        ).astype(BF16)
    early.swapped()
    early.deal()
    weight = sgat[...].reshape(width, units)
    forth = dot(abuf[aligned(cross * own, own), :], weight, 1, 1)
    copies[0].wait_recv()
    sh_cross[...] = (forth + shold[2].astype(F32)).astype(BF16)
    forth = dot(abuf[aligned(mine * own, own), :], weight, 1, 1)
    copies[1].wait_recv()
    sh_own[...] = forth + shold[3].astype(F32)
    mine_rows = cot[aligned(mine * own, own), :].astype(F32)
    stats[3:4, :] = jnp.sum(gate_second * mine_rows, axis=0, keepdims=True)
    normed, inverse = centred(middle[...])
    grad_in = summing.total(summing.near(held_buf[...]))
    stats[0:1, :] = jnp.sum(grad_in, axis=0, keepdims=True)
    stats[1:2, :] = jnp.sum(grad_in * normed, axis=0, keepdims=True)
    mgrad = mine_rows + normal_back(grad_in * (1.0 + scale_second), normed, inverse)
    mid_grad[...] = mgrad
    agrad = gate_first * mgrad
    attn_own[...] = agrad.astype(BF16)
    stats[2:3, :] = jnp.sum(mgrad * value[...], axis=0, keepdims=True)
    stats[4:5, :] = jnp.sum(agrad, axis=0, keepdims=True)
    stats[5:8, :] = jnp.zeros((3, width), F32)
    shrink_half[...] = early.dealt()
    early.drain()
    summing.drain()
    gather.drain()
    for copy in copies:
        copy.wait_send()


def branch(nf, nc, part, hidden, cot, expand, sweight, sbuf, hbias, mod, middle, value):
    rows, width = cot.shape
    own = rows // 4
    deep, units = sweight.shape
    group = nf * nc
    return call(
        partial(branch_body, nf, nc, part),
        "branch",
        (
            shape((own, width), BF16),
            shape((own, width), F32),
            shape((deep, units // 2), F32),
            shape((nf, nc, deep, units // 2), BF16),
            shape((width, units), BF16),
            shape((8, width), F32),
            shape((1, units), F32),
            shape((own, width), BF16),
            shape((own, width), F32),
        ),
        [
            pltpu.VMEM((rows, width), BF16),
            pltpu.VMEM((4, own, width), BF16),
            pltpu.VMEM((group, deep, units), BF16),
            pltpu.VMEM((deep, units), F32),
            pltpu.VMEM((group, deep, units), BF16),
            pltpu.VMEM((rows, width), BF16),
            pltpu.VMEM((rows, units), BF16),
            pltpu.VMEM((rows, units), BF16),
            pltpu.VMEM((rows, units), F32),
            pltpu.VMEM((own, width), F32),
            pltpu.VMEM((nf, nc, deep, units // 2), BF16),
            pltpu.VMEM((nc, deep, units // 2), BF16),
            pltpu.VMEM((nf - 1, nc, deep, units // 2), BF16),
            pltpu.VMEM((nc - 1, deep, units // 2), BF16),
            pltpu.VMEM((3, own, width), BF16),
            pltpu.VMEM((3, own, width), BF16),
            pltpu.VMEM((4, own, width), BF16),
            DMA((5,)), DMA((2,)), DMA((2,)),
        ]
        + share_sems()
        + [DMA((nf,))] * 2
        + [DMA((nc,))] * 2
        + gather_sems(nf, nc, 1),
        2,
        40,
        60,
        ins=(0, 1, 2, 3, 4),
    )(hidden, cot, expand, sweight, sbuf, hbias, mod, middle, value)


def backward_body(
    nf, nc, part, attn_own, out_t_hbm, heads_hbm, qkv_hbm, out_hbm, lse, sh_cross, sh_own, middle,
    cot_hbm, mod, bias, shrink_half, shrink_grad, expand_grad, weight_hbm, hidden_hbm, tok_hbm,
    mid_grad, stats_second, hidden_stats, modw_hbm, low,
    mixed, tokens_grad, shrink_sum, expand_sum, output_sum, joint_sum, modulate_sum,
    bias_rows, done,
    out_t, qkv, out, heads, att, cot_own, tok_own, weight_t, hidden, modw,
    attn_low, dout, dost, keys, vals, dq, dkv, stage, rland, delta, output_grad,
    sland, shrink_parts, eland, oland, expand_parts, output_parts, sdeal, edeal, odeal, joint_grad, sbuf, rbuf,
    kvgrad, kvland, kvparts, kvdeal, qgrad, qland, qparts, qdeal, pieces, land, total_piece, gathered, ftotal, gate_row,
    lsem, send, recv, jsend, jrecv, csend, crecv, gsend, grecv, tsend, trecv, hsend, hrecv,
    lowsend, lowrecv, hsend2, hrecv2, x1s, x1r, x2s, x2r, x3s, x3r, x4s, x4r, x5s, x5r, x6s, x6r,
    d1s, d1r, d2s, d2r, d3s, d3r, d4s, d4r, d5s, d5r, d6s, d6r, asend, arecv, bsend, brecv, f1s, f1r,
):
    f, c, t = lax.axis_index("fsdp"), lax.axis_index("ctx"), lax.axis_index("tp")
    mine, partner, cross, far = tp_places()
    own, width = middle.shape
    rows = 4 * own
    total = rows * nc
    hd = HEAD_DIM
    inner, group = nc * 4, nf * nc
    here, slot = c * 4 + t, f * nc + c
    bk = bq = 512
    per = rows // bk
    deep = joint_sum.shape[0]
    heads_wide = nc * hd
    units = expand_grad.shape[3]
    half = units // 2
    shrink = Scatter(nf, nc, shrink_grad, shrink_parts, sland, sdeal, x6s, x6r, d1s, d1r)
    early = Scatter(
        nf, nc, expand_grad, expand_parts, eland, edeal, x1s, x1r, d2s, d2r, (0, half)
    )
    late = Scatter(
        nf, nc, expand_grad, expand_parts, eland, edeal, x2s, x2r, d3s, d3r, (half, half)
    )
    project = Scatter(nf, nc, output_grad, output_parts, oland, odeal, x3s, x3r, d4s, d4r)
    kv = Scatter(nf, nc, kvgrad, kvparts, kvland, kvdeal, x4s, x4r, d5s, d5r)
    query = Scatter(nf, nc, qgrad, qparts, qland, qdeal, x5s, x5r, d6s, d6r)
    greeted = greet(all_peers(nf, nc))
    own_rows = aligned(mine * own, own)
    loads = load_all(
        (
            (out_t_hbm, out_t), (qkv_hbm, qkv), (out_hbm, out), (heads_hbm, heads),
            (cot_hbm.at[own_rows, :], cot_own), (tok_hbm.at[own_rows, :], tok_own),
            (weight_hbm, weight_t), (hidden_hbm, hidden), (modw_hbm, modw),
        ),
        lsem,
    )
    attn_low[mine] = attn_own[...]
    loads[0].wait()
    for k in range(4):
        dost[k] = dot(out_t[k], attn_own[...], 1, 1).astype(BF16).reshape(nc, hd, own)
    meet(greeted)
    where_own = aligned(c * rows + t * own, own)

    def send_out(o, k):
        cc, tt = lax.rem(c + o, nc), lax.rem(t + k, 4)
        return remote(
            dost.at[tt, cc], dout.at[:, where_own], send.at[o, k], recv.at[o, k],
            {"ctx": cc, "tp": tt},
        )

    order = [(o, k) for o in (0, 2, 1, 3) for k in range(4) if o or k]
    shrink.swap()
    for o, k in order:
        send_out(o, k).start()
    low_share = Share(attn_low, lowsend, lowrecv)
    low_share.start()
    crossing = remote(sh_cross, rland, csend, crecv, {"tp": cross})
    early.swap()
    dout[:, where_own] = dost[t, c]
    for copy in loads[1:4]:
        copy.wait()
    for at in range(0, total, 1024):
        keys[at : at + 1024, :] = transposed(qkv[hd : 2 * hd, at : at + 1024])
        vals[at : at + 1024, :] = transposed(qkv[2 * hd : 3 * hd, at : at + 1024])
    dq[...] = jnp.zeros_like(dq)
    dkv[...] = jnp.zeros_like(dkv)
    sharing = Share(mixed, gsend, grecv)
    exchange = [
        remote(heads.at[peer["tp"]], att.at[:, :, own_rows], hsend2.at[k], hrecv2.at[k], peer)
        for k, peer in zip(range(1, 4), ring_peers("tp", 4))
    ]

    def kv_back(o, owner):
        return remote(
            stage.at[owner, pl.ds(hd, 2 * hd), :], joint_grad.at[c, pl.ds(hd, 2 * hd), :],
            jsend.at[0, o], jrecv.at[0, o], {"ctx": owner},
        )

    def q_back(o, owner):
        return remote(
            stage.at[owner, pl.ds(0, hd), :], joint_grad.at[c, pl.ds(0, hd), :],
            jsend.at[1, o], jrecv.at[1, o], {"ctx": owner},
        )

    count = per * nc

    def block(i, vsum):
        turn, step = i // count, lax.rem(i, count)
        owners = (lax.rem(c + turn * (nc - 1), nc), lax.rem(c + 2 + turn * (nc - 1), nc))

        @pl.when(i == 0)
        def _():
            for o, k in order:
                if o in (0, 2):
                    send_out(o, k).wait_recv()

        @pl.when(i == count)
        def _():
            for o, k in order:
                if o in (1, 3):
                    send_out(o, k).wait_recv()

        @pl.when(step == 0)
        def _():
            for owner in owners:
                where_q = aligned(owner * rows, rows)
                delta[:, where_q] = jnp.sum(
                    dout[:, where_q].astype(F32) * out[:, where_q], axis=0, keepdims=True
                )

        o = 1 + step // per
        owner = lax.rem(c + o, nc)
        sub = lax.rem(step, per)
        where = aligned(owner * rows + sub * bk, bk)
        key, val, key_t = keys[where, :], vals[where, :], qkv[hd : 2 * hd, where]
        dk, dv = dkv[0:hd, where], dkv[hd : 2 * hd, where]
        for source in owners:
            for half_ in range(rows // bq):
                at = aligned(source * rows + half_ * bq, bq)
                query = qkv[0:hd, at] * BF16(hd**-0.5)
                grad = dout[:, at]
                p = jnp.exp(dot(key, query, 1, 0) - lse[:, at])
                ds = (p * (dot(val, grad, 1, 0) - delta[:, at])).astype(BF16)
                dv = dv + dot(grad, p.astype(BF16), 1, 1)
                dk = dk + dot(query, ds, 1, 1)
                dq[:, at] += dot(key_t, ds, 1, 0)
        dkv[0:hd, where] = dk
        dkv[hd : 2 * hd, where] = dv
        put = aligned(sub * bk, bk)

        @pl.when(turn == 1)
        def _():
            stage[owner, hd : 2 * hd, put] = dkv[0:hd, where].astype(BF16)
            stage[owner, 2 * hd : 3 * hd, put] = dkv[hd : 2 * hd, where].astype(BF16)

        @pl.when(jnp.logical_and(turn == 1, jnp.logical_and(sub == per - 1, o < nc)))
        def _():
            kv_back(o, owner).start()

        @pl.when(i == 1)
        def _():
            shrink.swapped()
            shrink.deal()

        @pl.when(i == 0)
        def _():
            att[:, :, own_rows] = heads[t]
            for copy in exchange:
                copy.start()

        @pl.when(i == 2)
        def _():
            low_share.relay()
            crossing.start()

        @pl.when(i == 8)
        def _():
            crossing.wait_recv()
            loads[4].wait()
            value = sh_own[...] + rland[...].astype(F32) + bias[1:2, :]
            gate = row_of(mod, 5 * width, width, part)
            mixed[mine] = (middle[...] + gate * value).astype(BF16)
            sharing.start()
            gate_row[...] = jnp.sum(
                cot_own[...].astype(F32) * value, axis=0, keepdims=True
            )

        @pl.when(i == 3)
        def _():
            early.swapped()
            early.deal()
            late.swap()

        @pl.when(i == 6)
        def _():
            for k in (1, 2):
                low_share.copy(k).wait_recv()
            for copy in exchange:
                copy.wait_recv()
            flat = dot(
                att[...].reshape(heads_wide, rows), attn_low[...].reshape(rows, width), 1, 0
            ).T.astype(BF16)
            output_grad[...] = flat.reshape(output_grad.shape)
            project.swap()

        @pl.when(i == count - 1)
        def _():
            for source in owners:
                stage[source, 0:hd, :] = (
                    dq[:, aligned(source * rows, rows)] * (hd**-0.5)
                ).astype(BF16)
            q_back(2, owners[1]).start()

        @pl.when(i == 9)
        def _():
            late.swapped()

        @pl.when(i == 11)
        def _():
            project.swapped()

        @pl.when(i == 14)
        def _():
            sharing.relay()

        return vsum

    lax.fori_loop(0, 2 * count, block, 0)
    for o in (1, 3):
        owner = lax.rem(c + o, nc)
        stage[owner, 0:hd, :] = (dq[:, aligned(owner * rows, rows)] * (hd**-0.5)).astype(BF16)
        q_back(o, owner).start()
    qsum = jnp.sum(dq[...] * (hd**-0.5), axis=1, keepdims=True)
    vsum = jnp.sum(dkv[hd : 2 * hd, :], axis=1, keepdims=True)
    late.deal()
    joint_grad[c] = stage[c]
    bias_column = jnp.concatenate([qsum, vsum], axis=0)
    for copy in loads[5:]:
        copy.wait()
    rows_f = width // nf

    def weight_grad(scatter, source, into):
        flat_grad = source.reshape(-1, rows)

        def put(lanes, member, first, count):
            block_ = dot(flat_grad, hidden[:, lanes], 1, 0).T.astype(BF16)
            for k in range(count):
                row = (member, first + k) if member is not None else divmod(first + k, nc)
                into[row[0], row[1]] = block_[k * deep : (k + 1) * deep, :]

        if rows_f % 128:
            for at in range(0, width, 256):
                put(pl.ds(at, 256), None, at // deep, 256 // deep)
            scatter.swap()
            return
        wide_step = min(256, rows_f)
        for o in range(1, nf + 1):
            member = lax.rem(f + o, nf)
            for at in range(0, rows_f, wide_step):
                put(
                    aligned(member * rows_f + at, wide_step), member, at // deep, wide_step // deep
                )
            if o < nf:
                scatter.swaps[o - 1].start()

    for o in range(1, nc):
        kv_back(o, lax.rem(c + o, nc)).wait_recv()
    weight_grad(kv, joint_grad[:, hd : 3 * hd, :], kvgrad)
    shrink_total = shrink.dealt()
    shrink_sum[:, 0:half] = shrink_half[...]
    shrink_sum[:, half:units] = shrink_total
    squares = jnp.sum(shrink_total * shrink_total) + jnp.sum(shrink_half[...] * shrink_half[...])
    for o in range(1, nc):
        q_back(o, lax.rem(c + o, nc)).wait_recv()

    columns = weight_t.shape[0]

    def piece_of(at):
        block_ = joint_grad[:, :, aligned(at * own, own)].reshape(columns, own)
        return dot(block_.astype(F32).T.astype(BF16), weight_t[...], 1, 0)

    summing = Sum(sbuf, rbuf, tsend, trecv)
    summing.give(0, piece_of(far))
    summing.give(1, piece_of(partner))
    summing.pass_on(piece_of(cross))
    weight_grad(query, joint_grad[:, 0:hd, :], qgrad)
    held = summing.near(piece_of(mine))
    kv.swapped()
    kv.deal()
    normed, inverse = centred(tok_own[...].astype(F32))
    grad_in = summing.total(held)
    scale = row_of(mod, width, width, part)
    shift_row = jnp.sum(grad_in, axis=0, keepdims=True)
    scale_row = jnp.sum(grad_in * normed, axis=0, keepdims=True)

    slim = part // nc // 128
    share = 2 * width // nc // 128
    hshare = hidden_stats.shape[1] // nc // 128
    last = slim + share + hshare
    vectors = [
        shift_row, scale_row, stats_second[2:3, :],
        stats_second[0:1, :], stats_second[1:2, :], gate_row[...],
    ]
    residual = [stats_second[4:5, :], stats_second[3:4, :]]
    pieces[...] = jnp.zeros_like(pieces)
    for cc in range(nc):
        for tt in range(4):
            k = cc * 4 + tt
            for n in range(slim):
                at = ((tt * part // 128) + cc * slim + n) * 128
                pieces[k, n : n + 1, :] = vectors[at // width][:, at % width : at % width + 128]
            for n in range(share):
                at = (cc * share + n) * 128
                pieces[k, slim + n : slim + n + 1, :] = residual[at // width][
                    :, at % width : at % width + 128
                ]
        for n in range(hshare):
            at = (cc * hshare + n) * 128
            pieces[cc * 4 + t, slim + share + n : slim + share + n + 1, :] = hidden_stats[
                :, at : at + 128
            ]
    pieces[here, last : last + 1, :] = jnp.broadcast_to(bias_column, (2 * hd, 128)).T[0:1, :]
    first = []
    for o in range(1, inner):
        other = lax.rem(here + o, inner)
        copy = remote(
            pieces.at[other], land.at[here], asend.at[o], arecv.at[o],
            {"ctx": other // 4, "tp": lax.rem(other, 4)},
        )
        copy.start()
        first.append(copy)
    tokens_grad[mine] = (
        mid_grad[...] + normal_back(grad_in * (1.0 + scale), normed, inverse)
    ).astype(BF16)
    token_share = Share(tokens_grad, hsend, hrecv)
    token_share.start()
    query.swapped()
    query.deal()
    land[here] = pieces[here]
    for copy in first:
        copy.wait_recv()
    acc = land[0]
    for k in range(1, inner):
        acc = acc + land[k]
    total_piece[...] = acc
    gathered[slot] = acc
    second = []
    for o, peer in zip(range(1, group), weight_peers(nf, nc)):
        copy = remote(total_piece, gathered.at[slot], bsend.at[o], brecv.at[o], peer)
        copy.start()
        second.append(copy)
    project.deal()
    expand_total = early.dealt()
    expand_sum[:, 0:half] = expand_total
    squares = squares + jnp.sum(expand_total * expand_total)
    expand_total = late.dealt()
    expand_sum[:, half:units] = expand_total
    squares = squares + jnp.sum(expand_total * expand_total)
    output_total = project.dealt()
    output_sum[...] = output_total
    squares = squares + jnp.sum(output_total * output_total)
    for copy in second:
        copy.wait_recv()

    grads = []
    for latent in range(nf):
        strips = []
        for cc in range(nc):
            for n in range(slim):
                strips.append(gathered[latent * nc + cc, n : n + 1, :])
        grads.append(jnp.concatenate(strips, axis=1))
    condition_bias = grads[0]
    for latent in range(1, nf):
        condition_bias = condition_bias + grads[latent]
    bias_rows[...] = jnp.zeros_like(bias_rows)
    bias_rows[0:1, 0:part] = condition_bias
    factors = low[...].T
    wide = modw[...].astype(BF16).astype(F32)
    outer = None
    ftotal[...] = jnp.zeros_like(ftotal)
    for latent in range(nf):
        term = factors[:, latent : latent + 1] * grads[latent]
        outer = term if outer is None else outer + term
        column = jnp.sum(wide * grads[latent], axis=1, keepdims=True)
        ftotal[latent : latent + 1, 0:deep] = jnp.broadcast_to(column, (deep, 128)).T[0:1, :]
    modulate_sum[...] = outer
    squares = squares + jnp.sum(outer * outer)

    def over(at, count):
        found = []
        for cc in range(nc):
            value = None
            for latent in range(nf):
                block_ = gathered[latent * nc + cc, at : at + count, :]
                value = block_ if value is None else value + block_
            for n in range(count):
                found.append(value[n : n + 1, :])
        return jnp.concatenate(found, axis=1)

    residual_sum = over(slim, share)
    hidden_sum = over(slim + share, hshare)
    head_sum = over(last, 1)
    bias_rows[1:2, 0 : hidden_sum.shape[1]] = hidden_sum
    bias_rows[2:3, 0 : head_sum.shape[1]] = head_sum
    bias_rows[3:4, 0:width] = residual_sum[:, 0:width]
    bias_rows[4:5, 0:width] = residual_sum[:, width : 2 * width]
    lead = (slot == 0).astype(F32)
    tensor_lead = (t == 0).astype(F32)
    squares = squares + lead * (
        jnp.sum(condition_bias * condition_bias)
        + jnp.sum(hidden_sum * hidden_sum)
        + jnp.sum(head_sum * head_sum)
        + tensor_lead * jnp.sum(residual_sum * residual_sum)
    )
    token_share.relay()
    kv_total, q_total = kv.dealt(), query.dealt()
    squares = squares + jnp.sum(kv_total * kv_total) + jnp.sum(q_total * q_total)
    ftotal[nf : nf + 1, :] = jnp.full((1, 128), squares)
    third = []
    for o, peer in zip(range(1, group * 4), all_peers(nf, nc)):
        copy = remote(ftotal, done.at[slot, t], f1s.at[o], f1r.at[o], peer)
        copy.start()
        third.append(copy)
    done[slot, t] = ftotal[...]
    kv_total, q_total = kv_total.T, q_total.T
    blocks = []
    for k in range(nc):
        blocks += [q_total[k * hd : (k + 1) * hd], kv_total[k * 2 * hd : (k + 1) * 2 * hd]]
    joint_sum[...] = jnp.concatenate(blocks, axis=0).T
    sharing.finish()
    token_share.finish()
    summing.drain()
    for o in range(1, nc):
        owner = lax.rem(c + o, nc)
        kv_back(o, owner).wait_send()
        q_back(o, owner).wait_send()
    for o, k in order:
        send_out(o, k).wait_send()
    for k in range(3):
        low_share.copy(k).wait_send()
    for copy in exchange:
        copy.wait_send()
    crossing.wait_send()
    for scatter in (shrink, early, late, project, kv, query):
        scatter.drain()
    for copy in third:
        copy.wait_recv()
    for copy in first + second + third:
        copy.wait_send()


def backward(
    nf, nc, part, attn_own, out_t, att, qkv, out, lse, sh_cross, sh_own, middle, cot, mod, bias,
    shrink_half, shrink_grad, expand_grad, weight_t, hidden, tok, mid_grad, stats_second, hidden_stats,
    modw, low,
):
    rows, width = cot.shape
    own = rows // 4
    total = rows * nc
    hd = HEAD_DIM
    inner, group = nc * 4, nf * nc
    deep = width // group
    units = expand_grad.shape[1]
    columns = weight_t.shape[0]
    heads_wide = nc * hd
    expand_grad = expand_grad.reshape(nf, nc, deep, units)
    high = -(-(part // nc + 2 * width // nc + hidden_stats.shape[1] // nc + 128) // 1024) * 8
    tall = -(-(nf + 1) // 8) * 8
    return call(
        partial(backward_body, nf, nc, part),
        "backward",
        (
            shape((4, own, width), BF16),
            shape((4, own, width), BF16),
            shape((deep, units), F32),
            shape((deep, units), F32),
            shape((deep, heads_wide), F32),
            shape((deep, columns), F32),
            shape((deep, part), F32),
            shape((8, max(part, width, hidden_stats.shape[1])), F32),
            shape((group, 4, tall, 128), F32),
        ),
        [
            pltpu.VMEM(out_t.shape, BF16),
            pltpu.VMEM(qkv.shape, BF16),
            pltpu.VMEM(out.shape, F32),
            pltpu.VMEM(att.shape, BF16),
            pltpu.VMEM((nc, hd, rows), BF16),
            pltpu.VMEM((own, width), BF16),
            pltpu.VMEM((own, width), BF16),
            pltpu.VMEM(weight_t.shape, BF16),
            pltpu.VMEM(hidden.shape, BF16),
            pltpu.VMEM(modw.shape, F32),
            pltpu.VMEM((4, own, width), BF16),
            pltpu.VMEM((hd, total), BF16),
            pltpu.VMEM((4, nc, hd, own), BF16),
            pltpu.VMEM((total, hd), BF16),
            pltpu.VMEM((total, hd), BF16),
            pltpu.VMEM((hd, total), F32),
            pltpu.VMEM((2 * hd, total), F32),
            pltpu.VMEM((nc, 3 * hd, rows), BF16),
            pltpu.VMEM((own, width), BF16),
            pltpu.VMEM((1, total), F32),
            pltpu.VMEM((nf, nc, deep, heads_wide), BF16),
            pltpu.VMEM((nf - 1, nc, deep, units // 2), BF16),
            pltpu.VMEM((nc, deep, units // 2), BF16),
            pltpu.VMEM((nf - 1, nc, deep, units), BF16),
            pltpu.VMEM((nf - 1, nc, deep, heads_wide), BF16),
            pltpu.VMEM((nc, deep, units), BF16),
            pltpu.VMEM((nc, deep, heads_wide), BF16),
            pltpu.VMEM((nc - 1, deep, units // 2), BF16),
            pltpu.VMEM((nc - 1, deep, units), BF16),
            pltpu.VMEM((nc - 1, deep, heads_wide), BF16),
            pltpu.VMEM((nc, 3 * hd, rows), BF16),
            pltpu.VMEM((3, own, width), BF16),
            pltpu.VMEM((3, own, width), BF16),
            pltpu.VMEM((nf, nc, deep, 2 * heads_wide), BF16),
            pltpu.VMEM((nf - 1, nc, deep, 2 * heads_wide), BF16),
            pltpu.VMEM((nc, deep, 2 * heads_wide), BF16),
            pltpu.VMEM((nc - 1, deep, 2 * heads_wide), BF16),
            pltpu.VMEM((nf, nc, deep, heads_wide), BF16),
            pltpu.VMEM((nf - 1, nc, deep, heads_wide), BF16),
            pltpu.VMEM((nc, deep, heads_wide), BF16),
            pltpu.VMEM((nc - 1, deep, heads_wide), BF16),
            pltpu.VMEM((inner, high, 128), F32),
            pltpu.VMEM((inner, high, 128), F32),
            pltpu.VMEM((high, 128), F32),
            pltpu.VMEM((group, high, 128), F32),
            pltpu.VMEM((tall, 128), F32),
            pltpu.VMEM((1, width), F32),
            DMA((9,)), DMA((nc, 4)), DMA((nc, 4)), DMA((2, nc)), DMA((2, nc)),
            DMA, DMA,
        ]
        + share_sems() * 4
        + [DMA((4,))] * 2
        + [DMA((nf,))] * 12
        + [DMA((nc,))] * 12
        + [DMA((inner,))] * 2
        + [DMA((group,))] * 2
        + [DMA((group * 4,))] * 2,
        3,
        150,
        60,
        ins=(1, 2, 3, 4, 9, 15, 16, 17, 21),
    )(
        attn_own, out_t, att, qkv, out, lse, sh_cross, sh_own, middle, cot, mod, bias,
        shrink_half, shrink_grad, expand_grad, weight_t, hidden, tok, mid_grad, stats_second,
        hidden_stats, modw, low,
    )


def update(master, first, root, gradient, clip, decay_rate):
    scaled = clip * gradient
    first_moment = first_decay * first + (1.0 - first_decay) * scaled
    second_moment = second_decay * root * root + (1.0 - second_decay) * scaled * scaled
    new_root = jnp.sqrt(second_moment)
    first_hat = first_moment * (1.0 / (1.0 - first_decay**ADAM_STEP))
    second_hat = second_moment * (1.0 / (1.0 - second_decay**ADAM_STEP))
    updated = master - learning_rate * (
        first_hat / (jnp.sqrt(second_hat) + adam_epsilon) + decay_rate * master
    )
    return updated, first_moment, new_root


def adam_body(count, nf, nc, done, condition, bias_rows, tokens_hbm, mixed_hbm, *refs):
    grads = refs[:count]
    masters = refs[count : 2 * count]
    moments = refs[2 * count : 3 * count]
    smalls = refs[3 * count : 3 * count + 8]
    outs = refs[3 * count + 8 :]
    news = outs[:count]
    averages = outs[count : 2 * count]
    small_outs = outs[2 * count : 2 * count + 8]
    condition_grad, norm, tokens_out, mixed_out = outs[2 * count + 8 : 2 * count + 12]
    scratch = outs[2 * count + 12 :]
    wbufs = scratch[:count]
    mbufs = scratch[count : 2 * count]
    gbufs = scratch[2 * count : 3 * count]
    tokens_low, mixed, wide, isem, osem, tsem = scratch[3 * count :]
    token_load = pltpu.make_async_copy(tokens_hbm, tokens_low, tsem.at[5])
    mixed_load = pltpu.make_async_copy(mixed_hbm, mixed, tsem.at[6])
    group = nf * nc
    f = lax.axis_index("fsdp")
    loads, stores = [], []
    for k in range(count):
        loads.append(
            (
                pltpu.make_async_copy(masters[k], wbufs[k], isem.at[0, k]),
                pltpu.make_async_copy(moments[k], mbufs[k], isem.at[1, k]),
                pltpu.make_async_copy(grads[k], gbufs[k], isem.at[2, k]),
            )
        )
        stores.append(
            (
                pltpu.make_async_copy(wbufs[k], news[k], osem.at[0, k]),
                pltpu.make_async_copy(mbufs[k], averages[k], osem.at[1, k]),
            )
        )
    for copy in loads[0]:
        copy.start()
    token_load.start()
    mixed_load.start()
    for group_ in loads[1:]:
        for copy in group_:
            copy.start()
    token_load.wait()
    mixed_load.wait()
    mixed_copy = pltpu.make_async_copy(mixed, mixed_out, tsem.at[4])
    mixed_copy.start()
    token_copies = []
    for k in range(4):

        def widen(i, carry, k=k):
            at = pl.ds(pl.multiple_of(i * 16, 16), 16)
            wide[k, at, :] = tokens_low[k, at, :].astype(F32)
            return carry

        lax.fori_loop(0, wide.shape[1] // 16, widen, 0)
        copy = pltpu.make_async_copy(wide.at[k], tokens_out.at[k], tsem.at[k])
        copy.start()
        token_copies.append(copy)
    folded = [done[k, 0] + done[k, 1] + done[k, 2] + done[k, 3] for k in range(group)]
    squares = folded[0][nf : nf + 1, 0:1]
    for k in range(1, group):
        squares = squares + folded[k][nf : nf + 1, 0:1]
    grad_norm = jnp.sqrt(squares)
    norm[...] = grad_norm
    clip = jnp.minimum(1.0, clip_limit / (grad_norm + 1e-06))
    deep = condition.shape[1] // group
    found = []
    for k in range(group):
        row = done[k, 0, pl.ds(f, 1), 0:deep]
        for tt in range(1, 4):
            row = row + done[k, tt, pl.ds(f, 1), 0:deep]
        found.append(row)
    v = condition[pl.ds(f, 1), :]
    gate = 1.0 / (1.0 + jnp.exp(-v))
    condition_grad[...] = jnp.concatenate(found, axis=1) * (gate * (1.0 + v * (1.0 - gate)))
    for k in range(4):
        master, moment = smalls[2 * k], smalls[2 * k + 1]
        if k < 3:
            row = (2, 1, 0)[k]
            grad = bias_rows[row : row + 1, 0 : master.shape[1]]
            new, first, root = update(master[...], moment[0:1, :], moment[1:2, :], grad, clip, 0.0)
            small_outs[2 * k][...] = new
            small_outs[2 * k + 1][0:1, :] = first
            small_outs[2 * k + 1][1:2, :] = root
        else:
            grad = bias_rows[3:5, 0 : master.shape[1]]
            new, first, root = update(master[...], moment[0], moment[1], grad, clip, 0.0)
            small_outs[2 * k][...] = new
            small_outs[2 * k + 1][0] = first
            small_outs[2 * k + 1][1] = root
    for k in range(count):
        for copy in loads[k]:
            copy.wait()
        deep_k = wbufs[k].shape[0]
        step = min(16, deep_k)

        def rows(i, carry, k=k, step=step):
            at = pl.ds(pl.multiple_of(i * step, step), step)
            new, first, root = update(
                wbufs[k][at, :], mbufs[k][0, at, :], mbufs[k][1, at, :], gbufs[k][at, :],
                clip, weight_decay,
            )
            wbufs[k][at, :] = new
            mbufs[k][0, at, :] = first
            mbufs[k][1, at, :] = root
            return carry

        lax.fori_loop(0, deep_k // step, rows, 0)
        for copy in stores[k]:
            copy.start()
    for pair in stores:
        for copy in pair:
            copy.wait()
    for copy in token_copies + [mixed_copy]:
        copy.wait()


def adam(nf, nc, done, condition, bias_rows, tokens_low, mixed, grads, masters, moments, smalls):
    count = len(grads)
    anywhere = pl.BlockSpec(memory_space=pltpu.HBM)
    small_shapes = tuple(shape(a.shape, F32) for a in smalls)
    outs = (
        tuple(shape(m.shape, F32) for m in masters)
        + tuple(shape(m.shape, F32) for m in moments)
        + small_shapes
        + (shape((1, condition.shape[1]), F32), shape((1, 1), F32))
        + (shape(tokens_low.shape, F32), shape(mixed.shape, BF16))
    )
    return pl.pallas_call(
        partial(adam_body, count, nf, nc),
        out_shape=outs,
        in_specs=vmem(3) + [anywhere] * (2 + 3 * count) + vmem(8),
        out_specs=[anywhere] * (2 * count) + vmem(10) + [anywhere] * 2,
        scratch_shapes=[pltpu.VMEM(m.shape, F32) for m in masters]
        + [pltpu.VMEM(m.shape, F32) for m in moments]
        + [pltpu.VMEM(m.shape, F32) for m in masters]
        + [
            pltpu.VMEM(tokens_low.shape, BF16), pltpu.VMEM(mixed.shape, BF16),
            pltpu.VMEM(tokens_low.shape, F32),
        ]
        + [DMA((3, count)), DMA((2, count)), DMA((7,))],
        compiler_params=pltpu.CompilerParams(vmem_limit_bytes=63 << 20),
        cost_estimate=cost(10),
        name="adam",
    )(done, condition, bias_rows, tokens_low, mixed, *grads, *masters, *moments, *smalls)


def local(
    nf,
    nc,
    tokens,
    condition,
    cotangent,
    joint_weight,
    joint_moments,
    output_weight,
    output_moments,
    expand_weight,
    expand_moments,
    shrink_weight,
    shrink_moments,
    modulate_weight,
    modulate_moments,
    attention_bias,
    attention_moments,
    hidden_bias,
    hidden_moments,
    condition_bias,
    condition_moments,
    residual_bias,
    residual_moments,
):
    latent_count, rows, width = tokens.shape
    heads = joint_weight.shape[1] // (3 * HEAD_DIM)
    assert latent_count == 1 and heads == nc and lax.axis_size("tp") == 4
    f, c, t = lax.axis_index("fsdp"), lax.axis_index("ctx"), lax.axis_index("tp")
    mine = f * nc + c
    deep, part = modulate_weight.shape
    units = expand_weight.shape[1]
    tok, cot = tokens[0], cotangent[0]

    condition_low = jax.nn.silu(condition).astype(BF16)
    condition_here = lax.dynamic_slice_in_dim(condition_low, mine * deep, deep, 1)
    condition_pad = jnp.pad(condition_here, ((0, 16 - nf), (0, 0)))
    (
        hidden_first, joint_full_t, mod, out_t, qkv, out, lse, att, expand_full,
        value, middle, hidden_two, shrink_early,
    ) = forward(
        nf, nc, part, tok, joint_weight, condition_pad, modulate_weight, condition_bias[None, :],
        attention_bias[None, :],
        output_weight, expand_weight, residual_bias, shrink_weight,
    )
    (
        attn_own, mid_grad, shrink_half, shrink_late, expand_grad, stats_second, hidden_stats,
        sh_cross, sh_own,
    ) = branch(
        nf, nc, part, hidden_two, cot, expand_full, shrink_weight, shrink_early, hidden_bias[None, :], mod, middle, value,
    )
    (
        mixed, tokens_grad, shrink_sum, expand_sum, output_sum, joint_sum, modulate_sum,
        bias_rows, done,
    ) = backward(
        nf, nc, part, attn_own, out_t, att, qkv, out, lse, sh_cross, sh_own, middle, cot,
        mod, residual_bias, shrink_half, shrink_late, expand_grad, joint_full_t, hidden_first,
        tok, mid_grad, stats_second, hidden_stats, modulate_weight, condition_pad.astype(F32),
    )
    weights = (joint_weight, output_weight, expand_weight, shrink_weight, modulate_weight)
    moments = (joint_moments, output_moments, expand_moments, shrink_moments, modulate_moments)
    grads = (joint_sum, output_sum, expand_sum, shrink_sum, modulate_sum)
    smalls = (
        attention_bias[None, :], attention_moments, hidden_bias[None, :], hidden_moments,
        condition_bias[None, :], condition_moments, residual_bias, residual_moments,
    )
    results = adam(nf, nc, done, condition, bias_rows, tokens_grad, mixed, grads, weights, moments, smalls)
    updated = []
    for k in range(5):
        updated += [results[k], results[5 + k]]
    for k in range(4):
        new = results[10 + 2 * k]
        updated += [new[0] if k < 3 else new, results[11 + 2 * k]]
    return (
        results[21].reshape(1, rows, width),
        results[20].reshape(1, rows, width),
        results[18],
        results[19].reshape(()),
    ) + tuple(updated)


def solution(mesh):
    rows = P(("fsdp", "ctx"), "tp")
    pair = P(None, ("fsdp", "ctx"), "tp")
    tokens = P("fsdp", "ctx", None)
    small = (P("tp"), P(None, "tp"))
    return jax.shard_map(
        partial(local, mesh.shape["fsdp"], mesh.shape["ctx"]),
        mesh=mesh,
        in_specs=(tokens, P(), tokens) + (rows, pair) * 5 + small * 3 + (P(), P()),
        out_specs=(tokens, tokens, P("fsdp", None), P())
        + (rows, pair) * 5
        + small * 3
        + (P(), P()),
        check_vma=False,
    )
```
